128 devices in a mesh: fsdp: 8 (over z_hi, y), tp: 16 (over z_lo, x, core).
Axes of the slice: x: 4, y: 4, z: 4 (z_hi: 2, z_lo: 2; z = z_hi * 2 + z_lo), core: 2. Of those that a mesh axis runs over, the one named last changes fastest.
Arguments:
- tokens: bfloat16 [2048, 8192], P('fsdp', 'tp'), may hold values from -6 to 6
- out_grad: bfloat16 [2048, 8192], P('fsdp', 'tp'), may hold values from -6 to 6
- gate_weight: bfloat16 [8192, 2048], P('fsdp', 'tp'), may hold values from -0.0625 to 0.0625
- up_weight: bfloat16 [8192, 2048], P('fsdp', 'tp'), may hold values from -0.0625 to 0.0625
- down_weight: bfloat16 [2048, 8192], P('tp', 'fsdp'), may hold values from -0.125 to 0.125
Outputs:
- input_grad: bfloat16 [2048, 8192], P('fsdp', 'tp')
- gate_grad: float32 [8192, 2048], P('fsdp', 'tp')
- up_grad: float32 [8192, 2048], P('fsdp', 'tp')
- down_grad: float32 [2048, 8192], P('tp', 'fsdp')
The draws below stay inside these ranges and needn't reach their ends.
All inputs are finite; a program needn't handle non-finite values.
Results may differ from the reference program's by a relative error of at most 0.0023.
Values may be sent and summed in bfloat16 or wider, within the bound.
A program may use at most 128 MiB of HBM per device.

```python
import math
import jax
import jax.numpy as jnp

D = 8192
FF_WIN = 2048
TOKENS = 2048


def spiked(values, stream_key, source, target, blocks, factor):
    def block_of(dim):
        return (jnp.arange(values.shape[dim]) // (values.shape[dim] // blocks)).reshape((-1,) + (1,) * (values.ndim - 1 - dim))

    one_side = jax.random.permutation(stream_key, blocks)[block_of(target)]
    other_side = (block_of(target) + blocks // 2) % blocks
    return jnp.where((block_of(source) == one_side) | (block_of(source) == other_side), factor * values, values)


def level_of(key, dims, shards, low, largest):
    factor_of = 1.0
    for dim, shards_of in shards:
        heights = jax.random.uniform(jax.random.fold_in(jax.random.fold_in(key, 6), dim), (shards_of,), jnp.float32, low / len(shards), largest / len(shards))
        factor_of = factor_of * jnp.repeat(jnp.exp(heights), dims[dim] // shards_of).reshape((-1,) + (1,) * (len(dims) - 1 - dim))
    return factor_of


def gaussian(key, extent, deviation, bound, pieces=(), dtype=jnp.bfloat16):
    array = jax.random.normal(key, extent, jnp.float32) * deviation
    if len(pieces) > 0:
        array = level_of(key, extent, pieces, -0.22, 0.18) * array
    return jnp.clip(array, min=-bound, max=bound).astype(dtype)


def bell_draw_with(rng, shape, width, most, split, heavy, kind=jnp.bfloat16):
    result = width * jax.random.normal(rng, shape, jnp.float32)
    if split:
        result = result * level_of(rng, shape, split, -0.22, 0.18)
    return jnp.clip(spiked(result, jax.random.fold_in(rng, 3), *heavy), -most, most).astype(kind)


def setup_inputs(seed: int = 0) -> dict:
    seeds = jax.random.split(jax.random.key(seed), 6)
    return {
        "tokens": bell_draw_with(seeds[0], (TOKENS, D), 1.0, 6.0, ((0, 8), (1, 16)), (0, 1, 16, 2.0)),
        "out_grad": bell_draw_with(seeds[1], (TOKENS, D), 1.0, 6.0, ((0, 8), (1, 16)), (0, 1, 16, 2.0)),
        "gate_weight": gaussian(seeds[2], (D, FF_WIN), D ** -0.5, 0.0625, ((0, 8), (1, 16))),
        "up_weight": gaussian(seeds[3], (D, FF_WIN), D ** -0.5, 0.0625, ((0, 8), (1, 16))),
        "down_weight": gaussian(seeds[4], (FF_WIN, D), FF_WIN ** -0.5, 0.125, ((0, 16), (1, 8))),
    }


def reference(tokens, out_grad, gate_weight, up_weight, down_weight):
    gate = jnp.dot(tokens, gate_weight, preferred_element_type=jnp.float32)
    up = jnp.dot(tokens, up_weight, preferred_element_type=jnp.float32)
    squashed = jax.nn.sigmoid(gate)
    activated = gate * squashed
    slope = squashed * (1.0 + gate * (1.0 - squashed))
    hidden = (activated * up).astype(jnp.bfloat16)
    hidden_grad = jnp.dot(out_grad, down_weight.T, preferred_element_type=jnp.float32)
    gate_delta = (hidden_grad * up * slope).astype(jnp.bfloat16)
    up_delta = (hidden_grad * activated).astype(jnp.bfloat16)
    input_grad = jnp.dot(gate_delta, gate_weight.T, preferred_element_type=jnp.float32)
    input_grad = input_grad + jnp.dot(up_delta, up_weight.T, preferred_element_type=jnp.float32)
    factor = 1.0 / math.sqrt(TOKENS)
    gate_grad = jnp.dot(tokens.T, gate_delta, preferred_element_type=jnp.float32) * factor
    up_grad = jnp.dot(tokens.T, up_delta, preferred_element_type=jnp.float32) * factor
    down_grad = jnp.dot(hidden.T, out_grad, preferred_element_type=jnp.float32) * factor
    return (input_grad.astype(jnp.bfloat16), gate_grad, up_grad, down_grad)
```

```python
import functools
import math

import jax
import jax.numpy as jnp
from jax import lax
from jax.experimental import pallas as pl
from jax.experimental.pallas import tpu as pltpu
from jax.sharding import PartitionSpec as P

MESH = pl.DeviceIdType.MESH
F32, BF16 = jnp.float32, jnp.bfloat16
COPIES = 160


class Copy:
    def __init__(self, sems, src, dst, to, here=None):
        self.index = sems[2][0]
        sems[2][0] += 1
        send, recv = sems[0].at[self.index], sems[1].at[self.index]
        self.remote = pltpu.make_async_remote_copy(
            src_ref=src, dst_ref=dst, send_sem=send, recv_sem=recv, device_id=to, device_id_type=MESH
        )
        self.local = None if here is None else pltpu.make_async_copy(src, dst, recv)
        self.here = here

    def start(self):
        if self.here is None:
            self.remote.start()
        else:
            pl.when(self.here)(self.local.start)
            pl.when(jnp.logical_not(self.here))(self.remote.start)
        return self

    def wait(self):
        self.remote.wait_recv()

    def sent(self):
        if self.here is None:
            self.remote.wait_send()
        else:
            pl.when(jnp.logical_not(self.here))(self.remote.wait_send)


def nt(a, b):
    return lax.dot_general(a, b, (((1,), (1,)), ((), ())), preferred_element_type=F32)


def tn(a, b):
    return lax.dot_general(a, b, (((0,), (0,)), ((), ())), preferred_element_type=F32)


def nn(a, b):
    return jnp.dot(a, b, preferred_element_type=F32)


def kernel(
    factor,
    tok_ref, grd_ref, gate_ref, up_ref, down_ref,
    ig_ref, gg_ref, ug_ref, dg_ref,
    G, WG, WD, DS, DR, Q, RF, RN, DL, X, XF, XN, IB,
    Z, ZS, ZF, ZN, S, SX,
    SD, send, recv, local_sem,
):
    f, t = lax.axis_index("fsdp"), lax.axis_index("tp")
    h, y = lax.div(f, 4), lax.rem(f, 4)
    c = lax.rem(t, 2)
    x = lax.rem(lax.div(t, 2), 4)
    l = lax.div(t, 8)
    z = 2 * h + l
    sems = (send, recv, [0])
    sent = []

    def dev(x=x, y=y, z=z, c=c):
        return (lax.div(z, 2) * 4 + y, (lax.rem(z, 2) * 4 + x) * 2 + c)

    def copy(src, dst, to, here=None):
        made = Copy(sems, src, dst, to, here)
        sent.append(made)
        return made.start()

    def turn(v, k):
        return lax.rem(v + k + 4, 4)

    xp, xm, yp, ym, zp, zm = (turn(v, k) for v in (x, y, z) for k in (1, -1))
    yf, xf, zf = turn(y, 2), turn(x, 2), turn(z, 2)
    cc, ll = 1 - c, 1 - l
    zo = 2 * h + ll
    diagonal = x == y
    twin = dev(c=cc)

    barrier = pltpu.get_barrier_semaphore()
    peers = [
        twin, dev(x=xp), dev(x=xm), dev(y=yp), dev(y=ym),
        dev(z=zp), dev(z=zm), dev(z=zp, c=cc), dev(z=zm, c=cc), dev(x=y, y=x, z=zo),
    ]
    for peer in peers:
        pl.semaphore_signal(barrier, inc=1, device_id=peer, device_id_type=MESH)

    @pl.when(jnp.logical_not(diagonal))
    def _():
        pl.semaphore_signal(barrier, inc=1, device_id=dev(x=y, y=x), device_id_type=MESH)
        pl.semaphore_wait(barrier, len(peers) + 1)

    @pl.when(diagonal)
    def _():
        pl.semaphore_wait(barrier, len(peers))

    moved = {}
    arrays = (tok_ref, grd_ref)
    for a in range(2):
        for other in range(2):
            to_l = ll if other else l
            moved[a, other] = copy(
                arrays[a].at[pl.ds(pl.multiple_of(to_l * 128, 128), 128), :],
                G.at[a, l, y],
                dev(x=y, y=x, z=zo) if other else dev(x=y, y=x),
                None if other else diagonal,
            )

    def weight_piece(i, k):
        half = pl.multiple_of(k * 512, 512)
        if i < 2:
            return (gate_ref, up_ref)[i].at[pl.ds(half, 512), :]
        return down_ref.at[:, pl.ds(half, 512)]

    def weight_slot(i, at_z, core):
        at_h, block = lax.div(at_z, 2), lax.rem(at_z, 2) * 2 + core
        return WG.at[i, at_h, block] if i < 2 else WD.at[at_h, block]

    own_weights, from_twin, wp, wm = [], {}, {}, {}
    for i in range(3):
        mine = pltpu.make_async_copy(weight_piece(i, c), weight_slot(i, z, c), local_sem.at[i])
        mine.start()
        own_weights.append(mine)
        slot = weight_slot(i, z, c)
        wp[i, 0] = copy(weight_piece(i, c), slot, dev(z=zp))
        wm[i, 1] = copy(weight_piece(i, cc), slot, dev(z=zm, c=cc))
        wp[i, 1] = copy(weight_piece(i, cc), slot, dev(z=zp, c=cc))
        wm[i, 0] = copy(weight_piece(i, c), slot, dev(z=zm))
        from_twin[i] = copy(weight_piece(i, cc), slot, twin)

    far_w = {}

    def pass_weights(i):
        wp[i, 0].wait()
        slot = weight_slot(i, zm, c)
        far_w[i, 0] = copy(slot, slot, dev(z=zp))
        wm[i, 1].wait()
        slot = weight_slot(i, zp, cc)
        far_w[i, 1] = copy(slot, slot, dev(z=zm))

    def weights_here(i):
        own_weights[i].wait()
        from_twin[i].wait()
        wp[i, 1].wait()
        wm[i, 0].wait()
        far_w[i, 0].wait()
        far_w[i, 1].wait()

    gp, gm, far_g = {}, {}, {}
    for a in range(2):
        for other in range(2):
            moved[a, other].wait()
            slot = G.at[a, ll if other else l, x]
            gp[a, other] = copy(slot, slot, dev(x=xp))
            gm[a, other] = copy(slot, slot, dev(x=xm))

    def pass_tokens(a):
        gp[a, 0].wait()
        slot = G.at[a, l, xm]
        far_g[a, 0] = copy(slot, slot, dev(x=xp))
        gm[a, 1].wait()
        slot = G.at[a, ll, xp]
        far_g[a, 1] = copy(slot, slot, dev(x=xm))

    def tokens_here(a):
        gp[a, 1].wait()
        gm[a, 0].wait()
        far_g[a, 0].wait()
        far_g[a, 1].wait()

    pass_weights(0)
    pass_tokens(0)
    pass_weights(1)
    pass_tokens(1)
    pass_weights(2)

    def product(i, pair, l_to):
        total = None
        for k in range(2):
            rows = jnp.concatenate([G[min(i // 2, 1), k, pair * 2], G[min(i // 2, 1), k, pair * 2 + 1]], axis=0)
            if i < 2:
                right = jnp.concatenate([WG[i, k, 2 * l_to], WG[i, k, 2 * l_to + 1]], axis=1)
                term = nn(rows, right)
            else:
                right = jnp.concatenate([WD[k, 2 * l_to], WD[k, 2 * l_to + 1]], axis=0)
                term = nt(rows, right)
            total = term if total is None else total + term
        return total

    to_twin = {}

    def multiply(i):
        for l_to in range(2):
            DS[i, :, l_to] = product(i, cc, l_to).reshape(4, 64, 256)
        to_twin[i] = copy(DS.at[i], DR.at[i], twin)
        for l_to in range(2):
            Q[i, :, l_to] = product(i, c, l_to).reshape(4, 64, 256)

    yfar, ynear = {}, {}

    def sum_start(i):
        to_twin[i].wait()
        Q[i] += DR[i]
        yfar[i, 0] = copy(Q.at[i, yf, 0], RF.at[i, 0], dev(y=yp))
        yfar[i, 1] = copy(Q.at[i, yf, 1], RF.at[i, 1], dev(y=ym))
        ynear[i, 0, 1] = copy(Q.at[i, yp, 1], RN.at[i, 0, 1], dev(y=yp))
        ynear[i, 1, 0] = copy(Q.at[i, ym, 0], RN.at[i, 1, 0], dev(y=ym))

    def sum_middle(i):
        yfar[i, 0].wait()
        Q[i, yp, 0] += RF[i, 0]
        ynear[i, 0, 0] = copy(Q.at[i, yp, 0], RN.at[i, 0, 0], dev(y=yp))
        yfar[i, 1].wait()
        Q[i, ym, 1] += RF[i, 1]
        ynear[i, 1, 1] = copy(Q.at[i, ym, 1], RN.at[i, 1, 1], dev(y=ym))

    def sum_end(i, half):
        return Q[i, y, half] + RN[i, 0, half] + RN[i, 1, half]

    tokens_here(0)
    weights_here(0)
    multiply(0)
    sum_start(0)
    weights_here(1)
    multiply(1)
    sum_middle(0)
    sum_start(1)
    tokens_here(1)
    weights_here(2)
    multiply(2)
    sum_middle(1)
    sum_start(2)
    sum_middle(2)
    for i in range(3):
        for side in range(2):
            for half in range(2):
                ynear[i, side, half].wait()

    for half in range(2):
        gate, up, hidden_grad = sum_end(0, half), sum_end(1, half), sum_end(2, half)
        squashed = jax.nn.sigmoid(gate)
        activated = gate * squashed
        slope = squashed * (1.0 + gate * (1.0 - squashed))
        DL[c, y, 0, half] = (hidden_grad * up * slope).astype(BF16)
        DL[c, y, 1, half] = (hidden_grad * activated).astype(BF16)
        DL[c, y, 2, half] = (activated * up).astype(BF16)

    dp, dm, far_d, over = {}, {}, {}, []
    first, second = pl.ds(0, 32), pl.ds(32, 32)

    def delta_part(at_y, rows):
        return DL.at[c, at_y, :, :, rows]

    dp[0] = copy(delta_part(y, first), delta_part(y, first), dev(y=yp))
    dm[1] = copy(delta_part(y, second), delta_part(y, second), dev(y=ym))
    dp[1] = copy(delta_part(y, second), delta_part(y, second), dev(y=yp))
    dm[0] = copy(delta_part(y, first), delta_part(y, first), dev(y=ym))
    over.append(copy(DL.at[c, y], DL.at[c, y], twin))
    dp[0].wait()
    far_d[0] = copy(delta_part(ym, first), delta_part(ym, first), dev(y=yp))
    dm[1].wait()
    far_d[1] = copy(delta_part(yp, second), delta_part(yp, second), dev(y=ym))
    dp[1].wait()
    over.append(copy(DL.at[c, ym], DL.at[c, ym], twin))
    dm[0].wait()
    over.append(copy(DL.at[c, yp], DL.at[c, yp], twin))
    far_d[0].wait()
    far_d[1].wait()
    over.append(copy(DL.at[c, yf], DL.at[c, yf], twin))
    for made in over:
        made.wait()

    def delta(kind, l_to, core):
        return jnp.concatenate([DL[core, k, kind, l_to] for k in range(4)], axis=0)

    def delta_all(kind, l_to):
        return jnp.concatenate([delta(kind, l_to, 0), delta(kind, l_to, 1)], axis=0)

    def gathered(a, k):
        return G[a, k].reshape(512, 512)

    def grads_of_weights(i):
        for k in range(2):
            for m in range(2):
                if i < 2:
                    Z[i, 2 * k + m] = tn(gathered(0, k), delta_all(i, m)).reshape(2, 256, 256)
                else:
                    block = tn(delta_all(2, m), gathered(1, k))
                    for j in range(2):
                        Z[2, 2 * k + m, j] = jnp.concatenate(
                            [block[j * 128 : j * 128 + 128, :256], block[j * 128 : j * 128 + 128, 256:]], axis=0
                        )

    zfar, znear = {}, {}

    def wsum_start(i):
        ZS[i, 0] = Z[i, zf].astype(BF16)
        ZS[i, 1, 1] = Z[i, zp, 1].astype(BF16)
        ZS[i, 2, 0] = Z[i, zm, 0].astype(BF16)
        zfar[i, 0] = copy(ZS.at[i, 0, 0], ZF.at[i, 0], dev(z=zp))
        zfar[i, 1] = copy(ZS.at[i, 0, 1], ZF.at[i, 1], dev(z=zm))
        znear[i, 0, 1] = copy(ZS.at[i, 1, 1], ZN.at[i, 0, 1], dev(z=zp))
        znear[i, 1, 0] = copy(ZS.at[i, 2, 0], ZN.at[i, 1, 0], dev(z=zm))

    def wsum_middle(i):
        zfar[i, 0].wait()
        ZS[i, 1, 0] = (Z[i, zp, 0] + ZF[i, 0].astype(F32)).astype(BF16)
        znear[i, 0, 0] = copy(ZS.at[i, 1, 0], ZN.at[i, 0, 0], dev(z=zp))
        zfar[i, 1].wait()
        ZS[i, 2, 1] = (Z[i, zm, 1] + ZF[i, 1].astype(F32)).astype(BF16)
        znear[i, 1, 1] = copy(ZS.at[i, 2, 1], ZN.at[i, 1, 1], dev(z=zm))

    def wsum_end(i):
        for side in range(2):
            for half in range(2):
                znear[i, side, half].wait()
        return [
            (Z[i, z, half] + ZN[i, 0, half].astype(F32) + ZN[i, 1, half].astype(F32)) * factor
            for half in range(2)
        ]

    def input_term(pair, k):
        total = None
        for kind in range(2):
            left = jnp.concatenate([delta_pair(kind, pair, 0), delta_pair(kind, pair, 1)], axis=1)
            right = jnp.concatenate([WG[kind, k, b] for b in range(4)], axis=1)
            term = nt(left, right)
            total = term if total is None else total + term
        return total

    def delta_pair(kind, pair, l_to):
        return delta(kind, l_to, pair)

    xfar, xnear = {}, {}

    def isum_start():
        xfar[0] = copy(X.at[xf, 0], XF.at[0], dev(x=xp))
        xfar[1] = copy(X.at[xf, 1], XF.at[1], dev(x=xm))
        xnear[0, 1] = copy(X.at[xp, 1], XN.at[0, 1], dev(x=xp))
        xnear[1, 0] = copy(X.at[xm, 0], XN.at[1, 0], dev(x=xm))

    def isum_middle():
        xfar[0].wait()
        X[xp, 0] += XF[0]
        xnear[0, 0] = copy(X.at[xp, 0], XN.at[0, 0], dev(x=xp))
        xfar[1].wait()
        X[xm, 1] += XF[1]
        xnear[1, 1] = copy(X.at[xm, 1], XN.at[1, 1], dev(x=xm))

    grads_of_weights(0)
    wsum_start(0)
    for pair in range(2):
        for k in range(2):
            term = input_term(pair, k)
            X[2 * pair, k] = term[:128]
            X[2 * pair + 1, k] = term[128:]
    isum_start()
    grads_of_weights(1)
    wsum_start(1)
    grads_of_weights(2)
    wsum_start(2)
    wsum_middle(0)
    isum_middle()
    wsum_middle(1)
    wsum_middle(2)

    back = {}
    for side in range(2):
        for half in range(2):
            xnear[side, half].wait()
    for k in range(2):
        IB[k] = (X[x, k] + XN[0, k] + XN[1, k]).astype(BF16)
    for other in range(2):
        k = ll if other else l
        back[other] = copy(
            IB.at[k],
            ig_ref.at[pl.ds(pl.multiple_of(l * 128, 128), 128), :],
            dev(x=y, y=x, z=zo) if other else dev(x=y, y=x),
            None if other else diagonal,
        )

    last = []
    half_at = pl.multiple_of(c * 512, 512)
    for i in range(2):
        out = (gg_ref, ug_ref)[i]
        done = wsum_end(i)
        for half in range(2):
            low, high = done[half][:, :128], done[half][:, 128:]
            SX[i, pl.ds(half * 256, 256), :] = jnp.where(c == 0, high, low)
            S[i, pl.ds(half * 256, 256), :] = jnp.where(c == 0, low, high)
        rows = pl.ds(half_at, 512)
        last.append(copy(SX.at[i], out.at[rows, :], twin))
        out[rows, :] = S[i]
    done = wsum_end(2)
    blocks = [jnp.concatenate([part[:128], part[128:]], axis=1) for part in done]
    columns = pl.ds(half_at, 512)
    SD[...] = jnp.where(c == 0, blocks[1], blocks[0])
    last.append(copy(SD, dg_ref.at[:, columns], twin))
    dg_ref[:, columns] = jnp.where(c == 0, blocks[0], blocks[1])
    for made in [*last, *back.values()]:
        made.wait()
    for made in sent:
        made.sent()


def solution(mesh):
    def shards(tokens, out_grad, gate_weight, up_weight, down_weight):
        factor = 1.0 / math.sqrt(tokens.shape[0] * mesh.shape["fsdp"])
        vmem = pl.BlockSpec(memory_space=pltpu.VMEM)
        return pl.pallas_call(
            functools.partial(kernel, factor),
            out_shape=(
                jax.ShapeDtypeStruct((256, 512), BF16),
                jax.ShapeDtypeStruct((1024, 128), F32),
                jax.ShapeDtypeStruct((1024, 128), F32),
                jax.ShapeDtypeStruct((128, 1024), F32),
            ),
            in_specs=[vmem] * 5,
            out_specs=(vmem,) * 4,
            scratch_shapes=[
                pltpu.VMEM((2, 2, 4, 128, 512), BF16),
                pltpu.VMEM((2, 2, 4, 512, 128), BF16),
                pltpu.VMEM((2, 4, 128, 512), BF16),
                pltpu.VMEM((3, 4, 2, 64, 256), F32),
                pltpu.VMEM((3, 4, 2, 64, 256), F32),
                pltpu.VMEM((3, 4, 2, 64, 256), F32),
                pltpu.VMEM((3, 2, 64, 256), F32),
                pltpu.VMEM((3, 2, 2, 64, 256), F32),
                pltpu.VMEM((2, 4, 3, 2, 64, 256), BF16),
                pltpu.VMEM((4, 2, 128, 512), F32),
                pltpu.VMEM((2, 128, 512), F32),
                pltpu.VMEM((2, 2, 128, 512), F32),
                pltpu.VMEM((2, 128, 512), BF16),
                pltpu.VMEM((3, 4, 2, 256, 256), F32),
                pltpu.VMEM((3, 3, 2, 256, 256), BF16),
                pltpu.VMEM((3, 2, 256, 256), BF16),
                pltpu.VMEM((3, 2, 2, 256, 256), BF16),
                pltpu.VMEM((2, 512, 128), F32),
                pltpu.VMEM((2, 512, 128), F32),
                pltpu.VMEM((128, 512), F32),
                pltpu.SemaphoreType.DMA((COPIES,)),
                pltpu.SemaphoreType.DMA((COPIES,)),
                pltpu.SemaphoreType.DMA((3,)),
            ],
            compiler_params=pltpu.CompilerParams(
                collective_id=0, has_side_effects=True, vmem_limit_bytes=60 * 1024 * 1024
            ),
        )(tokens, out_grad, gate_weight, up_weight, down_weight)

    return jax.shard_map(
        shards,
        mesh=mesh,
        in_specs=(P("fsdp", "tp"),) * 4 + (P("tp", "fsdp"),),
        out_specs=(P("fsdp", "tp"),) * 3 + (P("tp", "fsdp"),),
        check_vma=False,
    )
```

```python
import functools
import math

import jax
import jax.numpy as jnp
from jax import lax
from jax.experimental import pallas as pl
from jax.experimental.pallas import tpu as pltpu
from jax.sharding import PartitionSpec as P

MESH = pl.DeviceIdType.MESH
F32, BF16 = jnp.float32, jnp.bfloat16
COPIES = 160


class Copy:
    def __init__(self, sems, src, dst, to, here=None):
        self.index = sems[2][0]
        sems[2][0] += 1
        send, recv = sems[0].at[self.index], sems[1].at[self.index]
        self.remote = pltpu.make_async_remote_copy(
            src_ref=src, dst_ref=dst, send_sem=send, recv_sem=recv, device_id=to, device_id_type=MESH
        )
        self.local = None if here is None else pltpu.make_async_copy(src, dst, recv)
        self.here = here

    def start(self):
        if self.here is None:
            self.remote.start()
        else:
            pl.when(self.here)(self.local.start)
            pl.when(jnp.logical_not(self.here))(self.remote.start)
        return self

    def wait(self):
        self.remote.wait_recv()

    def sent(self):
        if self.here is None:
            self.remote.wait_send()
        else:
            pl.when(jnp.logical_not(self.here))(self.remote.wait_send)


def nt(a, b):
    return lax.dot_general(a, b, (((1,), (1,)), ((), ())), preferred_element_type=F32)


def tn(a, b):
    return lax.dot_general(a, b, (((0,), (0,)), ((), ())), preferred_element_type=F32)


def nn(a, b):
    return jnp.dot(a, b, preferred_element_type=F32)


def kernel(
    factor,
    tok_ref, grd_ref, gate_ref, up_ref, down_ref,
    ig_ref, gg_ref, ug_ref, dg_ref,
    G, WG, WD, DS, DR, Q, RF, RN, DL, X, XF, XN, IB,
    Z, ZS, ZF, ZN, S, SX,
    SD, send, recv, local_sem,
):
    f, t = lax.axis_index("fsdp"), lax.axis_index("tp")
    h, y = lax.div(f, 4), lax.rem(f, 4)
    c = lax.rem(t, 2)
    x = lax.rem(lax.div(t, 2), 4)
    l = lax.div(t, 8)
    z = 2 * h + l
    sems = (send, recv, [0])
    sent = []

    def dev(x=x, y=y, z=z, c=c):
        return (lax.div(z, 2) * 4 + y, (lax.rem(z, 2) * 4 + x) * 2 + c)

    def copy(src, dst, to, here=None):
        made = Copy(sems, src, dst, to, here)
        sent.append(made)
        return made.start()

    def turn(v, k):
        return lax.rem(v + k + 4, 4)

    xp, xm, yp, ym, zp, zm = (turn(v, k) for v in (x, y, z) for k in (1, -1))
    yf, xf, zf = turn(y, 2), turn(x, 2), turn(z, 2)
    cc, ll = 1 - c, 1 - l
    zo = 2 * h + ll
    diagonal = x == y
    twin = dev(c=cc)

    barrier = pltpu.get_barrier_semaphore()
    peers = [
        twin, dev(x=xp), dev(x=xm), dev(y=yp), dev(y=ym),
        dev(z=zp), dev(z=zm), dev(z=zp, c=cc), dev(z=zm, c=cc),
    ]
    for e in range(4):
        there, back_there = dict(x=turn(y, e), y=x), dict(x=y, y=turn(x, -e))
        peers += [dev(z=zo, **there), dev(z=zo, **back_there)]
        if e > 0:
            peers += [dev(**there), dev(**back_there)]
    for peer in peers:
        pl.semaphore_signal(barrier, inc=1, device_id=peer, device_id_type=MESH)

    @pl.when(jnp.logical_not(diagonal))
    def _():
        pl.semaphore_signal(barrier, inc=2, device_id=dev(x=y, y=x), device_id_type=MESH)
        pl.semaphore_wait(barrier, len(peers) + 2)

    @pl.when(diagonal)
    def _():
        pl.semaphore_wait(barrier, len(peers))

    moved = {}
    arrays = (tok_ref, grd_ref)
    for a in range(2):
        for other in range(2):
            to_l = ll if other else l
            for e in range(4):
                to_x = turn(y, e)
                moved[a, other, e] = copy(
                    arrays[a].at[pl.ds(pl.multiple_of(to_l * 128 + to_x * 32, 32), 32), :],
                    G.at[a, l, to_x, pl.ds(pl.multiple_of(y * 32, 32), 32), :],
                    dev(x=to_x, y=x, z=zo if other else z),
                    diagonal if e == 0 and not other else None,
                )

    def weight_piece(i, k):
        half = pl.multiple_of(k * 512, 512)
        if i < 2:
            return (gate_ref, up_ref)[i].at[pl.ds(half, 512), :]
        return down_ref.at[:, pl.ds(half, 512)]

    def weight_slot(i, at_z, core):
        at_h, block = lax.div(at_z, 2), lax.rem(at_z, 2) * 2 + core
        return WG.at[i, at_h, block] if i < 2 else WD.at[at_h, block]

    own_weights, from_twin, wp, wm = [], {}, {}, {}
    for i in range(3):
        mine = pltpu.make_async_copy(weight_piece(i, c), weight_slot(i, z, c), local_sem.at[i])
        mine.start()
        own_weights.append(mine)
        slot = weight_slot(i, z, c)
        wp[i, 0] = copy(weight_piece(i, c), slot, dev(z=zp))
        wm[i, 1] = copy(weight_piece(i, cc), slot, dev(z=zm, c=cc))
        wp[i, 1] = copy(weight_piece(i, cc), slot, dev(z=zp, c=cc))
        wm[i, 0] = copy(weight_piece(i, c), slot, dev(z=zm))
        from_twin[i] = copy(weight_piece(i, cc), slot, twin)

    far_w = {}

    def pass_weights(i):
        wp[i, 0].wait()
        slot = weight_slot(i, zm, c)
        far_w[i, 0] = copy(slot, slot, dev(z=zp))
        wm[i, 1].wait()
        slot = weight_slot(i, zp, cc)
        far_w[i, 1] = copy(slot, slot, dev(z=zm))

    def weights_here(i):
        own_weights[i].wait()
        from_twin[i].wait()
        wp[i, 1].wait()
        wm[i, 0].wait()
        far_w[i, 0].wait()
        far_w[i, 1].wait()

    gp, gm, far_g = {}, {}, {}
    for a in range(2):
        for other in range(2):
            for e in range(4):
                moved[a, other, e].wait()
            slot = G.at[a, ll if other else l, x]
            gp[a, other] = copy(slot, slot, dev(x=xp))
            gm[a, other] = copy(slot, slot, dev(x=xm))

    def pass_tokens(a):
        gp[a, 0].wait()
        slot = G.at[a, l, xm]
        far_g[a, 0] = copy(slot, slot, dev(x=xp))
        gm[a, 1].wait()
        slot = G.at[a, ll, xp]
        far_g[a, 1] = copy(slot, slot, dev(x=xm))

    def tokens_here(a):
        gp[a, 1].wait()
        gm[a, 0].wait()
        far_g[a, 0].wait()
        far_g[a, 1].wait()

    pass_weights(0)
    pass_tokens(0)
    pass_weights(1)
    pass_tokens(1)
    pass_weights(2)

    def product(i, pair, l_to):
        total = None
        for k in range(2):
            rows = jnp.concatenate([G[min(i // 2, 1), k, pair * 2], G[min(i // 2, 1), k, pair * 2 + 1]], axis=0)
            if i < 2:
                right = jnp.concatenate([WG[i, k, 2 * l_to], WG[i, k, 2 * l_to + 1]], axis=1)
                term = nn(rows, right)
            else:
                right = jnp.concatenate([WD[k, 2 * l_to], WD[k, 2 * l_to + 1]], axis=0)
                term = nt(rows, right)
            total = term if total is None else total + term
        return total

    to_twin = {}

    def multiply(i):
        for l_to in range(2):
            DS[i, :, l_to] = product(i, cc, l_to).reshape(4, 64, 256)
        to_twin[i] = copy(DS.at[i], DR.at[i], twin)
        for l_to in range(2):
            Q[i, :, l_to] = product(i, c, l_to).reshape(4, 64, 256)

    yfar, ynear = {}, {}

    def sum_start(i):
        to_twin[i].wait()
        Q[i] += DR[i]
        yfar[i, 0] = copy(Q.at[i, yf, 0], RF.at[i, 0], dev(y=yp))
        yfar[i, 1] = copy(Q.at[i, yf, 1], RF.at[i, 1], dev(y=ym))
        ynear[i, 0, 1] = copy(Q.at[i, yp, 1], RN.at[i, 0, 1], dev(y=yp))
        ynear[i, 1, 0] = copy(Q.at[i, ym, 0], RN.at[i, 1, 0], dev(y=ym))

    def sum_middle(i):
        yfar[i, 0].wait()
        Q[i, yp, 0] += RF[i, 0]
        ynear[i, 0, 0] = copy(Q.at[i, yp, 0], RN.at[i, 0, 0], dev(y=yp))
        yfar[i, 1].wait()
        Q[i, ym, 1] += RF[i, 1]
        ynear[i, 1, 1] = copy(Q.at[i, ym, 1], RN.at[i, 1, 1], dev(y=ym))

    def sum_end(i, half):
        return Q[i, y, half] + RN[i, 0, half] + RN[i, 1, half]

    tokens_here(0)
    weights_here(0)
    multiply(0)
    sum_start(0)
    weights_here(1)
    multiply(1)
    sum_middle(0)
    sum_start(1)
    tokens_here(1)
    weights_here(2)
    multiply(2)
    sum_middle(1)
    sum_start(2)
    sum_middle(2)
    for i in range(3):
        for side in range(2):
            for half in range(2):
                ynear[i, side, half].wait()

    for half in range(2):
        gate, up, hidden_grad = sum_end(0, half), sum_end(1, half), sum_end(2, half)
        squashed = jax.nn.sigmoid(gate)
        activated = gate * squashed
        slope = squashed * (1.0 + gate * (1.0 - squashed))
        DL[c, y, 0, half] = (hidden_grad * up * slope).astype(BF16)
        DL[c, y, 1, half] = (hidden_grad * activated).astype(BF16)
        DL[c, y, 2, half] = (activated * up).astype(BF16)

    dp, dm, far_d, over = {}, {}, {}, []
    first, second = pl.ds(0, 32), pl.ds(32, 32)

    def delta_part(at_y, rows):
        return DL.at[c, at_y, :, :, rows]

    dp[0] = copy(delta_part(y, first), delta_part(y, first), dev(y=yp))
    dm[1] = copy(delta_part(y, second), delta_part(y, second), dev(y=ym))
    dp[1] = copy(delta_part(y, second), delta_part(y, second), dev(y=yp))
    dm[0] = copy(delta_part(y, first), delta_part(y, first), dev(y=ym))
    over.append(copy(DL.at[c, y], DL.at[c, y], twin))
    dp[0].wait()
    far_d[0] = copy(delta_part(ym, first), delta_part(ym, first), dev(y=yp))
    dm[1].wait()
    far_d[1] = copy(delta_part(yp, second), delta_part(yp, second), dev(y=ym))
    dp[1].wait()
    over.append(copy(DL.at[c, ym], DL.at[c, ym], twin))
    dm[0].wait()
    over.append(copy(DL.at[c, yp], DL.at[c, yp], twin))
    far_d[0].wait()
    far_d[1].wait()
    over.append(copy(DL.at[c, yf], DL.at[c, yf], twin))
    for made in over:
        made.wait()

    def delta(kind, l_to, core):
        return jnp.concatenate([DL[core, k, kind, l_to] for k in range(4)], axis=0)

    def delta_all(kind, l_to):
        return jnp.concatenate([delta(kind, l_to, 0), delta(kind, l_to, 1)], axis=0)

    def gathered(a, k):
        return G[a, k].reshape(512, 512)

    def grads_of_weights(i):
        for k in range(2):
            for m in range(2):
                if i < 2:
                    Z[i, 2 * k + m] = tn(gathered(0, k), delta_all(i, m)).reshape(2, 256, 256)
                else:
                    block = tn(delta_all(2, m), gathered(1, k))
                    for j in range(2):
                        Z[2, 2 * k + m, j] = jnp.concatenate(
                            [block[j * 128 : j * 128 + 128, :256], block[j * 128 : j * 128 + 128, 256:]], axis=0
                        )

    zfar, znear = {}, {}

    def wsum_start(i):
        ZS[i, 0] = Z[i, zf].astype(BF16)
        ZS[i, 1, 1] = Z[i, zp, 1].astype(BF16)
        ZS[i, 2, 0] = Z[i, zm, 0].astype(BF16)
        zfar[i, 0] = copy(ZS.at[i, 0, 0], ZF.at[i, 0], dev(z=zp))
        zfar[i, 1] = copy(ZS.at[i, 0, 1], ZF.at[i, 1], dev(z=zm))
        znear[i, 0, 1] = copy(ZS.at[i, 1, 1], ZN.at[i, 0, 1], dev(z=zp))
        znear[i, 1, 0] = copy(ZS.at[i, 2, 0], ZN.at[i, 1, 0], dev(z=zm))

    def wsum_middle(i):
        zfar[i, 0].wait()
        ZS[i, 1, 0] = (Z[i, zp, 0] + ZF[i, 0].astype(F32)).astype(BF16)
        znear[i, 0, 0] = copy(ZS.at[i, 1, 0], ZN.at[i, 0, 0], dev(z=zp))
        zfar[i, 1].wait()
        ZS[i, 2, 1] = (Z[i, zm, 1] + ZF[i, 1].astype(F32)).astype(BF16)
        znear[i, 1, 1] = copy(ZS.at[i, 2, 1], ZN.at[i, 1, 1], dev(z=zm))

    def wsum_end(i):
        for side in range(2):
            for half in range(2):
                znear[i, side, half].wait()
        return [
            (Z[i, z, half] + ZN[i, 0, half].astype(F32) + ZN[i, 1, half].astype(F32)) * factor
            for half in range(2)
        ]

    def input_term(pair, k):
        total = None
        for kind in range(2):
            left = jnp.concatenate([delta_pair(kind, pair, 0), delta_pair(kind, pair, 1)], axis=1)
            right = jnp.concatenate([WG[kind, k, b] for b in range(4)], axis=1)
            term = nt(left, right)
            total = term if total is None else total + term
        return total

    def delta_pair(kind, pair, l_to):
        return delta(kind, l_to, pair)

    xfar, xnear = {}, {}

    def isum_start():
        xfar[0] = copy(X.at[xf, 0], XF.at[0], dev(x=xp))
        xfar[1] = copy(X.at[xf, 1], XF.at[1], dev(x=xm))
        xnear[0, 1] = copy(X.at[xp, 1], XN.at[0, 1], dev(x=xp))
        xnear[1, 0] = copy(X.at[xm, 0], XN.at[1, 0], dev(x=xm))

    def isum_middle():
        xfar[0].wait()
        X[xp, 0] += XF[0]
        xnear[0, 0] = copy(X.at[xp, 0], XN.at[0, 0], dev(x=xp))
        xfar[1].wait()
        X[xm, 1] += XF[1]
        xnear[1, 1] = copy(X.at[xm, 1], XN.at[1, 1], dev(x=xm))

    grads_of_weights(0)
    wsum_start(0)
    for pair in range(2):
        for k in range(2):
            term = input_term(pair, k)
            X[2 * pair, k] = term[:128]
            X[2 * pair + 1, k] = term[128:]
    isum_start()
    grads_of_weights(1)
    wsum_start(1)
    grads_of_weights(2)
    wsum_start(2)
    wsum_middle(0)
    isum_middle()
    wsum_middle(1)
    wsum_middle(2)

    back = {}
    for side in range(2):
        for half in range(2):
            xnear[side, half].wait()
    for k in range(2):
        IB[k] = (X[x, k] + XN[0, k] + XN[1, k]).astype(BF16)
    for other in range(2):
        k = ll if other else l
        for e in range(4):
            to_y = turn(x, -e)
            back[other, e] = copy(
                IB.at[k, pl.ds(pl.multiple_of(to_y * 32, 32), 32), :],
                ig_ref.at[pl.ds(pl.multiple_of(l * 128 + x * 32, 32), 32), :],
                dev(x=y, y=to_y, z=zo if other else z),
                diagonal if e == 0 and not other else None,
            )

    last = []
    half_at = pl.multiple_of(c * 512, 512)
    for i in range(2):
        out = (gg_ref, ug_ref)[i]
        done = wsum_end(i)
        for half in range(2):
            low, high = done[half][:, :128], done[half][:, 128:]
            SX[i, pl.ds(half * 256, 256), :] = jnp.where(c == 0, high, low)
            S[i, pl.ds(half * 256, 256), :] = jnp.where(c == 0, low, high)
        rows = pl.ds(half_at, 512)
        last.append(copy(SX.at[i], out.at[rows, :], twin))
        out[rows, :] = S[i]
    done = wsum_end(2)
    blocks = [jnp.concatenate([part[:128], part[128:]], axis=1) for part in done]
    columns = pl.ds(half_at, 512)
    SD[...] = jnp.where(c == 0, blocks[1], blocks[0])
    last.append(copy(SD, dg_ref.at[:, columns], twin))
    dg_ref[:, columns] = jnp.where(c == 0, blocks[0], blocks[1])
    for made in [*last, *back.values()]:
        made.wait()
    for made in sent:
        made.sent()


def solution(mesh):
    def shards(tokens, out_grad, gate_weight, up_weight, down_weight):
        factor = 1.0 / math.sqrt(tokens.shape[0] * mesh.shape["fsdp"])
        vmem = pl.BlockSpec(memory_space=pltpu.VMEM)
        return pl.pallas_call(
            functools.partial(kernel, factor),
            out_shape=(
                jax.ShapeDtypeStruct((256, 512), BF16),
                jax.ShapeDtypeStruct((1024, 128), F32),
                jax.ShapeDtypeStruct((1024, 128), F32),
                jax.ShapeDtypeStruct((128, 1024), F32),
            ),
            in_specs=[vmem] * 5,
            out_specs=(vmem,) * 4,
            scratch_shapes=[
                pltpu.VMEM((2, 2, 4, 128, 512), BF16),
                pltpu.VMEM((2, 2, 4, 512, 128), BF16),
                pltpu.VMEM((2, 4, 128, 512), BF16),
                pltpu.VMEM((3, 4, 2, 64, 256), F32),
                pltpu.VMEM((3, 4, 2, 64, 256), F32),
                pltpu.VMEM((3, 4, 2, 64, 256), F32),
                pltpu.VMEM((3, 2, 64, 256), F32),
                pltpu.VMEM((3, 2, 2, 64, 256), F32),
                pltpu.VMEM((2, 4, 3, 2, 64, 256), BF16),
                pltpu.VMEM((4, 2, 128, 512), F32),
                pltpu.VMEM((2, 128, 512), F32),
                pltpu.VMEM((2, 2, 128, 512), F32),
                pltpu.VMEM((2, 128, 512), BF16),
                pltpu.VMEM((3, 4, 2, 256, 256), F32),
                pltpu.VMEM((3, 3, 2, 256, 256), BF16),
                pltpu.VMEM((3, 2, 256, 256), BF16),
                pltpu.VMEM((3, 2, 2, 256, 256), BF16),
                pltpu.VMEM((2, 512, 128), F32),
                pltpu.VMEM((2, 512, 128), F32),
                pltpu.VMEM((128, 512), F32),
                pltpu.SemaphoreType.DMA((COPIES,)),
                pltpu.SemaphoreType.DMA((COPIES,)),
                pltpu.SemaphoreType.DMA((3,)),
            ],
            compiler_params=pltpu.CompilerParams(
                collective_id=0, has_side_effects=True, vmem_limit_bytes=60 * 1024 * 1024
            ),
        )(tokens, out_grad, gate_weight, up_weight, down_weight)

    return jax.shard_map(
        shards,
        mesh=mesh,
        in_specs=(P("fsdp", "tp"),) * 4 + (P("tp", "fsdp"),),
        out_specs=(P("fsdp", "tp"),) * 3 + (P("tp", "fsdp"),),
        check_vma=False,
    )
```

```python
import functools
import math

import jax
import jax.numpy as jnp
from jax import lax
from jax.experimental import pallas as pl
from jax.experimental.pallas import tpu as pltpu
from jax.sharding import PartitionSpec as P

MESH = pl.DeviceIdType.MESH
F32, BF16 = jnp.float32, jnp.bfloat16
COPIES = 200


class Copy:
    def __init__(self, sems, src, dst, to, here=None):
        index = sems[2][0]
        sems[2][0] += 1
        send, recv = sems[0].at[index], sems[1].at[index]
        self.remote = pltpu.make_async_remote_copy(
            src_ref=src, dst_ref=dst, send_sem=send, recv_sem=recv, device_id=to, device_id_type=MESH
        )
        self.local = None if here is None else pltpu.make_async_copy(src, dst, recv)
        self.here = here
        self.done = False

    def start(self):
        if self.here is None:
            self.remote.start()
        else:
            pl.when(self.here)(self.local.start)
            pl.when(jnp.logical_not(self.here))(self.remote.start)
        return self

    def wait(self):
        if not self.done:
            self.remote.wait_recv()
        self.done = True

    def sent(self):
        if self.here is None:
            self.remote.wait_send()
        else:
            pl.when(jnp.logical_not(self.here))(self.remote.wait_send)


def nt(a, b):
    return lax.dot_general(a, b, (((1,), (1,)), ((), ())), preferred_element_type=F32)


def tn(a, b):
    return lax.dot_general(a, b, (((0,), (0,)), ((), ())), preferred_element_type=F32)


def nn(a, b):
    return jnp.dot(a, b, preferred_element_type=F32)


def kernel(
    factor,
    tok_ref, grd_ref, gate_ref, up_ref, down_ref,
    ig_ref, gg_ref, ug_ref, dg_ref,
    TV, WV, WDV, G, GT, WG, WD, PS, DR, RF, RN, GU, DL, X, XF, XN, IB,
    Z, ZS, ZF, ZN, S, SX, SD,
    send, recv, local_sem, load_sem,
):
    f, t = lax.axis_index("fsdp"), lax.axis_index("tp")
    h, y = lax.div(f, 4), lax.rem(f, 4)
    c = lax.rem(t, 2)
    x = lax.rem(lax.div(t, 2), 4)
    l = lax.div(t, 8)
    z = 2 * h + l
    sems = (send, recv, [0])
    sent = []

    def dev(x=x, y=y, z=z, c=c):
        return (lax.div(z, 2) * 4 + y, (lax.rem(z, 2) * 4 + x) * 2 + c)

    def copy(src, dst, to, here=None):
        made = Copy(sems, src, dst, to, here)
        sent.append(made)
        return made.start()

    def turn(v, k):
        return lax.rem(v + k + 4, 4)

    xp, xm, yp, ym, zp, zm = (turn(v, k) for v in (x, y, z) for k in (1, -1))
    yf, xf, zf = turn(y, 2), turn(x, 2), turn(z, 2)
    cc, ll = 1 - c, 1 - l
    zo = 2 * h + ll
    zn = turn(z, 2 * l - 1)
    diagonal = x == y
    twin = dev(c=cc)

    loads = [
        pltpu.make_async_copy(src, dst, load_sem.at[n])
        for n, (src, dst) in enumerate(
            [(tok_ref, TV.at[0]), (grd_ref, TV.at[1]), (gate_ref, WV.at[0]), (up_ref, WV.at[1]), (down_ref, WDV)]
        )
    ]
    for load in loads:
        load.start()

    barrier = pltpu.get_barrier_semaphore()
    peers = [
        twin, dev(x=xp), dev(x=xm), dev(y=yp), dev(y=ym),
        dev(z=zp), dev(z=zm), dev(z=zp, c=cc), dev(z=zm, c=cc),
    ]
    for e in range(4):
        there, back_there = dict(x=turn(y, e), y=x), dict(x=y, y=turn(x, -e))
        peers += [dev(z=zo, **there), dev(z=zo, **back_there)]
        if e > 0:
            peers += [dev(**there), dev(**back_there)]
    for peer in peers:
        pl.semaphore_signal(barrier, inc=1, device_id=peer, device_id_type=MESH)

    @pl.when(jnp.logical_not(diagonal))
    def _():
        pl.semaphore_signal(barrier, inc=2, device_id=dev(x=y, y=x), device_id_type=MESH)
        pl.semaphore_wait(barrier, len(peers) + 2)

    @pl.when(diagonal)
    def _():
        pl.semaphore_wait(barrier, len(peers))

    moved = {}

    def move(a):
        loads[a].wait()
        for other in (1, 0):
            to_l = ll if other else l
            for e in range(4):
                to_x = turn(y, e)
                moved[a, other, e] = copy(
                    TV.at[a, pl.ds(pl.multiple_of(to_l * 128 + to_x * 32, 32), 32), :],
                    G.at[a, l, e // 2, to_x, pl.ds(e % 2 * 32, 32), :],
                    dev(x=to_x, y=x, z=zo if other else z),
                    diagonal if e == 0 and not other else None,
                )

    def weight_piece(i, k):
        half = pl.multiple_of(k * 512, 512)
        if i < 2:
            return WV.at[i, pl.ds(half, 512), :]
        return WDV.at[:, pl.ds(half, 512)]

    def weight_slot(i, at_z, core):
        at_h, block = lax.div(at_z, 2), lax.rem(at_z, 2) * 2 + core
        return WG.at[i, at_h, block] if i < 2 else WD.at[at_h, block]

    own_weights, from_twin, wn, wo, far_w = {}, {}, {}, {}, {}
    cores = (c, cc)

    def send_weights(i):
        loads[2 + i].wait()
        slot = weight_slot(i, z, c)
        mine = pltpu.make_async_copy(weight_piece(i, c), slot, local_sem.at[i])
        mine.start()
        own_weights[i] = mine
        from_twin[i] = copy(weight_piece(i, cc), slot, twin)

    def send_weights_to(i, s, over_n):
        to_z, made = (zn, wn) if over_n else (zo, wo)
        made[i, s] = copy(weight_piece(i, cores[s]), weight_slot(i, z, c), dev(z=to_z, c=cores[s]))

    def pass_weights(i, s):
        over_n = s == 0 or i == 0
        arrived, at_z, to_z = (wo, zo, zn) if over_n else (wn, zn, zo)
        arrived[i, s].wait()
        slot = weight_slot(i, at_z, cores[s])
        far_w[i, s] = copy(slot, slot, dev(z=to_z))

    def weights_here(i, part):
        if part == 0:
            for s in range(2):
                wn[i, s].wait()
                wo[i, s].wait()
        else:
            own_weights[i].wait()
            from_twin[i].wait()
            far_w[i, 0].wait()
            far_w[i, 1].wait()

    gp, gm, far_g = {}, {}, {}

    def spread(a, other):
        for e in range(4):
            moved[a, other, e].wait()
        slot = G.at[a, ll if other else l, :, x]
        gp[a, other] = copy(slot, slot, dev(x=xp))
        gm[a, other] = copy(slot, slot, dev(x=xm))

    def pass_tokens(a):
        gp[a, 0].wait()
        slot = G.at[a, l, :, xm]
        far_g[a, 0] = copy(slot, slot, dev(x=xp))
        gm[a, 1].wait()
        slot = G.at[a, ll, :, xp]
        far_g[a, 1] = copy(slot, slot, dev(x=xm))

    def tokens_here(a):
        gp[a, 1].wait()
        gm[a, 0].wait()
        far_g[a, 0].wait()
        far_g[a, 1].wait()

    sides = (ll, l)

    def gathered(a, k):
        return G[a, k].reshape(512, 512)

    def multiply(unit):
        parts, arrays_of, chunks = unit
        for part in range(*parts):
            l_to = sides[part]
            for i in range(*arrays_of):
                a = min(i // 2, 1)
                total = None
                for k in range(2):
                    rows = gathered(a, k) if chunks == (0, 2) else G[a, k, chunks[0]].reshape(256, 512)
                    if i < 2:
                        right = jnp.concatenate([WG[i, k, 2 * l_to], WG[i, k, 2 * l_to + 1]], axis=1)
                        term = nn(rows, right)
                    else:
                        right = jnp.concatenate([WD[k, 2 * l_to], WD[k, 2 * l_to + 1]], axis=0)
                        term = nt(rows, right)
                    total = term if total is None else total + term
                for half in range(2):
                    block = total[:, half * 128 : half * 128 + 128]
                    PS[part, i, chunks[0] : chunks[1], :, :, half] = block.reshape(
                        chunks[1] - chunks[0], 2, 4, 32, 128
                    )
        to_twin[unit] = copy(at(PS, unit, cc), at(DR, unit), twin)

    to_twin, yfar, ynear = {}, {}, {}

    def at(ref, unit, *more):
        return ref.at[(*(pl.ds(first, end - first) for first, end in unit), *more)]

    def over_unit(unit):
        parts, arrays_of, chunks = unit
        return [(p, i, q) for p in range(*parts) for i in range(*arrays_of) for q in range(*chunks)]

    def sum_start(unit):
        to_twin[unit].wait()
        for u in over_unit(unit):
            PS[(*u, c)] += DR[u]
        yfar[unit, 0] = copy(at(PS, unit, c, yf, 0), at(RF, unit, 0), dev(y=yp))
        yfar[unit, 1] = copy(at(PS, unit, c, yf, 1), at(RF, unit, 1), dev(y=ym))
        ynear[unit, 0, 1] = copy(at(PS, unit, c, yp, 1), at(RN, unit, 0, 1), dev(y=yp))
        ynear[unit, 1, 0] = copy(at(PS, unit, c, ym, 0), at(RN, unit, 1, 0), dev(y=ym))

    def sum_middle(unit):
        yfar[unit, 0].wait()
        for u in over_unit(unit):
            PS[(*u, c, yp, 0)] += RF[(*u, 0)]
        ynear[unit, 0, 0] = copy(at(PS, unit, c, yp, 0), at(RN, unit, 0, 0), dev(y=yp))
        yfar[unit, 1].wait()
        for u in over_unit(unit):
            PS[(*u, c, ym, 1)] += RF[(*u, 1)]
        ynear[unit, 1, 1] = copy(at(PS, unit, c, ym, 1), at(RN, unit, 1, 1), dev(y=ym))

    def sum_arrived(unit):
        for side in range(2):
            for half in range(2):
                ynear[unit, side, half].wait()

    def sum_end(part, i, q):
        return PS[part, i, q, c, y] + RN[part, i, q, 0] + RN[part, i, q, 1]

    def make_hidden(unit):
        sum_arrived(unit)
        for part in range(*unit[0]):
            for q in range(2):
                gate, up = sum_end(part, 0, q), sum_end(part, 1, q)
                GU[part, 0, q] = gate
                GU[part, 1, q] = up
                DL[part, c, y, 2, q] = (gate * jax.nn.sigmoid(gate) * up).astype(BF16)

    def make_deltas(unit):
        sum_arrived(unit)
        for part, _, q in over_unit(unit):
            gate, up, hidden_grad = GU[part, 0, q], GU[part, 1, q], sum_end(part, 2, q)
            squashed = jax.nn.sigmoid(gate)
            activated = gate * squashed
            slope = squashed * (1.0 + gate * (1.0 - squashed))
            DL[part, c, y, 0, q] = (hidden_grad * up * slope).astype(BF16)
            DL[part, c, y, 1, q] = (hidden_grad * activated).astype(BF16)

    dp, dm, far_d, over = {}, {}, {}, {}

    def delta_at(group, at_y, *half):
        parts, kinds, chunks = (pl.ds(first, end - first) for first, end in group)
        return DL.at[(parts, c, at_y, kinds, chunks, *half)]

    def give(group):
        for half in range(2):
            part = delta_at(group, y, half)
            dp[group, half] = copy(part, part, dev(y=yp))
            part = delta_at(group, y, 1 - half)
            dm[group, 1 - half] = copy(part, part, dev(y=ym))
        over[group] = [copy(delta_at(group, y), delta_at(group, y), twin)]

    def give_on(group):
        dp[group, 0].wait()
        part = delta_at(group, ym, 0)
        far_d[group, 0] = copy(part, part, dev(y=yp))
        dm[group, 1].wait()
        part = delta_at(group, yp, 1)
        far_d[group, 1] = copy(part, part, dev(y=ym))
        dp[group, 1].wait()
        over[group].append(copy(delta_at(group, ym), delta_at(group, ym), twin))
        dm[group, 0].wait()
        over[group].append(copy(delta_at(group, yp), delta_at(group, yp), twin))

    def give_end(group):
        far_d[group, 0].wait()
        far_d[group, 1].wait()
        over[group].append(copy(delta_at(group, yf), delta_at(group, yf), twin))

    def given(group):
        for made in over[group]:
            made.wait()

    def delta(kind, part, q):
        return jnp.concatenate([DL[part, :, :, kind, q, half].reshape(256, 128) for half in range(2)], axis=1)

    def delta_all(kind, part):
        return jnp.concatenate([delta(kind, part, 0), delta(kind, part, 1)], axis=0)

    halves = (h, 1 - h)

    def grads_of_weights(i, part):
        for r in range(2):
            if i < 2:
                Z[i, 2 * part + r] = nn(GT[halves[r]], delta_all(i, part)).reshape(2, 256, 256)
            else:
                block = tn(delta_all(2, part), gathered(1, halves[r]))
                for j in range(2):
                    Z[2, 2 * part + r, j] = jnp.concatenate(
                        [block[j * 128 : j * 128 + 128, :256], block[j * 128 : j * 128 + 128, 256:]], axis=0
                    )

    zfar, znear = {}, {}

    def wsum_near(i):
        ZS[i, 0, 1] = Z[i, 0, 1].astype(BF16)
        znear[i, 0, 1] = copy(ZS.at[i, 0, 1], ZN.at[i, 0, 1], dev(z=zo))
        ZS[i, 1, 0] = Z[i, 1, 0].astype(BF16)
        znear[i, 1, 0] = copy(ZS.at[i, 1, 0], ZN.at[i, 1, 0], dev(z=zn))

    def wsum_far(i):
        ZS[i, 2] = Z[i, 3].astype(BF16)
        zfar[i, 0] = copy(ZS.at[i, 2, 0], ZF.at[i, 0], dev(z=zn))
        zfar[i, 1] = copy(ZS.at[i, 2, 1], ZF.at[i, 1], dev(z=zo))

    def wsum_middle(i):
        zfar[i, 0].wait()
        ZS[i, 0, 0] = (Z[i, 0, 0] + ZF[i, 0].astype(F32)).astype(BF16)
        znear[i, 0, 0] = copy(ZS.at[i, 0, 0], ZN.at[i, 0, 0], dev(z=zo))
        zfar[i, 1].wait()
        ZS[i, 1, 1] = (Z[i, 1, 1] + ZF[i, 1].astype(F32)).astype(BF16)
        znear[i, 1, 1] = copy(ZS.at[i, 1, 1], ZN.at[i, 1, 1], dev(z=zn))

    last = []
    half_at = pl.ds(pl.multiple_of(c * 512, 512), 512)

    def wsum_end(i):
        for side in range(2):
            for half in range(2):
                znear[i, side, half].wait()
        done = [
            (Z[i, 2, half] + ZN[i, 0, half].astype(F32) + ZN[i, 1, half].astype(F32)) * factor
            for half in range(2)
        ]
        if i < 2:
            out = (gg_ref, ug_ref)[i]
            for half in range(2):
                low, high = done[half][:, :128], done[half][:, 128:]
                SX[i, pl.ds(half * 256, 256), :] = jnp.where(c == 0, high, low)
                S[i, pl.ds(half * 256, 256), :] = jnp.where(c == 0, low, high)
            last.append(copy(SX.at[i], out.at[half_at, :], twin))
            out[half_at, :] = S[i]
        else:
            blocks = [jnp.concatenate([part[:128], part[128:]], axis=1) for part in done]
            SD[...] = jnp.where(c == 0, blocks[1], blocks[0])
            last.append(copy(SD, dg_ref.at[:, half_at], twin))
            dg_ref[:, half_at] = jnp.where(c == 0, blocks[0], blocks[1])

    def input_rows(q):
        left = jnp.concatenate([delta(kind, part, q) for part in range(2) for kind in range(2)], axis=1)
        for k in range(2):
            right = jnp.concatenate(
                [WG[kind, k, 2 * sides[part] + b] for part in range(2) for kind in range(2) for b in range(2)], axis=1
            )
            X[q, :, k] = nt(left, right).reshape(4, 64, 512)

    xfar, xnear = {}, {}

    def isum_start(q):
        xfar[q, 0] = copy(X.at[q, xf, 0], XF.at[q, 0], dev(x=xp))
        xfar[q, 1] = copy(X.at[q, xf, 1], XF.at[q, 1], dev(x=xm))
        xnear[q, 0, 1] = copy(X.at[q, xp, 1], XN.at[q, 0, 1], dev(x=xp))
        xnear[q, 1, 0] = copy(X.at[q, xm, 0], XN.at[q, 1, 0], dev(x=xm))

    def isum_middle(q):
        xfar[q, 0].wait()
        X[q, xp, 0] += XF[q, 0]
        xnear[q, 0, 0] = copy(X.at[q, xp, 0], XN.at[q, 0, 0], dev(x=xp))
        xfar[q, 1].wait()
        X[q, xm, 1] += XF[q, 1]
        xnear[q, 1, 1] = copy(X.at[q, xm, 1], XN.at[q, 1, 1], dev(x=xm))

    def isum_end(q):
        for side in range(2):
            for half in range(2):
                xnear[q, side, half].wait()
        for k in range(2):
            IB[k, pl.ds(2 * q, 2)] = (X[q, x, k] + XN[q, 0, k] + XN[q, 1, k]).astype(BF16).reshape(2, 32, 512)

    back = {}

    def send_back(q):
        for other in (1, 0):
            for e in (2 * q, 2 * q + 1):
                back[other, e] = copy(
                    IB.at[ll if other else l, e],
                    ig_ref.at[pl.ds(pl.multiple_of(l * 128 + x * 32, 32), 32), :],
                    dev(x=y, y=turn(x, -e), z=zo if other else z),
                    diagonal if e == 0 and not other else None,
                )

    GATE_UP, HIDDEN = 0, 1
    both = (0, 2)
    gate_up = [((part, part + 1), both, both) for part in range(2)]
    down = [(both, (2, 3), (q, q + 1)) for q in range(2)]
    hidden = (both, (2, 3), both)
    deltas = [(both, both, (q, q + 1)) for q in range(2)]
    move(0)
    for i in range(3):
        send_weights(i)
        for s in range(2):
            send_weights_to(i, s, False)
            send_weights_to(i, s, True)
        if i == 0:
            move(1)
    spread(0, 0)
    spread(0, 1)
    spread(1, 0)
    pass_weights(0, 0)
    pass_tokens(0)
    spread(1, 1)
    pass_weights(0, 1)
    pass_weights(1, 1)
    pass_weights(1, 0)
    tokens_here(0)
    weights_here(0, 0)
    weights_here(1, 0)
    multiply(gate_up[0])
    pass_tokens(1)
    sum_start(gate_up[0])
    weights_here(0, 1)
    weights_here(1, 1)
    multiply(gate_up[1])
    pass_weights(2, 0)
    pass_weights(2, 1)
    sum_middle(gate_up[0])
    sum_start(gate_up[1])
    for k in range(2):
        GT[k] = gathered(0, k).T
    tokens_here(1)
    weights_here(2, 0)
    weights_here(2, 1)
    multiply(down[0])
    multiply(down[1])
    sum_middle(gate_up[1])
    make_hidden(gate_up[0])
    sum_start(down[0])
    sum_start(down[1])
    make_hidden(gate_up[1])
    give(hidden)
    sum_middle(down[0])
    sum_middle(down[1])
    give_on(hidden)
    make_deltas(down[0])
    give(deltas[0])
    make_deltas(down[1])
    give(deltas[1])
    give_end(hidden)
    given(hidden)
    grads_of_weights(2, 1)
    wsum_far(2)
    grads_of_weights(2, 0)
    wsum_near(2)
    give_on(deltas[0])
    give_on(deltas[1])
    give_end(deltas[0])
    give_end(deltas[1])
    given(deltas[0])
    input_rows(0)
    isum_start(0)
    wsum_middle(2)
    given(deltas[1])
    grads_of_weights(0, 1)
    wsum_far(0)
    grads_of_weights(0, 0)
    wsum_near(0)
    input_rows(1)
    isum_start(1)
    grads_of_weights(1, 1)
    wsum_far(1)
    grads_of_weights(1, 0)
    wsum_near(1)
    isum_middle(0)
    isum_middle(1)
    wsum_middle(0)
    wsum_middle(1)
    wsum_end(2)
    isum_end(0)
    send_back(0)
    isum_end(1)
    send_back(1)
    wsum_end(0)
    wsum_end(1)
    for made in [*last, *back.values()]:
        made.wait()
    for made in sent:
        assert made.done
        made.sent()


def put_out(a, b, c, d, a_out, b_out, c_out, d_out, sems):
    copies = [
        pltpu.make_async_copy(src, dst, sems.at[n])
        for n, (src, dst) in enumerate([(a, a_out), (b, b_out), (c, c_out), (d, d_out)])
    ]
    for made in copies:
        made.start()
    for made in copies:
        made.wait()


def solution(mesh):
    def shards(tokens, out_grad, gate_weight, up_weight, down_weight):
        factor = 1.0 / math.sqrt(tokens.shape[0] * mesh.shape["fsdp"])
        vmem = pl.BlockSpec(memory_space=pltpu.VMEM)
        made = pl.pallas_call(
            functools.partial(kernel, factor),
            out_shape=(
                pltpu.VMEM((256, 512), BF16),
                pltpu.VMEM((1024, 128), F32),
                pltpu.VMEM((1024, 128), F32),
                pltpu.VMEM((128, 1024), F32),
            ),
            in_specs=[pl.BlockSpec(memory_space=pl.ANY)] * 5,
            out_specs=(vmem,) * 4,
            scratch_shapes=[
                pltpu.VMEM((2, 256, 512), BF16),
                pltpu.VMEM((2, 1024, 128), BF16),
                pltpu.VMEM((128, 1024), BF16),
                pltpu.VMEM((2, 2, 2, 4, 64, 512), BF16),
                pltpu.VMEM((2, 512, 512), BF16),
                pltpu.VMEM((2, 2, 4, 512, 128), BF16),
                pltpu.VMEM((2, 4, 128, 512), BF16),
                pltpu.VMEM((2, 3, 2, 2, 4, 2, 32, 128), F32),
                pltpu.VMEM((2, 3, 2, 4, 2, 32, 128), F32),
                pltpu.VMEM((2, 3, 2, 2, 32, 128), F32),
                pltpu.VMEM((2, 3, 2, 2, 2, 32, 128), F32),
                pltpu.VMEM((2, 2, 2, 2, 32, 128), F32),
                pltpu.VMEM((2, 2, 4, 3, 2, 2, 32, 128), BF16),
                pltpu.VMEM((2, 4, 2, 64, 512), F32),
                pltpu.VMEM((2, 2, 64, 512), F32),
                pltpu.VMEM((2, 2, 2, 64, 512), F32),
                pltpu.VMEM((2, 4, 32, 512), BF16),
                pltpu.VMEM((3, 4, 2, 256, 256), F32),
                pltpu.VMEM((3, 3, 2, 256, 256), BF16),
                pltpu.VMEM((3, 2, 256, 256), BF16),
                pltpu.VMEM((3, 2, 2, 256, 256), BF16),
                pltpu.VMEM((2, 512, 128), F32),
                pltpu.VMEM((2, 512, 128), F32),
                pltpu.VMEM((128, 512), F32),
                pltpu.SemaphoreType.DMA((COPIES,)),
                pltpu.SemaphoreType.DMA((COPIES,)),
                pltpu.SemaphoreType.DMA((3,)),
                pltpu.SemaphoreType.DMA((5,)),
            ],
            compiler_params=pltpu.CompilerParams(
                collective_id=0, has_side_effects=True, vmem_limit_bytes=60 * 1024 * 1024
            ),
        )(tokens, out_grad, gate_weight, up_weight, down_weight)
        return pl.pallas_call(
            put_out,
            out_shape=tuple(jax.ShapeDtypeStruct(part.shape, part.dtype) for part in made),
            in_specs=[vmem] * 4,
            out_specs=(pl.BlockSpec(memory_space=pl.ANY),) * 4,
            scratch_shapes=[pltpu.SemaphoreType.DMA((4,))],
        )(*(pltpu.with_memory_space_constraint(part, pltpu.VMEM) for part in made))

    return jax.shard_map(
        shards,
        mesh=mesh,
        in_specs=(P("fsdp", "tp"),) * 4 + (P("tp", "fsdp"),),
        out_specs=(P("fsdp", "tp"),) * 3 + (P("tp", "fsdp"),),
        check_vma=False,
    )
```

```python
import functools
import math

import jax
import jax.numpy as jnp
from jax import lax
from jax.experimental import pallas as pl
from jax.experimental.pallas import tpu as pltpu
from jax.sharding import PartitionSpec as P

MESH = pl.DeviceIdType.MESH
F32, BF16 = jnp.float32, jnp.bfloat16
COPIES = 180


class Copy:
    def __init__(self, sems, src, dst, to, here=None, index=None):
        if index is None:
            index = sems[2][0]
            sems[2][0] += 1
        send, recv = sems[0].at[index], sems[1].at[index]
        self.remote = pltpu.make_async_remote_copy(
            src_ref=src, dst_ref=dst, send_sem=send, recv_sem=recv, device_id=to, device_id_type=MESH
        )
        self.local = None if here is None else pltpu.make_async_copy(src, dst, recv)
        self.here = here
        self.done = False

    def start(self):
        if self.here is None:
            self.remote.start()
        else:
            pl.when(self.here)(self.local.start)
            pl.when(jnp.logical_not(self.here))(self.remote.start)
        return self

    def wait(self):
        if not self.done:
            self.remote.wait_recv()
        self.done = True

    def sent(self):
        if self.here is None:
            self.remote.wait_send()
        else:
            pl.when(jnp.logical_not(self.here))(self.remote.wait_send)


def nt(a, b):
    return lax.dot_general(a, b, (((1,), (1,)), ((), ())), preferred_element_type=F32)


def tn(a, b):
    return lax.dot_general(a, b, (((0,), (0,)), ((), ())), preferred_element_type=F32)


def nn(a, b):
    return jnp.dot(a, b, preferred_element_type=F32)


def kernel(
    factor,
    tok_ref, grd_ref, gate_ref, up_ref, down_ref,
    ig_ref, gg_ref, ug_ref, dg_ref,
    TV, WV, WDV, G, GT, WG, WD, PS, DR, RF, RN, GU, DL, X, XF, XN, IB, BB,
    Z, ZS, ZF, ZN, S, SX, SD,
    send, recv, local_sem, load_sem,
):
    f, t = lax.axis_index("fsdp"), lax.axis_index("tp")
    h, y = lax.div(f, 4), lax.rem(f, 4)
    c = lax.rem(t, 2)
    x = lax.rem(lax.div(t, 2), 4)
    l = lax.div(t, 8)
    z = 2 * h + l
    sems = (send, recv, [0])
    sent = []

    def dev(x=x, y=y, z=z, c=c):
        return (lax.div(z, 2) * 4 + y, (lax.rem(z, 2) * 4 + x) * 2 + c)

    def copy(src, dst, to, here=None, index=None):
        made = Copy(sems, src, dst, to, here, index)
        sent.append(made)
        return made.start()

    def turn(v, k):
        return lax.rem(v + k + 4, 4)

    xp, xm, yp, ym, zp, zm = (turn(v, k) for v in (x, y, z) for k in (1, -1))
    yf, xf, zf = turn(y, 2), turn(x, 2), turn(z, 2)
    cc, ll = 1 - c, 1 - l
    zo = 2 * h + ll
    zn = turn(z, 2 * l - 1)
    diagonal = x == y
    twin = dev(c=cc)

    loads = [
        pltpu.make_async_copy(src, dst, load_sem.at[n])
        for n, (src, dst) in enumerate(
            [(tok_ref, TV.at[0]), (grd_ref, TV.at[1]), (gate_ref, WV.at[0]), (up_ref, WV.at[1]), (down_ref, WDV)]
        )
    ]
    for load in loads:
        load.start()

    barrier = pltpu.get_barrier_semaphore()
    peers = [
        twin, dev(x=xp), dev(x=xm), dev(y=yp), dev(y=ym),
        dev(z=zp), dev(z=zm), dev(z=zp, c=cc), dev(z=zm, c=cc),
    ]
    for e in range(4):
        there, back_there = dict(x=turn(y, e), y=x), dict(x=y, y=turn(x, -e))
        peers += [dev(z=zo, **there), dev(z=zo, **back_there)]
        if e > 0:
            peers += [dev(**there), dev(**back_there)]
    for peer in peers:
        pl.semaphore_signal(barrier, inc=1, device_id=peer, device_id_type=MESH)

    @pl.when(jnp.logical_not(diagonal))
    def _():
        pl.semaphore_signal(barrier, inc=2, device_id=dev(x=y, y=x), device_id_type=MESH)
        pl.semaphore_wait(barrier, len(peers) + 2)

    @pl.when(diagonal)
    def _():
        pl.semaphore_wait(barrier, len(peers))

    moved = {}

    def move(a):
        loads[a].wait()
        for other in (1, 0):
            to_l = ll if other else l
            for e in range(4):
                to_x = turn(y, e)
                moved[a, other, e] = copy(
                    TV.at[a, pl.ds(pl.multiple_of(to_l * 128 + to_x * 32, 32), 32), :],
                    G.at[a, l, e // 2, to_x, pl.ds(e % 2 * 32, 32), :],
                    dev(x=to_x, y=x, z=zo if other else z),
                    diagonal if e == 0 and not other else None,
                )

    def weight_piece(i, k):
        half = pl.multiple_of(k * 512, 512)
        if i < 2:
            return WV.at[i, pl.ds(half, 512), :]
        return WDV.at[:, pl.ds(half, 512)]

    def weight_slot(i, at_z, core):
        at_h, block = lax.div(at_z, 2), lax.rem(at_z, 2) * 2 + core
        return WG.at[i, at_h, block] if i < 2 else WD.at[at_h, block]

    own_weights, from_twin, wn, wo, far_w = {}, {}, {}, {}, {}
    cores = (c, cc)

    def send_weights(i):
        loads[2 + i].wait()
        slot = weight_slot(i, z, c)
        mine = pltpu.make_async_copy(weight_piece(i, c), slot, local_sem.at[i])
        mine.start()
        own_weights[i] = mine
        from_twin[i] = copy(weight_piece(i, cc), slot, twin)

    def send_weights_to(i, s, over_n):
        to_z, made = (zn, wn) if over_n else (zo, wo)
        made[i, s] = copy(weight_piece(i, cores[s]), weight_slot(i, z, c), dev(z=to_z, c=cores[s]))

    def pass_weights(i, s):
        over_n = s == 0 or i == 0
        arrived, at_z, to_z = (wo, zo, zn) if over_n else (wn, zn, zo)
        arrived[i, s].wait()
        slot = weight_slot(i, at_z, cores[s])
        far_w[i, s] = copy(slot, slot, dev(z=to_z))

    def weights_here(i, part):
        if part == 0:
            for s in range(2):
                wn[i, s].wait()
                wo[i, s].wait()
        else:
            own_weights[i].wait()
            from_twin[i].wait()
            far_w[i, 0].wait()
            far_w[i, 1].wait()

    gp, gm, far_g = {}, {}, {}

    def spread(a, other):
        for e in range(4):
            moved[a, other, e].wait()
        slot = G.at[a, ll if other else l, :, x]
        gp[a, other] = copy(slot, slot, dev(x=xp))
        gm[a, other] = copy(slot, slot, dev(x=xm))

    def pass_tokens(a, side):
        if side == 0:
            gp[a, 0].wait()
            slot = G.at[a, l, :, xm]
            far_g[a, 0] = copy(slot, slot, dev(x=xp))
        else:
            gm[a, 1].wait()
            slot = G.at[a, ll, :, xp]
            far_g[a, 1] = copy(slot, slot, dev(x=xm))

    def tokens_here(a):
        gp[a, 1].wait()
        gm[a, 0].wait()
        far_g[a, 0].wait()
        far_g[a, 1].wait()

    sides = (ll, l)

    def gathered(a, k):
        return G[a, k].reshape(512, 512)

    def multiply(unit):
        parts, arrays_of, chunks = unit
        for part in range(*parts):
            l_to = sides[part]
            for i in range(*arrays_of):
                a = min(i // 2, 1)
                total = None
                for k in range(2):
                    rows = gathered(a, k) if chunks == (0, 2) else G[a, k, chunks[0]].reshape(256, 512)
                    if i < 2:
                        right = jnp.concatenate([WG[i, k, 2 * l_to], WG[i, k, 2 * l_to + 1]], axis=1)
                        term = nn(rows, right)
                    else:
                        right = jnp.concatenate([WD[k, 2 * l_to], WD[k, 2 * l_to + 1]], axis=0)
                        term = nt(rows, right)
                    total = term if total is None else total + term
                for half in range(2):
                    block = total[:, half * 128 : half * 128 + 128]
                    PS[part, i, chunks[0] : chunks[1], :, :, half] = block.reshape(
                        chunks[1] - chunks[0], 2, 4, 32, 128
                    )
        to_twin[unit] = copy(at(PS, unit, cc), at(DR, unit), twin)

    to_twin, yfar, ynear = {}, {}, {}

    def at(ref, unit, *more):
        return ref.at[(*(pl.ds(first, end - first) for first, end in unit), *more)]

    def over_unit(unit):
        parts, arrays_of, chunks = unit
        return [(p, i, q) for p in range(*parts) for i in range(*arrays_of) for q in range(*chunks)]

    def sum_start(unit):
        to_twin[unit].wait()
        for u in over_unit(unit):
            PS[(*u, c)] += DR[u]
        yfar[unit, 0] = copy(at(PS, unit, c, yf, 0), at(RF, unit, 0), dev(y=yp))
        yfar[unit, 1] = copy(at(PS, unit, c, yf, 1), at(RF, unit, 1), dev(y=ym))
        ynear[unit, 0, 1] = copy(at(PS, unit, c, yp, 1), at(RN, unit, 0, 1), dev(y=yp))
        ynear[unit, 1, 0] = copy(at(PS, unit, c, ym, 0), at(RN, unit, 1, 0), dev(y=ym))

    def sum_middle(unit):
        yfar[unit, 0].wait()
        for u in over_unit(unit):
            PS[(*u, c, yp, 0)] += RF[(*u, 0)]
        ynear[unit, 0, 0] = copy(at(PS, unit, c, yp, 0), at(RN, unit, 0, 0), dev(y=yp))
        yfar[unit, 1].wait()
        for u in over_unit(unit):
            PS[(*u, c, ym, 1)] += RF[(*u, 1)]
        ynear[unit, 1, 1] = copy(at(PS, unit, c, ym, 1), at(RN, unit, 1, 1), dev(y=ym))

    def sum_arrived(unit):
        for side in range(2):
            for half in range(2):
                ynear[unit, side, half].wait()

    def sum_end(part, i, q):
        return PS[part, i, q, c, y] + RN[part, i, q, 0] + RN[part, i, q, 1]

    def make_hidden(unit):
        sum_arrived(unit)
        for part in range(*unit[0]):
            for q in range(2):
                gate, up = sum_end(part, 0, q), sum_end(part, 1, q)
                GU[part, 0, q] = gate
                GU[part, 1, q] = up
                DL[part, c, y, 2, q] = (gate * jax.nn.sigmoid(gate) * up).astype(BF16)

    def make_deltas(unit):
        sum_arrived(unit)
        for part, _, q in over_unit(unit):
            gate, up, hidden_grad = GU[part, 0, q], GU[part, 1, q], sum_end(part, 2, q)
            squashed = jax.nn.sigmoid(gate)
            activated = gate * squashed
            slope = squashed * (1.0 + gate * (1.0 - squashed))
            DL[part, c, y, 0, q] = (hidden_grad * up * slope).astype(BF16)
            DL[part, c, y, 1, q] = (hidden_grad * activated).astype(BF16)

    dp, dm, far_d, over = {}, {}, {}, {}

    def delta_at(group, at_y, *half):
        parts, kinds, chunks = (pl.ds(first, end - first) for first, end in group)
        return DL.at[(parts, c, at_y, kinds, chunks, *half)]

    def give(group):
        for half in range(2):
            part = delta_at(group, y, half)
            dp[group, half] = copy(part, part, dev(y=yp))
            part = delta_at(group, y, 1 - half)
            dm[group, 1 - half] = copy(part, part, dev(y=ym))
        over[group] = [copy(delta_at(group, y), delta_at(group, y), twin)]

    def give_on(group):
        dp[group, 0].wait()
        part = delta_at(group, ym, 0)
        far_d[group, 0] = copy(part, part, dev(y=yp))
        dm[group, 1].wait()
        part = delta_at(group, yp, 1)
        far_d[group, 1] = copy(part, part, dev(y=ym))

    def give_over(group):
        dp[group, 1].wait()
        over[group].append(copy(delta_at(group, ym), delta_at(group, ym), twin))
        dm[group, 0].wait()
        over[group].append(copy(delta_at(group, yp), delta_at(group, yp), twin))

    def give_end(group):
        far_d[group, 0].wait()
        far_d[group, 1].wait()
        over[group].append(copy(delta_at(group, yf), delta_at(group, yf), twin))

    def given(group):
        for made in over[group]:
            made.wait()

    def delta(kind, part, q):
        return jnp.concatenate([DL[part, :, :, kind, q, half].reshape(256, 128) for half in range(2)], axis=1)

    def delta_all(kind, part):
        return jnp.concatenate([delta(kind, part, 0), delta(kind, part, 1)], axis=0)

    halves = (h, 1 - h)

    def grads_of_weights(i, part):
        for r in range(2):
            if i < 2:
                Z[i, 2 * part + r] = nn(GT[halves[r]], delta_all(i, part)).reshape(2, 256, 256)
            else:
                block = tn(delta_all(2, part), gathered(1, halves[r]))
                for j in range(2):
                    Z[2, 2 * part + r, j] = jnp.concatenate(
                        [block[j * 128 : j * 128 + 128, :256], block[j * 128 : j * 128 + 128, 256:]], axis=0
                    )

    zfar, znear = {}, {}

    def wsum_near(i):
        ZS[i, 0, 1] = Z[i, 0, 1].astype(BF16)
        znear[i, 0, 1] = copy(ZS.at[i, 0, 1], ZN.at[i, 0, 1], dev(z=zo))
        ZS[i, 1, 0] = Z[i, 1, 0].astype(BF16)
        znear[i, 1, 0] = copy(ZS.at[i, 1, 0], ZN.at[i, 1, 0], dev(z=zn))

    def wsum_far(i):
        ZS[i, 2] = Z[i, 3].astype(BF16)
        zfar[i, 0] = copy(ZS.at[i, 2, 0], ZF.at[i, 0], dev(z=zn))
        zfar[i, 1] = copy(ZS.at[i, 2, 1], ZF.at[i, 1], dev(z=zo))

    def wsum_middle(i):
        zfar[i, 0].wait()
        ZS[i, 0, 0] = (Z[i, 0, 0] + ZF[i, 0].astype(F32)).astype(BF16)
        znear[i, 0, 0] = copy(ZS.at[i, 0, 0], ZN.at[i, 0, 0], dev(z=zo))
        zfar[i, 1].wait()
        ZS[i, 1, 1] = (Z[i, 1, 1] + ZF[i, 1].astype(F32)).astype(BF16)
        znear[i, 1, 1] = copy(ZS.at[i, 1, 1], ZN.at[i, 1, 1], dev(z=zn))

    last = []
    half_at = pl.ds(pl.multiple_of(c * 512, 512), 512)

    def wsum_end(i):
        for side in range(2):
            for half in range(2):
                znear[i, side, half].wait()
        done = [
            (Z[i, 2, half] + ZN[i, 0, half].astype(F32) + ZN[i, 1, half].astype(F32)) * factor
            for half in range(2)
        ]
        if i < 2:
            out = (gg_ref, ug_ref)[i]
            for half in range(2):
                low, high = done[half][:, :128], done[half][:, 128:]
                SX[i, pl.ds(half * 256, 256), :] = jnp.where(c == 0, high, low)
                S[i, pl.ds(half * 256, 256), :] = jnp.where(c == 0, low, high)
            last.append(copy(SX.at[i], out.at[half_at, :], twin))
            out[half_at, :] = S[i]
        else:
            blocks = [jnp.concatenate([part[:128], part[128:]], axis=1) for part in done]
            SD[...] = jnp.where(c == 0, blocks[1], blocks[0])
            last.append(copy(SD, dg_ref.at[:, half_at], twin))
            dg_ref[:, half_at] = jnp.where(c == 0, blocks[0], blocks[1])

    def input_rows(q):
        left = jnp.concatenate([delta(kind, part, q) for part in range(2) for kind in range(2)], axis=1)
        for k in range(2):
            right = jnp.concatenate(
                [WG[kind, k, 2 * sides[part] + b] for part in range(2) for kind in range(2) for b in range(2)], axis=1
            )
            X[q, :, k] = nt(left, right).reshape(4, 64, 512)

    xfar, xnear = {}, {}

    def isum_start(q):
        xfar[q, 0] = copy(X.at[q, xf, 0], XF.at[q, 0], dev(x=xp))
        xfar[q, 1] = copy(X.at[q, xf, 1], XF.at[q, 1], dev(x=xm))
        xnear[q, 0, 1] = copy(X.at[q, xp, 1], XN.at[q, 0, 1], dev(x=xp))
        xnear[q, 1, 0] = copy(X.at[q, xm, 0], XN.at[q, 1, 0], dev(x=xm))

    def isum_middle(q):
        xfar[q, 0].wait()
        X[q, xp, 0] += XF[q, 0]
        xnear[q, 0, 0] = copy(X.at[q, xp, 0], XN.at[q, 0, 0], dev(x=xp))
        xfar[q, 1].wait()
        X[q, xm, 1] += XF[q, 1]
        xnear[q, 1, 1] = copy(X.at[q, xm, 1], XN.at[q, 1, 1], dev(x=xm))

    def isum_end(q):
        for side in range(2):
            for half in range(2):
                xnear[q, side, half].wait()
        for k in range(2):
            IB[pl.ds(2 * q, 2), k] = (X[q, x, k] + XN[q, 0, k] + XN[q, 1, k]).astype(BF16).reshape(2, 32, 512)

    FIRST, SECOND = COPIES, COPIES + 4

    def arrives(index, ref):
        return pltpu.make_async_copy(ref, ref, recv.at[index])

    def send_back(q):
        for e in (2 * q, 2 * q + 1):
            far = turn(y - x, e)
            copy_back(IB.at[e], BB.at[far], dev(y=turn(x, -e)), far == 0, FIRST + far)

    def copy_back(src, dst, to, here, index):
        made = Copy(sems, src, dst, to, here, index)
        made.done = True
        sent.append(made.start())

    def pass_back():
        for d in range(4):
            arrives(FIRST + d, BB.at[d]).wait()
            to_x = turn(y, d)
            far = turn(to_x - x, 0)
            for other in (1, 0):
                copy_back(
                    BB.at[d, ll if other else l],
                    ig_ref.at[pl.ds(pl.multiple_of(l * 128 + x * 32, 32), 32), :],
                    dev(x=to_x, z=zo if other else z),
                    None if other else far == 0,
                    SECOND + 2 * far + other,
                )

    def back_here():
        for n in range(8):
            arrives(SECOND + n, ig_ref.at[pl.ds(0, 32), :]).wait()

    GATE_UP, HIDDEN = 0, 1
    both = (0, 2)
    gate_up = [((part, part + 1), both, both) for part in range(2)]
    down = [(both, (2, 3), (q, q + 1)) for q in range(2)]
    hidden = [((part, part + 1), (2, 3), both) for part in range(2)]
    deltas = [(both, both, (q, q + 1)) for q in range(2)]
    move(0)
    for i in range(2):
        send_weights(i)
        for s in range(2):
            send_weights_to(i, s, False)
            send_weights_to(i, s, True)
        if i == 0:
            move(1)
    send_weights(2)
    send_weights_to(2, 0, True)
    spread(0, 0)
    spread(0, 1)
    pass_weights(0, 0)
    pass_tokens(0, 0)
    pass_tokens(0, 1)
    spread(1, 0)
    spread(1, 1)
    pass_weights(0, 1)
    pass_weights(1, 1)
    send_weights_to(2, 0, False)
    pass_weights(1, 0)
    send_weights_to(2, 1, True)
    send_weights_to(2, 1, False)
    tokens_here(0)
    weights_here(0, 0)
    weights_here(1, 0)
    multiply(gate_up[0])
    sum_start(gate_up[0])
    pass_tokens(1, 0)
    pass_tokens(1, 1)
    weights_here(0, 1)
    weights_here(1, 1)
    multiply(gate_up[1])
    sum_middle(gate_up[0])
    pass_weights(2, 0)
    sum_start(gate_up[1])
    pass_weights(2, 1)
    for k in range(2):
        GT[k] = gathered(0, k).T
    make_hidden(gate_up[0])
    give(hidden[0])
    sum_middle(gate_up[1])
    tokens_here(1)
    weights_here(2, 0)
    weights_here(2, 1)
    multiply(down[0])
    multiply(down[1])
    give_on(hidden[0])
    give_over(hidden[0])
    sum_start(down[0])
    sum_start(down[1])
    make_hidden(gate_up[1])
    give(hidden[1])
    give_end(hidden[0])
    sum_middle(down[0])
    sum_middle(down[1])
    given(hidden[0])
    grads_of_weights(2, 0)
    wsum_near(2)
    give_on(hidden[1])
    give_over(hidden[1])
    make_deltas(down[0])
    give(deltas[0])
    make_deltas(down[1])
    give(deltas[1])
    give_end(hidden[1])
    given(hidden[1])
    grads_of_weights(2, 1)
    wsum_far(2)
    give_on(deltas[0])
    give_over(deltas[0])
    give_on(deltas[1])
    give_over(deltas[1])
    give_end(deltas[0])
    give_end(deltas[1])
    given(deltas[0])
    input_rows(0)
    isum_start(0)
    given(deltas[1])
    grads_of_weights(0, 1)
    wsum_far(0)
    grads_of_weights(0, 0)
    wsum_near(0)
    wsum_middle(2)
    input_rows(1)
    isum_start(1)
    grads_of_weights(1, 1)
    wsum_far(1)
    grads_of_weights(1, 0)
    wsum_near(1)
    isum_middle(0)
    isum_middle(1)
    wsum_middle(0)
    isum_end(0)
    send_back(0)
    wsum_middle(1)
    isum_end(1)
    send_back(1)
    wsum_end(2)
    pass_back()
    wsum_end(0)
    wsum_end(1)
    back_here()
    for made in last:
        made.wait()
    for made in sent:
        assert made.done and sems[2][0] <= COPIES
        made.sent()


def put_out(a, b, c, d, a_out, b_out, c_out, d_out, sems):
    copies = [
        pltpu.make_async_copy(src, dst, sems.at[n])
        for n, (src, dst) in enumerate([(a, a_out), (b, b_out), (c, c_out), (d, d_out)])
    ]
    for made in copies:
        made.start()
    for made in copies:
        made.wait()


def solution(mesh):
    def shards(tokens, out_grad, gate_weight, up_weight, down_weight):
        factor = 1.0 / math.sqrt(tokens.shape[0] * mesh.shape["fsdp"])
        vmem = pl.BlockSpec(memory_space=pltpu.VMEM)
        made = pl.pallas_call(
            functools.partial(kernel, factor),
            out_shape=(
                pltpu.VMEM((256, 512), BF16),
                pltpu.VMEM((1024, 128), F32),
                pltpu.VMEM((1024, 128), F32),
                pltpu.VMEM((128, 1024), F32),
            ),
            in_specs=[pl.BlockSpec(memory_space=pl.ANY)] * 5,
            out_specs=(vmem,) * 4,
            scratch_shapes=[
                pltpu.VMEM((2, 256, 512), BF16),
                pltpu.VMEM((2, 1024, 128), BF16),
                pltpu.VMEM((128, 1024), BF16),
                pltpu.VMEM((2, 2, 2, 4, 64, 512), BF16),
                pltpu.VMEM((2, 512, 512), BF16),
                pltpu.VMEM((2, 2, 4, 512, 128), BF16),
                pltpu.VMEM((2, 4, 128, 512), BF16),
                pltpu.VMEM((2, 3, 2, 2, 4, 2, 32, 128), F32),
                pltpu.VMEM((2, 3, 2, 4, 2, 32, 128), F32),
                pltpu.VMEM((2, 3, 2, 2, 32, 128), F32),
                pltpu.VMEM((2, 3, 2, 2, 2, 32, 128), F32),
                pltpu.VMEM((2, 2, 2, 2, 32, 128), F32),
                pltpu.VMEM((2, 2, 4, 3, 2, 2, 32, 128), BF16),
                pltpu.VMEM((2, 4, 2, 64, 512), F32),
                pltpu.VMEM((2, 2, 64, 512), F32),
                pltpu.VMEM((2, 2, 2, 64, 512), F32),
                pltpu.VMEM((4, 2, 32, 512), BF16),
                pltpu.VMEM((4, 2, 32, 512), BF16),
                pltpu.VMEM((3, 4, 2, 256, 256), F32),
                pltpu.VMEM((3, 3, 2, 256, 256), BF16),
                pltpu.VMEM((3, 2, 256, 256), BF16),
                pltpu.VMEM((3, 2, 2, 256, 256), BF16),
                pltpu.VMEM((2, 512, 128), F32),
                pltpu.VMEM((2, 512, 128), F32),
                pltpu.VMEM((128, 512), F32),
                pltpu.SemaphoreType.DMA((COPIES + 12,)),
                pltpu.SemaphoreType.DMA((COPIES + 12,)),
                pltpu.SemaphoreType.DMA((3,)),
                pltpu.SemaphoreType.DMA((5,)),
            ],
            compiler_params=pltpu.CompilerParams(
                collective_id=0, has_side_effects=True, vmem_limit_bytes=60 * 1024 * 1024
            ),
        )(tokens, out_grad, gate_weight, up_weight, down_weight)
        return pl.pallas_call(
            put_out,
            out_shape=tuple(jax.ShapeDtypeStruct(part.shape, part.dtype) for part in made),
            in_specs=[vmem] * 4,
            out_specs=(pl.BlockSpec(memory_space=pl.ANY),) * 4,
            scratch_shapes=[pltpu.SemaphoreType.DMA((4,))],
        )(*(pltpu.with_memory_space_constraint(part, pltpu.VMEM) for part in made))

    return jax.shard_map(
        shards,
        mesh=mesh,
        in_specs=(P("fsdp", "tp"),) * 4 + (P("tp", "fsdp"),),
        out_specs=(P("fsdp", "tp"),) * 3 + (P("tp", "fsdp"),),
        check_vma=False,
    )
```

```python
import functools
import math

import jax
import jax.numpy as jnp
from jax import lax
from jax.experimental import pallas as pl
from jax.experimental.pallas import tpu as pltpu
from jax.sharding import PartitionSpec as P

MESH = pl.DeviceIdType.MESH
F32, BF16 = jnp.float32, jnp.bfloat16
COPIES = 180


class Copy:
    def __init__(self, sems, src, dst, to, here=None, index=None):
        if index is None:
            index = sems[2][0]
            sems[2][0] += 1
        send, recv = sems[0].at[index], sems[1].at[index]
        self.remote = pltpu.make_async_remote_copy(
            src_ref=src, dst_ref=dst, send_sem=send, recv_sem=recv, device_id=to, device_id_type=MESH
        )
        self.local = None if here is None else pltpu.make_async_copy(src, dst, recv)
        self.here = here
        self.done = False

    def start(self):
        if self.here is None:
            self.remote.start()
        else:
            pl.when(self.here)(self.local.start)
            pl.when(jnp.logical_not(self.here))(self.remote.start)
        return self

    def wait(self):
        if not self.done:
            self.remote.wait_recv()
        self.done = True

    def sent(self):
        if self.here is None:
            self.remote.wait_send()
        else:
            pl.when(jnp.logical_not(self.here))(self.remote.wait_send)


def nt(a, b):
    return lax.dot_general(a, b, (((1,), (1,)), ((), ())), preferred_element_type=F32)


def tn(a, b):
    return lax.dot_general(a, b, (((0,), (0,)), ((), ())), preferred_element_type=F32)


def nn(a, b):
    return jnp.dot(a, b, preferred_element_type=F32)


def kernel(
    factor,
    tok_ref, grd_ref, gate_ref, up_ref, down_ref,
    ig_ref, gg_ref, ug_ref, dg_ref,
    TV, WV, WDV, G, GT, WG, WD, PS, DR, RF, RN, GU, DL, X, XB, XF, XN, IB, BB,
    Z, ZS, ZF, ZN, S, SX, SD,
    send, recv, local_sem, load_sem,
):
    f, t = lax.axis_index("fsdp"), lax.axis_index("tp")
    h, y = lax.div(f, 4), lax.rem(f, 4)
    c = lax.rem(t, 2)
    x = lax.rem(lax.div(t, 2), 4)
    l = lax.div(t, 8)
    z = 2 * h + l
    sems = (send, recv, [0])
    sent = []

    def dev(x=x, y=y, z=z, c=c):
        return (lax.div(z, 2) * 4 + y, (lax.rem(z, 2) * 4 + x) * 2 + c)

    def copy(src, dst, to, here=None, index=None):
        made = Copy(sems, src, dst, to, here, index)
        sent.append(made)
        return made.start()

    def turn(v, k):
        return lax.rem(v + k + 4, 4)

    xp, xm, yp, ym, zp, zm = (turn(v, k) for v in (x, y, z) for k in (1, -1))
    yf, xf, zf = turn(y, 2), turn(x, 2), turn(z, 2)
    cc, ll = 1 - c, 1 - l
    zo = 2 * h + ll
    zn = turn(z, 2 * l - 1)
    diagonal = x == y
    twin = dev(c=cc)

    loads = [
        pltpu.make_async_copy(src, dst, load_sem.at[n])
        for n, (src, dst) in enumerate(
            [(tok_ref, TV.at[0]), (grd_ref, TV.at[1]), (gate_ref, WV.at[0]), (up_ref, WV.at[1]), (down_ref, WDV)]
        )
    ]
    for load in loads:
        load.start()

    barrier = pltpu.get_barrier_semaphore()
    peers = [
        twin, dev(x=xp), dev(x=xm), dev(y=yp), dev(y=ym),
        dev(z=zp), dev(z=zm), dev(z=zf), dev(z=zp, c=cc), dev(z=zm, c=cc),
    ]
    for e in range(4):
        there, back_there = dict(x=turn(y, e), y=x), dict(x=y, y=turn(x, -e))
        peers += [dev(z=zo, **there), dev(z=zo, **back_there)]
        if e > 0:
            peers += [dev(**there), dev(**back_there)]
    for peer in peers:
        pl.semaphore_signal(barrier, inc=1, device_id=peer, device_id_type=MESH)

    @pl.when(jnp.logical_not(diagonal))
    def _():
        pl.semaphore_signal(barrier, inc=2, device_id=dev(x=y, y=x), device_id_type=MESH)
        pl.semaphore_wait(barrier, len(peers) + 2)

    @pl.when(diagonal)
    def _():
        pl.semaphore_wait(barrier, len(peers))

    moved = {}

    def move(a):
        loads[a].wait()
        for other in (1, 0):
            to_l = ll if other else l
            for e in range(4):
                to_x = turn(y, e)
                moved[a, other, e] = copy(
                    TV.at[a, pl.ds(pl.multiple_of(to_l * 128 + to_x * 32, 32), 32), :],
                    G.at[a, l, e // 2, to_x, pl.ds(e % 2 * 32, 32), :],
                    dev(x=to_x, y=x, z=zo if other else z),
                    diagonal if e == 0 and not other else None,
                )

    def weight_piece(i, k):
        half = pl.multiple_of(k * 512, 512)
        if i < 2:
            return WV.at[i, pl.ds(half, 512), :]
        return WDV.at[:, pl.ds(half, 512)]

    def weight_slot(i, at_z, core):
        at_h, block = lax.div(at_z, 2), lax.rem(at_z, 2) * 2 + core
        return WG.at[i, at_h, block] if i < 2 else WD.at[at_h, block]

    own_weights, from_twin, wn, wo, far_w = {}, {}, {}, {}, {}
    cores = (c, cc)

    def send_weights(i):
        loads[2 + i].wait()
        slot = weight_slot(i, z, c)
        mine = pltpu.make_async_copy(weight_piece(i, c), slot, local_sem.at[i])
        mine.start()
        own_weights[i] = mine
        from_twin[i] = copy(weight_piece(i, cc), slot, twin)

    def send_weights_to(i, s, over_n):
        to_z, made = (zn, wn) if over_n else (zo, wo)
        made[i, s] = copy(weight_piece(i, cores[s]), weight_slot(i, z, c), dev(z=to_z, c=cores[s]))

    def pass_weights(i, s):
        over_n = s == 0 or i == 0
        arrived, at_z, to_z = (wo, zo, zn) if over_n else (wn, zn, zo)
        arrived[i, s].wait()
        slot = weight_slot(i, at_z, cores[s])
        far_w[i, s] = copy(slot, slot, dev(z=to_z))

    def weights_here(i, part):
        if part == 0:
            for s in range(2):
                wn[i, s].wait()
                wo[i, s].wait()
        else:
            own_weights[i].wait()
            from_twin[i].wait()
            far_w[i, 0].wait()
            far_w[i, 1].wait()

    gp, gm, far_g = {}, {}, {}

    def spread(a, other):
        for e in range(4):
            moved[a, other, e].wait()
        slot = G.at[a, ll if other else l, :, x]
        gp[a, other] = copy(slot, slot, dev(x=xp))
        gm[a, other] = copy(slot, slot, dev(x=xm))

    def pass_tokens(a, side):
        if side == 0:
            gp[a, 0].wait()
            slot = G.at[a, l, :, xm]
            far_g[a, 0] = copy(slot, slot, dev(x=xp))
        else:
            gm[a, 1].wait()
            slot = G.at[a, ll, :, xp]
            far_g[a, 1] = copy(slot, slot, dev(x=xm))

    def tokens_here(a):
        gp[a, 1].wait()
        gm[a, 0].wait()
        far_g[a, 0].wait()
        far_g[a, 1].wait()

    sides = (ll, l)

    def gathered(a, k):
        return G[a, k].reshape(512, 512)

    def multiply(unit):
        parts, arrays_of, chunks = unit
        for part in range(*parts):
            l_to = sides[part]
            for i in range(*arrays_of):
                a = min(i // 2, 1)
                total = None
                for k in range(2):
                    rows = gathered(a, k) if chunks == (0, 2) else G[a, k, chunks[0]].reshape(256, 512)
                    if i < 2:
                        right = jnp.concatenate([WG[i, k, 2 * l_to], WG[i, k, 2 * l_to + 1]], axis=1)
                        term = nn(rows, right)
                    else:
                        right = jnp.concatenate([WD[k, 2 * l_to], WD[k, 2 * l_to + 1]], axis=0)
                        term = nt(rows, right)
                    total = term if total is None else total + term
                for half in range(2):
                    block = total[:, half * 128 : half * 128 + 128]
                    PS[part, i, chunks[0] : chunks[1], :, :, half] = block.reshape(
                        chunks[1] - chunks[0], 2, 4, 32, 128
                    )
        to_twin[unit] = copy(at(PS, unit, cc), at(DR, unit), twin)

    to_twin, yfar, ynear = {}, {}, {}

    def at(ref, unit, *more):
        return ref.at[(*(pl.ds(first, end - first) for first, end in unit), *more)]

    def over_unit(unit):
        parts, arrays_of, chunks = unit
        return [(p, i, q) for p in range(*parts) for i in range(*arrays_of) for q in range(*chunks)]

    def sum_start(unit):
        to_twin[unit].wait()
        for u in over_unit(unit):
            PS[(*u, c)] += DR[u]
        yfar[unit, 0] = copy(at(PS, unit, c, yf, 0), at(RF, unit, 0), dev(y=yp))
        yfar[unit, 1] = copy(at(PS, unit, c, yf, 1), at(RF, unit, 1), dev(y=ym))
        ynear[unit, 0, 1] = copy(at(PS, unit, c, yp, 1), at(RN, unit, 0, 1), dev(y=yp))
        ynear[unit, 1, 0] = copy(at(PS, unit, c, ym, 0), at(RN, unit, 1, 0), dev(y=ym))

    def sum_middle(unit):
        yfar[unit, 0].wait()
        for u in over_unit(unit):
            PS[(*u, c, yp, 0)] += RF[(*u, 0)]
        ynear[unit, 0, 0] = copy(at(PS, unit, c, yp, 0), at(RN, unit, 0, 0), dev(y=yp))
        yfar[unit, 1].wait()
        for u in over_unit(unit):
            PS[(*u, c, ym, 1)] += RF[(*u, 1)]
        ynear[unit, 1, 1] = copy(at(PS, unit, c, ym, 1), at(RN, unit, 1, 1), dev(y=ym))

    def sum_arrived(unit):
        for side in range(2):
            for half in range(2):
                ynear[unit, side, half].wait()

    def sum_end(part, i, q):
        return PS[part, i, q, c, y] + RN[part, i, q, 0] + RN[part, i, q, 1]

    def make_hidden(unit):
        sum_arrived(unit)
        for part in range(*unit[0]):
            for q in range(2):
                gate, up = sum_end(part, 0, q), sum_end(part, 1, q)
                GU[part, 0, q] = gate
                GU[part, 1, q] = up
                DL[part, c, y, 2, q] = (gate * jax.nn.sigmoid(gate) * up).astype(BF16)

    def make_deltas(unit):
        sum_arrived(unit)
        for part, _, q in over_unit(unit):
            gate, up, hidden_grad = GU[part, 0, q], GU[part, 1, q], sum_end(part, 2, q)
            squashed = jax.nn.sigmoid(gate)
            activated = gate * squashed
            slope = squashed * (1.0 + gate * (1.0 - squashed))
            DL[part, c, y, 0, q] = (hidden_grad * up * slope).astype(BF16)
            DL[part, c, y, 1, q] = (hidden_grad * activated).astype(BF16)

    dp, dm, far_d, over = {}, {}, {}, {}

    def delta_at(group, at_y, *half):
        parts, kinds, chunks = (pl.ds(first, end - first) for first, end in group)
        return DL.at[(parts, c, at_y, kinds, chunks, *half)]

    def give(group):
        for half in range(2):
            part = delta_at(group, y, half)
            dp[group, half] = copy(part, part, dev(y=yp))
            part = delta_at(group, y, 1 - half)
            dm[group, 1 - half] = copy(part, part, dev(y=ym))
        over[group] = [copy(delta_at(group, y), delta_at(group, y), twin)]

    def give_on(group):
        dp[group, 0].wait()
        part = delta_at(group, ym, 0)
        far_d[group, 0] = copy(part, part, dev(y=yp))
        dm[group, 1].wait()
        part = delta_at(group, yp, 1)
        far_d[group, 1] = copy(part, part, dev(y=ym))

    def give_over(group):
        dp[group, 1].wait()
        over[group].append(copy(delta_at(group, ym), delta_at(group, ym), twin))
        dm[group, 0].wait()
        over[group].append(copy(delta_at(group, yp), delta_at(group, yp), twin))

    def give_end(group):
        far_d[group, 0].wait()
        far_d[group, 1].wait()
        over[group].append(copy(delta_at(group, yf), delta_at(group, yf), twin))

    def given(group):
        for made in over[group]:
            made.wait()

    def delta(kind, part, q):
        return jnp.concatenate([DL[part, :, :, kind, q, half].reshape(256, 128) for half in range(2)], axis=1)

    def delta_all(kind, part):
        return jnp.concatenate([delta(kind, part, 0), delta(kind, part, 1)], axis=0)

    halves = (h, 1 - h)

    def grads_of_weights(i, part):
        for r in range(2):
            if i < 2:
                Z[i, 2 * part + r] = nn(GT[halves[r]], delta_all(i, part)).reshape(2, 256, 256)
            else:
                block = tn(delta_all(2, part), gathered(1, halves[r]))
                for j in range(2):
                    Z[2, 2 * part + r, j] = jnp.concatenate(
                        [block[j * 128 : j * 128 + 128, :256], block[j * 128 : j * 128 + 128, 256:]], axis=0
                    )

    zfar, znear = {}, {}

    def wsum_near(i):
        if i == 2:
            for side, to_z in enumerate((zo, zn)):
                ZS[2, side] = Z[2, side].astype(BF16)
                znear[2, side] = copy(ZS.at[2, side], ZN.at[2, side], dev(z=to_z))
            return
        ZS[i, 0, 1] = Z[i, 0, 1].astype(BF16)
        znear[i, 0, 1] = copy(ZS.at[i, 0, 1], ZN.at[i, 0, 1], dev(z=zo))
        ZS[i, 1, 0] = Z[i, 1, 0].astype(BF16)
        znear[i, 1, 0] = copy(ZS.at[i, 1, 0], ZN.at[i, 1, 0], dev(z=zn))

    def wsum_far(i):
        ZS[i, 2] = Z[i, 3].astype(BF16)
        if i == 2:
            zfar[2] = copy(ZS.at[2, 2], ZF.at[2], dev(z=zf))
            return
        zfar[i, 0] = copy(ZS.at[i, 2, 0], ZF.at[i, 0], dev(z=zn))
        zfar[i, 1] = copy(ZS.at[i, 2, 1], ZF.at[i, 1], dev(z=zo))

    def wsum_middle(i):
        zfar[i, 0].wait()
        ZS[i, 0, 0] = (Z[i, 0, 0] + ZF[i, 0].astype(F32)).astype(BF16)
        znear[i, 0, 0] = copy(ZS.at[i, 0, 0], ZN.at[i, 0, 0], dev(z=zo))
        zfar[i, 1].wait()
        ZS[i, 1, 1] = (Z[i, 1, 1] + ZF[i, 1].astype(F32)).astype(BF16)
        znear[i, 1, 1] = copy(ZS.at[i, 1, 1], ZN.at[i, 1, 1], dev(z=zn))

    last = []
    half_at = pl.ds(pl.multiple_of(c * 512, 512), 512)

    def wsum_end(i):
        sums = []
        for half in range(2):
            for side in range(2):
                znear[(i, side) if i == 2 else (i, side, half)].wait()
            total = Z[i, 2, half] + ZN[i, 0, half].astype(F32) + ZN[i, 1, half].astype(F32)
            if i == 2:
                zfar[2].wait()
                total = total + ZF[2, half].astype(F32)
            sums.append(total)
        done = [total * factor for total in sums]
        if i < 2:
            out = (gg_ref, ug_ref)[i]
            for half in range(2):
                low, high = done[half][:, :128], done[half][:, 128:]
                SX[i, pl.ds(half * 256, 256), :] = jnp.where(c == 0, high, low)
                S[i, pl.ds(half * 256, 256), :] = jnp.where(c == 0, low, high)
            last.append(copy(SX.at[i], out.at[half_at, :], twin))
            out[half_at, :] = S[i]
        else:
            blocks = [jnp.concatenate([part[:128], part[128:]], axis=1) for part in done]
            SD[...] = jnp.where(c == 0, blocks[1], blocks[0])
            last.append(copy(SD, dg_ref.at[:, half_at], twin))
            dg_ref[:, half_at] = jnp.where(c == 0, blocks[0], blocks[1])

    def input_rows(q):
        left = jnp.concatenate([delta(kind, part, q) for part in range(2) for kind in range(2)], axis=1)
        for k in range(2):
            right = jnp.concatenate(
                [WG[kind, k, 2 * sides[part] + b] for part in range(2) for kind in range(2) for b in range(2)], axis=1
            )
            X[q, :, k] = nt(left, right).reshape(4, 64, 512)

    xfar, xnear = {}, {}

    def isum_start(q):
        XB[q] = X[q, xf].astype(BF16)
        xfar[q, 0] = copy(XB.at[q, 0], XF.at[q, 0], dev(x=xp))
        xfar[q, 1] = copy(XB.at[q, 1], XF.at[q, 1], dev(x=xm))
        xnear[q, 0, 1] = copy(X.at[q, xp, 1], XN.at[q, 0, 1], dev(x=xp))
        xnear[q, 1, 0] = copy(X.at[q, xm, 0], XN.at[q, 1, 0], dev(x=xm))

    def isum_middle(q):
        xfar[q, 0].wait()
        X[q, xp, 0] += XF[q, 0].astype(F32)
        xnear[q, 0, 0] = copy(X.at[q, xp, 0], XN.at[q, 0, 0], dev(x=xp))
        xfar[q, 1].wait()
        X[q, xm, 1] += XF[q, 1].astype(F32)
        xnear[q, 1, 1] = copy(X.at[q, xm, 1], XN.at[q, 1, 1], dev(x=xm))

    def isum_end(q):
        for side in range(2):
            for half in range(2):
                xnear[q, side, half].wait()
        for k in range(2):
            IB[pl.ds(2 * q, 2), k] = (X[q, x, k] + XN[q, 0, k] + XN[q, 1, k]).astype(BF16).reshape(2, 32, 512)

    FIRST, SECOND = COPIES, COPIES + 4

    def arrives(index, ref):
        return pltpu.make_async_copy(ref, ref, recv.at[index])

    def send_back(q):
        for e in (2 * q, 2 * q + 1):
            far = turn(y - x, e)
            copy_back(IB.at[e], BB.at[far], dev(y=turn(x, -e)), far == 0, FIRST + far)

    def copy_back(src, dst, to, here, index):
        made = Copy(sems, src, dst, to, here, index)
        made.done = True
        sent.append(made.start())

    def pass_back():
        for d in range(4):
            arrives(FIRST + d, BB.at[d]).wait()
            to_x = turn(y, d)
            far = turn(to_x - x, 0)
            for other in (1, 0):
                copy_back(
                    BB.at[d, ll if other else l],
                    ig_ref.at[pl.ds(pl.multiple_of(l * 128 + x * 32, 32), 32), :],
                    dev(x=to_x, z=zo if other else z),
                    None if other else far == 0,
                    SECOND + 2 * far + other,
                )

    def back_here():
        for n in range(8):
            arrives(SECOND + n, ig_ref.at[pl.ds(0, 32), :]).wait()

    GATE_UP, HIDDEN = 0, 1
    both = (0, 2)
    gate_up = [((part, part + 1), both, both) for part in range(2)]
    down = [(both, (2, 3), (q, q + 1)) for q in range(2)]
    hidden = [((part, part + 1), (2, 3), both) for part in range(2)]
    deltas = [(both, both, (q, q + 1)) for q in range(2)]
    move(0)
    send_weights(0)
    send_weights_to(0, 0, False)
    send_weights_to(0, 0, True)
    send_weights_to(0, 1, False)
    send_weights_to(0, 1, True)
    move(1)
    send_weights(1)
    send_weights_to(1, 0, False)
    send_weights_to(1, 0, True)
    send_weights_to(1, 1, False)
    send_weights_to(1, 1, True)
    send_weights(2)
    send_weights_to(2, 0, True)
    spread(0, 0)
    spread(0, 1)
    pass_weights(0, 0)
    pass_tokens(0, 0)
    pass_tokens(0, 1)
    spread(1, 0)
    spread(1, 1)
    pass_weights(0, 1)
    weights_here(0, 0)
    pass_weights(1, 1)
    send_weights_to(2, 0, False)
    pass_weights(1, 0)
    send_weights_to(2, 1, True)
    send_weights_to(2, 1, False)
    tokens_here(0)
    weights_here(1, 0)
    multiply(gate_up[0])
    sum_start(gate_up[0])
    pass_tokens(1, 0)
    weights_here(0, 1)
    weights_here(1, 1)
    multiply(gate_up[1])
    sum_middle(gate_up[0])
    pass_weights(2, 0)
    sum_start(gate_up[1])
    pass_tokens(1, 1)
    pass_weights(2, 1)
    for k in range(2):
        GT[k] = gathered(0, k).T
    make_hidden(gate_up[0])
    give(hidden[0])
    sum_middle(gate_up[1])
    weights_here(2, 0)
    weights_here(2, 1)
    tokens_here(1)
    multiply(down[0])
    multiply(down[1])
    give_on(hidden[0])
    give_over(hidden[0])
    sum_start(down[0])
    sum_start(down[1])
    make_hidden(gate_up[1])
    give(hidden[1])
    give_end(hidden[0])
    sum_middle(down[0])
    sum_middle(down[1])
    given(hidden[0])
    grads_of_weights(2, 0)
    wsum_near(2)
    give_on(hidden[1])
    give_over(hidden[1])
    make_deltas(down[0])
    give(deltas[0])
    make_deltas(down[1])
    give(deltas[1])
    give_end(hidden[1])
    given(hidden[1])
    grads_of_weights(2, 1)
    wsum_far(2)
    give_on(deltas[0])
    give_over(deltas[0])
    give_on(deltas[1])
    give_over(deltas[1])
    give_end(deltas[0])
    give_end(deltas[1])
    given(deltas[0])
    input_rows(0)
    isum_start(0)
    given(deltas[1])
    grads_of_weights(0, 1)
    wsum_far(0)
    grads_of_weights(0, 0)
    wsum_near(0)
    input_rows(1)
    isum_start(1)
    grads_of_weights(1, 1)
    wsum_far(1)
    grads_of_weights(1, 0)
    wsum_near(1)
    isum_middle(0)
    isum_middle(1)
    wsum_middle(0)
    isum_end(0)
    send_back(0)
    wsum_middle(1)
    isum_end(1)
    send_back(1)
    wsum_end(2)
    pass_back()
    wsum_end(0)
    wsum_end(1)
    back_here()
    for made in last:
        made.wait()
    for made in sent:
        assert made.done and sems[2][0] <= COPIES
        made.sent()


def put_out(a, b, c, d, a_out, b_out, c_out, d_out, sems):
    copies = [
        pltpu.make_async_copy(src, dst, sems.at[n])
        for n, (src, dst) in enumerate([(a, a_out), (b, b_out), (c, c_out), (d, d_out)])
    ]
    for made in copies:
        made.start()
    for made in copies:
        made.wait()


def solution(mesh):
    def shards(tokens, out_grad, gate_weight, up_weight, down_weight):
        factor = 1.0 / math.sqrt(tokens.shape[0] * mesh.shape["fsdp"])
        vmem = pl.BlockSpec(memory_space=pltpu.VMEM)
        made = pl.pallas_call(
            functools.partial(kernel, factor),
            out_shape=(
                pltpu.VMEM((256, 512), BF16),
                pltpu.VMEM((1024, 128), F32),
                pltpu.VMEM((1024, 128), F32),
                pltpu.VMEM((128, 1024), F32),
            ),
            in_specs=[pl.BlockSpec(memory_space=pl.ANY)] * 5,
            out_specs=(vmem,) * 4,
            scratch_shapes=[
                pltpu.VMEM((2, 256, 512), BF16),
                pltpu.VMEM((2, 1024, 128), BF16),
                pltpu.VMEM((128, 1024), BF16),
                pltpu.VMEM((2, 2, 2, 4, 64, 512), BF16),
                pltpu.VMEM((2, 512, 512), BF16),
                pltpu.VMEM((2, 2, 4, 512, 128), BF16),
                pltpu.VMEM((2, 4, 128, 512), BF16),
                pltpu.VMEM((2, 3, 2, 2, 4, 2, 32, 128), F32),
                pltpu.VMEM((2, 3, 2, 4, 2, 32, 128), F32),
                pltpu.VMEM((2, 3, 2, 2, 32, 128), F32),
                pltpu.VMEM((2, 3, 2, 2, 2, 32, 128), F32),
                pltpu.VMEM((2, 2, 2, 2, 32, 128), F32),
                pltpu.VMEM((2, 2, 4, 3, 2, 2, 32, 128), BF16),
                pltpu.VMEM((2, 4, 2, 64, 512), F32),
                pltpu.VMEM((2, 2, 64, 512), BF16),
                pltpu.VMEM((2, 2, 64, 512), BF16),
                pltpu.VMEM((2, 2, 2, 64, 512), F32),
                pltpu.VMEM((4, 2, 32, 512), BF16),
                pltpu.VMEM((4, 2, 32, 512), BF16),
                pltpu.VMEM((3, 4, 2, 256, 256), F32),
                pltpu.VMEM((3, 3, 2, 256, 256), BF16),
                pltpu.VMEM((3, 2, 256, 256), BF16),
                pltpu.VMEM((3, 2, 2, 256, 256), BF16),
                pltpu.VMEM((2, 512, 128), F32),
                pltpu.VMEM((2, 512, 128), F32),
                pltpu.VMEM((128, 512), F32),
                pltpu.SemaphoreType.DMA((COPIES + 12,)),
                pltpu.SemaphoreType.DMA((COPIES + 12,)),
                pltpu.SemaphoreType.DMA((3,)),
                pltpu.SemaphoreType.DMA((5,)),
            ],
            compiler_params=pltpu.CompilerParams(
                collective_id=0, has_side_effects=True, vmem_limit_bytes=60 * 1024 * 1024
            ),
        )(tokens, out_grad, gate_weight, up_weight, down_weight)
        return pl.pallas_call(
            put_out,
            out_shape=tuple(jax.ShapeDtypeStruct(part.shape, part.dtype) for part in made),
            in_specs=[vmem] * 4,
            out_specs=(pl.BlockSpec(memory_space=pl.ANY),) * 4,
            scratch_shapes=[pltpu.SemaphoreType.DMA((4,))],
        )(*(pltpu.with_memory_space_constraint(part, pltpu.VMEM) for part in made))

    return jax.shard_map(
        shards,
        mesh=mesh,
        in_specs=(P("fsdp", "tp"),) * 4 + (P("tp", "fsdp"),),
        out_specs=(P("fsdp", "tp"),) * 3 + (P("tp", "fsdp"),),
        check_vma=False,
    )
```

```python
import functools
import math

import jax
import jax.numpy as jnp
from jax import lax
from jax.experimental import pallas as pl
from jax.experimental.pallas import tpu as pltpu
from jax.sharding import PartitionSpec as P

MESH = pl.DeviceIdType.MESH
F32, BF16 = jnp.float32, jnp.bfloat16
COPIES = 200


class Copy:
    def __init__(self, sems, src, dst, to, here=None, index=None):
        if index is None:
            index = sems[2][0]
            sems[2][0] += 1
        send, recv = sems[0].at[index], sems[1].at[index]
        self.remote = pltpu.make_async_remote_copy(
            src_ref=src, dst_ref=dst, send_sem=send, recv_sem=recv, device_id=to, device_id_type=MESH
        )
        self.local = None if here is None else pltpu.make_async_copy(src, dst, recv)
        self.here = here
        self.done = False

    def start(self):
        if self.here is None:
            self.remote.start()
        else:
            pl.when(self.here)(self.local.start)
            pl.when(jnp.logical_not(self.here))(self.remote.start)
        return self

    def wait(self):
        if not self.done:
            self.remote.wait_recv()
        self.done = True

    def sent(self):
        if self.here is None:
            self.remote.wait_send()
        else:
            pl.when(jnp.logical_not(self.here))(self.remote.wait_send)


class View:
    def __init__(self, ref, *lead):
        self.ref, self.lead = ref, lead

    def place(self, key):
        return (*self.lead, *(key if isinstance(key, tuple) else (key,)))

    def __getitem__(self, key):
        return self.ref[self.place(key)]

    def __setitem__(self, key, value):
        self.ref[self.place(key)] = value

    def at(self, *key):
        return self.ref.at[self.place(key)]


def nt(a, b):
    return lax.dot_general(a, b, (((1,), (1,)), ((), ())), preferred_element_type=F32)


def tn(a, b):
    return lax.dot_general(a, b, (((0,), (0,)), ((), ())), preferred_element_type=F32)


def nn(a, b):
    return jnp.dot(a, b, preferred_element_type=F32)


def kernel(
    factor,
    tok_ref, grd_ref, gate_ref, up_ref, down_ref,
    ig_ref, gg_ref, ug_ref, dg_ref,
    TV, WV, WDV, G, GT, WG, WD, PS, DR, RF, RN, GU, DL, X, XB, XF, XN, IB, BB,
    Z, ZS, ZF, ZN, ZU, ZSU, ZFU, ZNU, S, SX, SD,
    send, recv, local_sem, load_sem,
):
    f, t = lax.axis_index("fsdp"), lax.axis_index("tp")
    h, y = lax.div(f, 4), lax.rem(f, 4)
    c = lax.rem(t, 2)
    x = lax.rem(lax.div(t, 2), 4)
    l = lax.div(t, 8)
    z = 2 * h + l
    sems = (send, recv, [0])
    sent = []

    def dev(x=x, y=y, z=z, c=c):
        return (lax.div(z, 2) * 4 + y, (lax.rem(z, 2) * 4 + x) * 2 + c)

    def copy(src, dst, to, here=None, index=None):
        made = Copy(sems, src, dst, to, here, index)
        sent.append(made)
        return made.start()

    def turn(v, k):
        return lax.rem(v + k + 4, 4)

    xp, xm, yp, ym, zp, zm = (turn(v, k) for v in (x, y, z) for k in (1, -1))
    yf, xf, zf = turn(y, 2), turn(x, 2), turn(z, 2)
    cc, ll = 1 - c, 1 - l
    zo = 2 * h + ll
    zn = turn(z, 2 * l - 1)
    diagonal = x == y
    twin = dev(c=cc)

    loads = [
        pltpu.make_async_copy(src, dst, load_sem.at[n])
        for n, (src, dst) in enumerate(
            [(tok_ref, TV.at[0]), (grd_ref, TV.at[1]), (gate_ref, WV.at[0]), (up_ref, WV.at[1]), (down_ref, WDV)]
        )
    ]
    for load in loads:
        load.start()

    barrier = pltpu.get_barrier_semaphore()
    peers = [
        twin, dev(x=xp), dev(x=xm), dev(y=yp), dev(y=ym),
        dev(z=zp), dev(z=zm), dev(z=zf), dev(z=zp, c=cc), dev(z=zm, c=cc),
    ]
    for e in range(4):
        there, back_there = dict(x=turn(y, e), y=x), dict(x=y, y=turn(x, -e))
        peers += [dev(z=zo, **there), dev(z=zo, **back_there)]
        if e > 0:
            peers += [dev(**there), dev(**back_there)]
    for peer in peers:
        pl.semaphore_signal(barrier, inc=1, device_id=peer, device_id_type=MESH)

    @pl.when(jnp.logical_not(diagonal))
    def _():
        pl.semaphore_signal(barrier, inc=2, device_id=dev(x=y, y=x), device_id_type=MESH)
        pl.semaphore_wait(barrier, len(peers) + 2)

    @pl.when(diagonal)
    def _():
        pl.semaphore_wait(barrier, len(peers))

    moved = {}

    def move(a):
        loads[a].wait()
        for other in (1, 0):
            to_l = ll if other else l
            for e in range(4):
                to_x = turn(y, e)
                moved[a, other, e] = copy(
                    TV.at[a, pl.ds(pl.multiple_of(to_l * 128 + to_x * 32, 32), 32), :],
                    G.at[a, l, e // 2, to_x, pl.ds(e % 2 * 32, 32), :],
                    dev(x=to_x, y=x, z=zo if other else z),
                    diagonal if e == 0 and not other else None,
                )

    def weight_piece(i, k):
        half = pl.multiple_of(k * 512, 512)
        if i < 2:
            return WV.at[i, pl.ds(half, 512), :]
        return WDV.at[:, pl.ds(half, 512)]

    def weight_slot(i, at_z, core):
        at_h, block = lax.div(at_z, 2), lax.rem(at_z, 2) * 2 + core
        return WG.at[i, at_h, block] if i < 2 else WD.at[at_h, block]

    own_weights, from_twin, wn, wo, far_w = {}, {}, {}, {}, {}
    cores = (c, cc)

    def send_weights(i):
        loads[2 + i].wait()
        slot = weight_slot(i, z, c)
        mine = pltpu.make_async_copy(weight_piece(i, c), slot, local_sem.at[i])
        mine.start()
        own_weights[i] = mine
        from_twin[i] = copy(weight_piece(i, cc), slot, twin)

    def send_weights_to(i, s, over_n):
        to_z, made = (zn, wn) if over_n else (zo, wo)
        made[i, s] = copy(weight_piece(i, cores[s]), weight_slot(i, z, c), dev(z=to_z, c=cores[s]))

    def pass_weights(i, s):
        over_n = s == 0 or i == 0
        arrived, at_z, to_z = (wo, zo, zn) if over_n else (wn, zn, zo)
        arrived[i, s].wait()
        slot = weight_slot(i, at_z, cores[s])
        far_w[i, s] = copy(slot, slot, dev(z=to_z))

    def weights_here(i, part):
        if part == 0:
            for s in range(2):
                wn[i, s].wait()
                wo[i, s].wait()
        else:
            own_weights[i].wait()
            from_twin[i].wait()
            far_w[i, 0].wait()
            far_w[i, 1].wait()

    gp, gm, far_g = {}, {}, {}

    def spread(a, other):
        for e in range(4):
            moved[a, other, e].wait()
        slot = G.at[a, ll if other else l, :, x]
        gp[a, other] = copy(slot, slot, dev(x=xp))
        gm[a, other] = copy(slot, slot, dev(x=xm))

    def pass_tokens(a, side):
        if side == 0:
            gp[a, 0].wait()
            slot = G.at[a, l, :, xm]
            far_g[a, 0] = copy(slot, slot, dev(x=xp))
        else:
            gm[a, 1].wait()
            slot = G.at[a, ll, :, xp]
            far_g[a, 1] = copy(slot, slot, dev(x=xm))

    def tokens_here(a):
        gp[a, 1].wait()
        gm[a, 0].wait()
        far_g[a, 0].wait()
        far_g[a, 1].wait()

    sides = (ll, l)

    def gathered(a, k):
        return G[a, k].reshape(512, 512)

    def multiply(unit):
        parts, arrays_of, chunks = unit
        for part in range(*parts):
            l_to = sides[part]
            for i in range(*arrays_of):
                a = min(i // 2, 1)
                total = None
                for k in range(2):
                    rows = gathered(a, k) if chunks == (0, 2) else G[a, k, chunks[0]].reshape(256, 512)
                    if i < 2:
                        right = jnp.concatenate([WG[i, k, 2 * l_to], WG[i, k, 2 * l_to + 1]], axis=1)
                        term = nn(rows, right)
                    else:
                        right = jnp.concatenate([WD[k, 2 * l_to], WD[k, 2 * l_to + 1]], axis=0)
                        term = nt(rows, right)
                    total = term if total is None else total + term
                for half in range(2):
                    block = total[:, half * 128 : half * 128 + 128]
                    PS[part, i, chunks[0] : chunks[1], :, :, half] = block.reshape(
                        chunks[1] - chunks[0], 2, 4, 32, 128
                    )
        to_twin[unit] = copy(at(PS, unit, cc), at(DR, unit), twin)

    to_twin, yfar, ynear = {}, {}, {}

    def at(ref, unit, *more):
        return ref.at[(*(pl.ds(first, end - first) for first, end in unit), *more)]

    def over_unit(unit):
        parts, arrays_of, chunks = unit
        return [(p, i, q) for p in range(*parts) for i in range(*arrays_of) for q in range(*chunks)]

    def sum_start(unit):
        to_twin[unit].wait()
        for u in over_unit(unit):
            PS[(*u, c)] += DR[u]
        yfar[unit, 0] = copy(at(PS, unit, c, yf, 0), at(RF, unit, 0), dev(y=yp))
        yfar[unit, 1] = copy(at(PS, unit, c, yf, 1), at(RF, unit, 1), dev(y=ym))
        ynear[unit, 0, 1] = copy(at(PS, unit, c, yp, 1), at(RN, unit, 0, 1), dev(y=yp))
        ynear[unit, 1, 0] = copy(at(PS, unit, c, ym, 0), at(RN, unit, 1, 0), dev(y=ym))

    def sum_middle(unit):
        yfar[unit, 0].wait()
        for u in over_unit(unit):
            PS[(*u, c, yp, 0)] += RF[(*u, 0)]
        ynear[unit, 0, 0] = copy(at(PS, unit, c, yp, 0), at(RN, unit, 0, 0), dev(y=yp))
        yfar[unit, 1].wait()
        for u in over_unit(unit):
            PS[(*u, c, ym, 1)] += RF[(*u, 1)]
        ynear[unit, 1, 1] = copy(at(PS, unit, c, ym, 1), at(RN, unit, 1, 1), dev(y=ym))

    def sum_arrived(unit):
        for side in range(2):
            for half in range(2):
                ynear[unit, side, half].wait()

    def sum_end(part, i, q):
        return PS[part, i, q, c, y] + RN[part, i, q, 0] + RN[part, i, q, 1]

    def make_hidden(unit):
        sum_arrived(unit)
        for part in range(*unit[0]):
            for q in range(2):
                gate, up = sum_end(part, 0, q), sum_end(part, 1, q)
                GU[part, 0, q] = gate
                GU[part, 1, q] = up
                DL[part, c, y, 2, q] = (gate * jax.nn.sigmoid(gate) * up).astype(BF16)

    def make_deltas(unit):
        sum_arrived(unit)
        for part, _, q in over_unit(unit):
            gate, up, hidden_grad = GU[part, 0, q], GU[part, 1, q], sum_end(part, 2, q)
            squashed = jax.nn.sigmoid(gate)
            activated = gate * squashed
            slope = squashed * (1.0 + gate * (1.0 - squashed))
            DL[part, c, y, 0, q] = (hidden_grad * up * slope).astype(BF16)
            DL[part, c, y, 1, q] = (hidden_grad * activated).astype(BF16)

    dp, dm, far_d, over = {}, {}, {}, {}

    def delta_at(group, at_y, *half):
        parts, kinds, chunks = (pl.ds(first, end - first) for first, end in group)
        return DL.at[(parts, c, at_y, kinds, chunks, *half)]

    def give(group):
        for half in range(2):
            part = delta_at(group, y, half)
            dp[group, half] = copy(part, part, dev(y=yp))
            part = delta_at(group, y, 1 - half)
            dm[group, 1 - half] = copy(part, part, dev(y=ym))
        over[group] = [copy(delta_at(group, y), delta_at(group, y), twin)]

    def give_on(group):
        dp[group, 0].wait()
        part = delta_at(group, ym, 0)
        far_d[group, 0] = copy(part, part, dev(y=yp))
        dm[group, 1].wait()
        part = delta_at(group, yp, 1)
        far_d[group, 1] = copy(part, part, dev(y=ym))

    def give_over(group):
        dp[group, 1].wait()
        over[group].append(copy(delta_at(group, ym), delta_at(group, ym), twin))
        dm[group, 0].wait()
        over[group].append(copy(delta_at(group, yp), delta_at(group, yp), twin))

    def give_end(group):
        far_d[group, 0].wait()
        far_d[group, 1].wait()
        over[group].append(copy(delta_at(group, yf), delta_at(group, yf), twin))

    def given(group):
        for made in over[group]:
            made.wait()

    def delta(kind, part, q, owners=(0, 1)):
        return jnp.concatenate([DL[part, :, :, kind, q, half].reshape(256, 128) for half in owners], axis=1)

    def delta_all(kind, part, owners=(0, 1)):
        return jnp.concatenate([delta(kind, part, q, owners) for q in range(2)], axis=0)

    halves = (h, 1 - h)

    def grads_of_weights(i, part):
        for r in range(2):
            if i == 0:
                Z[0, 2 * part + r] = nn(GT[halves[r]], delta_all(0, part)).reshape(2, 256, 256)
            elif i == 1:
                block = nn(GT[halves[r]], delta_all(1, part, (cc, c))).reshape(2, 256, 256)
                ZU[0, 2 * part + r] = block[:, :, :128]
                ZU[1, 2 * part + r] = block[:, :, 128:]
            else:
                block = tn(delta_all(2, part), gathered(1, halves[r]))
                for j in range(2):
                    Z[2, 2 * part + r, j] = jnp.concatenate(
                        [block[j * 128 : j * 128 + 128, :256], block[j * 128 : j * 128 + 128, 256:]], axis=0
                    )

    zfar, znear = {}, {}

    def stream(i):
        if i in (0, 2):
            return [View(ref, i) for ref in (Z, ZS, ZF, ZN)]
        return [View(ref, i // 2) for ref in (ZU, ZSU, ZFU, ZNU)]

    def wsum_near(i):
        part, out, _, near = stream(i)
        if i == 2:
            for side, to_z in enumerate((zo, zn)):
                out[side] = part[side].astype(BF16)
                znear[2, side] = copy(out.at(side), near.at(side), dev(z=to_z))
            return
        out[0, 1] = part[0, 1].astype(BF16)
        znear[i, 0, 1] = copy(out.at(0, 1), near.at(0, 1), dev(z=zo))
        out[1, 0] = part[1, 0].astype(BF16)
        znear[i, 1, 0] = copy(out.at(1, 0), near.at(1, 0), dev(z=zn))

    def wsum_far(i):
        part, out, far, _ = stream(i)
        out[2] = part[3].astype(BF16)
        if i == 2:
            zfar[2] = copy(out.at(2), far.at(), dev(z=zf))
            return
        zfar[i, 0] = copy(out.at(2, 0), far.at(0), dev(z=zn))
        zfar[i, 1] = copy(out.at(2, 1), far.at(1), dev(z=zo))

    def wsum_middle(i):
        part, out, far, near = stream(i)
        zfar[i, 0].wait()
        out[0, 0] = (part[0, 0] + far[0].astype(F32)).astype(BF16)
        znear[i, 0, 0] = copy(out.at(0, 0), near.at(0, 0), dev(z=zo))
        zfar[i, 1].wait()
        out[1, 1] = (part[1, 1] + far[1].astype(F32)).astype(BF16)
        znear[i, 1, 1] = copy(out.at(1, 1), near.at(1, 1), dev(z=zn))

    last = []
    half_at = pl.ds(pl.multiple_of(c * 512, 512), 512)

    def wsum_end(i):
        part, _, far, near = stream(i)
        sums = []
        for half in range(2):
            for side in range(2):
                znear[(i, side) if i == 2 else (i, side, half)].wait()
            total = part[2, half] + near[0, half].astype(F32) + near[1, half].astype(F32)
            if i == 2:
                zfar[2].wait()
                total = total + far[half].astype(F32)
            sums.append(total)
        done = [total * factor for total in sums]
        if i == 0:
            for half in range(2):
                low, high = done[half][:, :128], done[half][:, 128:]
                SX[0, pl.ds(half * 256, 256), :] = jnp.where(c == 0, high, low)
                S[0, pl.ds(half * 256, 256), :] = jnp.where(c == 0, low, high)
            last.append(copy(SX.at[0], gg_ref.at[half_at, :], twin))
            gg_ref[half_at, :] = S[0]
        elif i == 1:
            for half in range(2):
                SX[1, pl.ds(half * 256, 256), :] = done[half]
            last.append(copy(SX.at[1], ug_ref.at[half_at, :], twin))
        elif i == 3:
            for half in range(2):
                ug_ref[pl.ds(pl.multiple_of(c * 512 + half * 256, 256), 256), :] = done[half]
        else:
            blocks = [jnp.concatenate([part[:128], part[128:]], axis=1) for part in done]
            SD[...] = jnp.where(c == 0, blocks[1], blocks[0])
            last.append(copy(SD, dg_ref.at[:, half_at], twin))
            dg_ref[:, half_at] = jnp.where(c == 0, blocks[0], blocks[1])

    def input_rows(q):
        left = jnp.concatenate([delta(kind, part, q) for part in range(2) for kind in range(2)], axis=1)
        for k in range(2):
            right = jnp.concatenate(
                [WG[kind, k, 2 * sides[part] + b] for part in range(2) for kind in range(2) for b in range(2)], axis=1
            )
            term = nt(left, right).reshape(4, 2, 32, 512)
            X[2 * q, :, k] = term[:, 0]
            X[2 * q + 1, :, k] = term[:, 1]

    xfar, xnear = {}, {}

    def isum_start(q):
        XB[q] = X[q, xf].astype(BF16)
        xfar[q, 0] = copy(XB.at[q, 0], XF.at[q, 0], dev(x=xp))
        xfar[q, 1] = copy(XB.at[q, 1], XF.at[q, 1], dev(x=xm))
        xnear[q, 0, 1] = copy(X.at[q, xp, 1], XN.at[q, 0, 1], dev(x=xp))
        xnear[q, 1, 0] = copy(X.at[q, xm, 0], XN.at[q, 1, 0], dev(x=xm))

    def isum_middle(q):
        xfar[q, 0].wait()
        X[q, xp, 0] += XF[q, 0].astype(F32)
        xnear[q, 0, 0] = copy(X.at[q, xp, 0], XN.at[q, 0, 0], dev(x=xp))
        xfar[q, 1].wait()
        X[q, xm, 1] += XF[q, 1].astype(F32)
        xnear[q, 1, 1] = copy(X.at[q, xm, 1], XN.at[q, 1, 1], dev(x=xm))

    def isum_end(q):
        for side in range(2):
            for half in range(2):
                xnear[q, side, half].wait()
        for k in range(2):
            IB[q, k] = (X[q, x, k] + XN[q, 0, k] + XN[q, 1, k]).astype(BF16)

    FIRST, SECOND = COPIES, COPIES + 4

    def arrives(index, ref):
        return pltpu.make_async_copy(ref, ref, recv.at[index])

    def send_back(e):
        far = turn(y - x, e)
        copy_back(IB.at[e], BB.at[far], dev(y=turn(x, -e)), far == 0, FIRST + far)

    def copy_back(src, dst, to, here, index):
        made = Copy(sems, src, dst, to, here, index)
        made.done = True
        sent.append(made.start())

    def pass_back():
        for d in range(4):
            arrives(FIRST + d, BB.at[d]).wait()
            to_x = turn(y, d)
            far = turn(to_x - x, 0)
            for other in (1, 0):
                copy_back(
                    BB.at[d, ll if other else l],
                    ig_ref.at[pl.ds(pl.multiple_of(l * 128 + x * 32, 32), 32), :],
                    dev(x=to_x, z=zo if other else z),
                    None if other else far == 0,
                    SECOND + 2 * far + other,
                )

    def back_here():
        for n in range(8):
            arrives(SECOND + n, ig_ref.at[pl.ds(0, 32), :]).wait()

    GATE_UP, HIDDEN = 0, 1
    both = (0, 2)
    gate_up = [((part, part + 1), both, both) for part in range(2)]
    down = [(both, (2, 3), (q, q + 1)) for q in range(2)]
    hidden = [((part, part + 1), (2, 3), both) for part in range(2)]
    deltas = [(both, both, (q, q + 1)) for q in range(2)]
    move(0)
    send_weights(0)
    send_weights_to(0, 0, False)
    send_weights_to(0, 0, True)
    send_weights_to(0, 1, False)
    send_weights_to(0, 1, True)
    move(1)
    send_weights(1)
    send_weights_to(1, 0, False)
    send_weights_to(1, 0, True)
    send_weights_to(1, 1, False)
    send_weights_to(1, 1, True)
    send_weights(2)
    spread(0, 0)
    spread(0, 1)
    pass_weights(0, 0)
    pass_tokens(0, 0)
    pass_tokens(0, 1)
    pass_weights(0, 1)
    spread(1, 0)
    spread(1, 1)
    weights_here(0, 0)
    pass_weights(1, 1)
    send_weights_to(2, 0, False)
    pass_weights(1, 0)
    send_weights_to(2, 0, True)
    send_weights_to(2, 1, True)
    send_weights_to(2, 1, False)
    tokens_here(0)
    weights_here(1, 0)
    multiply(gate_up[0])
    sum_start(gate_up[0])
    pass_tokens(1, 0)
    weights_here(0, 1)
    weights_here(1, 1)
    multiply(gate_up[1])
    sum_middle(gate_up[0])
    pass_weights(2, 0)
    sum_start(gate_up[1])
    pass_tokens(1, 1)
    pass_weights(2, 1)
    for k in range(2):
        GT[k] = gathered(0, k).T
    make_hidden(gate_up[0])
    give(hidden[0])
    sum_middle(gate_up[1])
    weights_here(2, 0)
    weights_here(2, 1)
    tokens_here(1)
    multiply(down[0])
    multiply(down[1])
    give_on(hidden[0])
    give_over(hidden[0])
    sum_start(down[0])
    sum_start(down[1])
    make_hidden(gate_up[1])
    give(hidden[1])
    give_end(hidden[0])
    sum_middle(down[0])
    sum_middle(down[1])
    given(hidden[0])
    grads_of_weights(2, 0)
    wsum_near(2)
    give_on(hidden[1])
    give_over(hidden[1])
    make_deltas(down[0])
    give(deltas[0])
    make_deltas(down[1])
    give(deltas[1])
    give_end(hidden[1])
    given(hidden[1])
    grads_of_weights(2, 1)
    wsum_far(2)
    give_on(deltas[0])
    give_over(deltas[0])
    give_on(deltas[1])
    give_over(deltas[1])
    give_end(deltas[0])
    give_end(deltas[1])
    given(deltas[0])
    input_rows(0)
    isum_start(0)
    isum_start(1)
    given(deltas[1])
    grads_of_weights(0, 1)
    wsum_far(0)
    grads_of_weights(0, 0)
    wsum_near(0)
    input_rows(1)
    isum_start(2)
    isum_start(3)
    grads_of_weights(1, 1)
    wsum_far(1)
    wsum_far(3)
    grads_of_weights(1, 0)
    wsum_near(1)
    wsum_near(3)
    isum_middle(0)
    isum_middle(1)
    isum_middle(2)
    isum_middle(3)
    wsum_middle(0)
    isum_end(0)
    send_back(0)
    wsum_middle(1)
    wsum_middle(3)
    isum_end(1)
    send_back(1)
    isum_end(2)
    send_back(2)
    isum_end(3)
    send_back(3)
    wsum_end(2)
    pass_back()
    wsum_end(0)
    wsum_end(1)
    wsum_end(3)
    back_here()
    for made in last:
        made.wait()
    for made in sent:
        assert made.done and sems[2][0] <= COPIES
        made.sent()


def put_out(a, b, c, d, a_out, b_out, c_out, d_out, sems):
    copies = [
        pltpu.make_async_copy(src, dst, sems.at[n])
        for n, (src, dst) in enumerate([(a, a_out), (b, b_out), (c, c_out), (d, d_out)])
    ]
    for made in copies:
        made.start()
    for made in copies:
        made.wait()


def solution(mesh):
    def shards(tokens, out_grad, gate_weight, up_weight, down_weight):
        factor = 1.0 / math.sqrt(tokens.shape[0] * mesh.shape["fsdp"])
        vmem = pl.BlockSpec(memory_space=pltpu.VMEM)
        made = pl.pallas_call(
            functools.partial(kernel, factor),
            out_shape=(
                pltpu.VMEM((256, 512), BF16),
                pltpu.VMEM((1024, 128), F32),
                pltpu.VMEM((1024, 128), F32),
                pltpu.VMEM((128, 1024), F32),
            ),
            in_specs=[pl.BlockSpec(memory_space=pl.ANY)] * 5,
            out_specs=(vmem,) * 4,
            scratch_shapes=[
                pltpu.VMEM((2, 256, 512), BF16),
                pltpu.VMEM((2, 1024, 128), BF16),
                pltpu.VMEM((128, 1024), BF16),
                pltpu.VMEM((2, 2, 2, 4, 64, 512), BF16),
                pltpu.VMEM((2, 512, 512), BF16),
                pltpu.VMEM((2, 2, 4, 512, 128), BF16),
                pltpu.VMEM((2, 4, 128, 512), BF16),
                pltpu.VMEM((2, 3, 2, 2, 4, 2, 32, 128), F32),
                pltpu.VMEM((2, 3, 2, 4, 2, 32, 128), F32),
                pltpu.VMEM((2, 3, 2, 2, 32, 128), F32),
                pltpu.VMEM((2, 3, 2, 2, 2, 32, 128), F32),
                pltpu.VMEM((2, 2, 2, 2, 32, 128), F32),
                pltpu.VMEM((2, 2, 4, 3, 2, 2, 32, 128), BF16),
                pltpu.VMEM((4, 4, 2, 32, 512), F32),
                pltpu.VMEM((4, 2, 32, 512), BF16),
                pltpu.VMEM((4, 2, 32, 512), BF16),
                pltpu.VMEM((4, 2, 2, 32, 512), F32),
                pltpu.VMEM((4, 2, 32, 512), BF16),
                pltpu.VMEM((4, 2, 32, 512), BF16),
                pltpu.VMEM((3, 4, 2, 256, 256), F32),
                pltpu.VMEM((3, 3, 2, 256, 256), BF16),
                pltpu.VMEM((3, 2, 256, 256), BF16),
                pltpu.VMEM((3, 2, 2, 256, 256), BF16),
                pltpu.VMEM((2, 4, 2, 256, 128), F32),
                pltpu.VMEM((2, 3, 2, 256, 128), BF16),
                pltpu.VMEM((2, 2, 256, 128), BF16),
                pltpu.VMEM((2, 2, 2, 256, 128), BF16),
                pltpu.VMEM((2, 512, 128), F32),
                pltpu.VMEM((2, 512, 128), F32),
                pltpu.VMEM((128, 512), F32),
                pltpu.SemaphoreType.DMA((COPIES + 12,)),
                pltpu.SemaphoreType.DMA((COPIES + 12,)),
                pltpu.SemaphoreType.DMA((3,)),
                pltpu.SemaphoreType.DMA((5,)),
            ],
            compiler_params=pltpu.CompilerParams(
                collective_id=0, has_side_effects=True, vmem_limit_bytes=60 * 1024 * 1024
            ),
        )(tokens, out_grad, gate_weight, up_weight, down_weight)
        return pl.pallas_call(
            put_out,
            out_shape=tuple(jax.ShapeDtypeStruct(part.shape, part.dtype) for part in made),
            in_specs=[vmem] * 4,
            out_specs=(pl.BlockSpec(memory_space=pl.ANY),) * 4,
            scratch_shapes=[pltpu.SemaphoreType.DMA((4,))],
        )(*(pltpu.with_memory_space_constraint(part, pltpu.VMEM) for part in made))

    return jax.shard_map(
        shards,
        mesh=mesh,
        in_specs=(P("fsdp", "tp"),) * 4 + (P("tp", "fsdp"),),
        out_specs=(P("fsdp", "tp"),) * 3 + (P("tp", "fsdp"),),
        check_vma=False,
    )
```

```python
import functools
import math

import jax
import jax.numpy as jnp
from jax import lax
from jax.experimental import pallas as pl
from jax.experimental.pallas import tpu as pltpu
from jax.sharding import PartitionSpec as P

MESH = pl.DeviceIdType.MESH
F32, BF16 = jnp.float32, jnp.bfloat16
COPIES = 200


class Copy:
    def __init__(self, sems, src, dst, to, here=None, index=None):
        if index is None:
            index = sems[2][0]
            sems[2][0] += 1
        send, recv = sems[0].at[index], sems[1].at[index]
        self.remote = pltpu.make_async_remote_copy(
            src_ref=src, dst_ref=dst, send_sem=send, recv_sem=recv, device_id=to, device_id_type=MESH
        )
        self.local = None if here is None else pltpu.make_async_copy(src, dst, recv)
        self.here = here
        self.done = False

    def start(self):
        if self.here is None:
            self.remote.start()
        else:
            pl.when(self.here)(self.local.start)
            pl.when(jnp.logical_not(self.here))(self.remote.start)
        return self

    def wait(self):
        if not self.done:
            self.remote.wait_recv()
        self.done = True

    def sent(self):
        if self.here is None:
            self.remote.wait_send()
        else:
            pl.when(jnp.logical_not(self.here))(self.remote.wait_send)


class View:
    def __init__(self, ref, *lead):
        self.ref, self.lead = ref, lead

    def place(self, key):
        return (*self.lead, *(key if isinstance(key, tuple) else (key,)))

    def __getitem__(self, key):
        return self.ref[self.place(key)]

    def __setitem__(self, key, value):
        self.ref[self.place(key)] = value

    def at(self, *key):
        return self.ref.at[self.place(key)]


def nt(a, b):
    return lax.dot_general(a, b, (((1,), (1,)), ((), ())), preferred_element_type=F32)


def tn(a, b):
    return lax.dot_general(a, b, (((0,), (0,)), ((), ())), preferred_element_type=F32)


def nn(a, b):
    return jnp.dot(a, b, preferred_element_type=F32)


def kernel(
    factor,
    tok_ref, grd_ref, gate_ref, up_ref, down_ref,
    ig_ref, gg_ref, ug_ref, dg_ref,
    TV, WV, WDV, G, GT, WG, WD, PS, DR, RF, RN, GU, DL, X, XB, XF, XN, IB, BB,
    Z, ZS, ZF, ZN, ZU, ZSU, ZFU, ZNU, S, SX, SD,
    send, recv, local_sem, load_sem,
):
    f, t = lax.axis_index("fsdp"), lax.axis_index("tp")
    h, y = lax.div(f, 4), lax.rem(f, 4)
    c = lax.rem(t, 2)
    x = lax.rem(lax.div(t, 2), 4)
    l = lax.div(t, 8)
    z = 2 * h + l
    sems = (send, recv, [0])
    sent = []

    def dev(x=x, y=y, z=z, c=c):
        return (lax.div(z, 2) * 4 + y, (lax.rem(z, 2) * 4 + x) * 2 + c)

    def copy(src, dst, to, here=None, index=None):
        made = Copy(sems, src, dst, to, here, index)
        sent.append(made)
        return made.start()

    def turn(v, k):
        return lax.rem(v + k + 4, 4)

    xp, xm, yp, ym, zp, zm = (turn(v, k) for v in (x, y, z) for k in (1, -1))
    yf, xf, zf = turn(y, 2), turn(x, 2), turn(z, 2)
    cc, ll = 1 - c, 1 - l
    zo = 2 * h + ll
    zn = turn(z, 2 * l - 1)
    diagonal = x == y
    twin = dev(c=cc)

    loads = [
        pltpu.make_async_copy(src, dst, load_sem.at[n])
        for n, (src, dst) in enumerate(
            [(tok_ref, TV.at[0]), (grd_ref, TV.at[1]), (gate_ref, WV.at[0]), (up_ref, WV.at[1]), (down_ref, WDV)]
        )
    ]
    for load in loads:
        load.start()

    barrier = pltpu.get_barrier_semaphore()
    peers = [
        twin, dev(x=xp), dev(x=xm), dev(y=yp), dev(y=ym),
        dev(z=zp), dev(z=zm), dev(z=zf), dev(z=zp, c=cc), dev(z=zm, c=cc),
    ]
    for e in range(4):
        there, back_there = dict(x=turn(y, e), y=x), dict(x=y, y=turn(x, -e))
        peers += [dev(z=zo, **there), dev(z=zo, **back_there)]
        if e > 0:
            peers += [dev(**there), dev(**back_there)]
    for peer in peers:
        pl.semaphore_signal(barrier, inc=1, device_id=peer, device_id_type=MESH)

    @pl.when(jnp.logical_not(diagonal))
    def _():
        pl.semaphore_signal(barrier, inc=2, device_id=dev(x=y, y=x), device_id_type=MESH)
        pl.semaphore_wait(barrier, len(peers) + 2)

    @pl.when(diagonal)
    def _():
        pl.semaphore_wait(barrier, len(peers))

    moved = {}

    def move(a):
        loads[a].wait()
        for other in (1, 0):
            to_l = ll if other else l
            for e in range(4):
                to_x = turn(y, e)
                moved[a, other, e] = copy(
                    TV.at[a, pl.ds(pl.multiple_of(to_l * 128 + to_x * 32, 32), 32), :],
                    G.at[a, l, e // 2, to_x, pl.ds(e % 2 * 32, 32), :],
                    dev(x=to_x, y=x, z=zo if other else z),
                    diagonal if e == 0 and not other else None,
                )

    def weight_piece(i, k):
        half = pl.multiple_of(k * 512, 512)
        if i < 2:
            return WV.at[i, pl.ds(half, 512), :]
        return WDV.at[:, pl.ds(half, 512)]

    def weight_slot(i, at_z, core):
        at_h, block = lax.div(at_z, 2), lax.rem(at_z, 2) * 2 + core
        return WG.at[i, at_h, block] if i < 2 else WD.at[at_h, block]

    own_weights, from_twin, wn, wo, far_w = {}, {}, {}, {}, {}
    cores = (c, cc)

    def send_weights(i):
        loads[2 + i].wait()
        slot = weight_slot(i, z, c)
        mine = pltpu.make_async_copy(weight_piece(i, c), slot, local_sem.at[i])
        mine.start()
        own_weights[i] = mine
        from_twin[i] = copy(weight_piece(i, cc), slot, twin)

    def send_weights_to(i, s, over_n):
        to_z, made = (zn, wn) if over_n else (zo, wo)
        made[i, s] = copy(weight_piece(i, cores[s]), weight_slot(i, z, c), dev(z=to_z, c=cores[s]))

    def pass_weights(i, s):
        over_n = s == 0 or i == 0
        arrived, at_z, to_z = (wo, zo, zn) if over_n else (wn, zn, zo)
        arrived[i, s].wait()
        slot = weight_slot(i, at_z, cores[s])
        far_w[i, s] = copy(slot, slot, dev(z=to_z))

    def weights_here(i, part):
        if part == 0:
            for s in range(2):
                wn[i, s].wait()
                wo[i, s].wait()
        else:
            own_weights[i].wait()
            from_twin[i].wait()
            far_w[i, 0].wait()
            far_w[i, 1].wait()

    gp, gm, far_g = {}, {}, {}

    def spread(a, other):
        for e in range(4):
            moved[a, other, e].wait()
        slot = G.at[a, ll if other else l, :, x]
        gp[a, other] = copy(slot, slot, dev(x=xp))
        gm[a, other] = copy(slot, slot, dev(x=xm))

    def pass_tokens(a, side):
        if side == 0:
            gp[a, 0].wait()
            slot = G.at[a, l, :, xm]
            far_g[a, 0] = copy(slot, slot, dev(x=xp))
        else:
            gm[a, 1].wait()
            slot = G.at[a, ll, :, xp]
            far_g[a, 1] = copy(slot, slot, dev(x=xm))

    def tokens_here(a):
        gp[a, 1].wait()
        gm[a, 0].wait()
        far_g[a, 0].wait()
        far_g[a, 1].wait()

    sides = (ll, l)

    def gathered(a, k):
        return G[a, k].reshape(512, 512)

    def multiply(unit):
        parts, arrays_of, chunks = unit
        to_twin[unit] = []
        for i in range(*arrays_of):
            for part in range(*parts):
                l_to = sides[part]
                a = min(i // 2, 1)
                total = None
                for k in range(2):
                    rows = gathered(a, k) if chunks == (0, 2) else G[a, k, chunks[0]].reshape(256, 512)
                    if i < 2:
                        right = jnp.concatenate([WG[i, k, 2 * l_to], WG[i, k, 2 * l_to + 1]], axis=1)
                        term = nn(rows, right)
                    else:
                        right = jnp.concatenate([WD[k, 2 * l_to], WD[k, 2 * l_to + 1]], axis=0)
                        term = nt(rows, right)
                    total = term if total is None else total + term
                for half in range(2):
                    block = total[:, half * 128 : half * 128 + 128]
                    PS[part, i, chunks[0] : chunks[1], :, :, half] = block.reshape(
                        chunks[1] - chunks[0], 2, 4, 32, 128
                    )
            one = (parts, (i, i + 1), chunks)
            to_twin[unit].append(copy(at(PS, one, cc), at(DR, one), twin))

    to_twin, yfar, ynear = {}, {}, {}

    def at(ref, unit, *more):
        return ref.at[(*(pl.ds(first, end - first) for first, end in unit), *more)]

    def over_unit(unit):
        parts, arrays_of, chunks = unit
        return [(p, i, q) for p in range(*parts) for i in range(*arrays_of) for q in range(*chunks)]

    def sum_start(unit):
        for made in to_twin[unit]:
            made.wait()
        for u in over_unit(unit):
            PS[(*u, c)] += DR[u]
        yfar[unit, 0] = copy(at(PS, unit, c, yf, 0), at(RF, unit, 0), dev(y=yp))
        yfar[unit, 1] = copy(at(PS, unit, c, yf, 1), at(RF, unit, 1), dev(y=ym))
        ynear[unit, 0, 1] = copy(at(PS, unit, c, yp, 1), at(RN, unit, 0, 1), dev(y=yp))
        ynear[unit, 1, 0] = copy(at(PS, unit, c, ym, 0), at(RN, unit, 1, 0), dev(y=ym))

    def sum_middle(unit):
        yfar[unit, 0].wait()
        for u in over_unit(unit):
            PS[(*u, c, yp, 0)] += RF[(*u, 0)]
        ynear[unit, 0, 0] = copy(at(PS, unit, c, yp, 0), at(RN, unit, 0, 0), dev(y=yp))
        yfar[unit, 1].wait()
        for u in over_unit(unit):
            PS[(*u, c, ym, 1)] += RF[(*u, 1)]
        ynear[unit, 1, 1] = copy(at(PS, unit, c, ym, 1), at(RN, unit, 1, 1), dev(y=ym))

    def sum_arrived(unit):
        for side in range(2):
            for half in range(2):
                ynear[unit, side, half].wait()

    def sum_end(part, i, q):
        return PS[part, i, q, c, y] + RN[part, i, q, 0] + RN[part, i, q, 1]

    def make_hidden(unit):
        sum_arrived(unit)
        for part in range(*unit[0]):
            for q in range(2):
                gate, up = sum_end(part, 0, q), sum_end(part, 1, q)
                GU[part, 0, q] = gate
                GU[part, 1, q] = up
                DL[part, c, y, 2, q] = (gate * jax.nn.sigmoid(gate) * up).astype(BF16)

    def make_deltas(unit):
        sum_arrived(unit)
        for part, _, q in over_unit(unit):
            gate, up, hidden_grad = GU[part, 0, q], GU[part, 1, q], sum_end(part, 2, q)
            squashed = jax.nn.sigmoid(gate)
            activated = gate * squashed
            slope = squashed * (1.0 + gate * (1.0 - squashed))
            DL[part, c, y, 0, q] = (hidden_grad * up * slope).astype(BF16)
            DL[part, c, y, 1, q] = (hidden_grad * activated).astype(BF16)

    dp, dm, far_d, over = {}, {}, {}, {}

    def delta_at(group, at_y, *half):
        parts, kinds, chunks = (pl.ds(first, end - first) for first, end in group)
        return DL.at[(parts, c, at_y, kinds, chunks, *half)]

    def give(group):
        for half in range(2):
            part = delta_at(group, y, half)
            dp[group, half] = copy(part, part, dev(y=yp))
            part = delta_at(group, y, 1 - half)
            dm[group, 1 - half] = copy(part, part, dev(y=ym))
        over[group] = [copy(delta_at(group, y), delta_at(group, y), twin)]

    def give_on(group):
        dp[group, 0].wait()
        part = delta_at(group, ym, 0)
        far_d[group, 0] = copy(part, part, dev(y=yp))
        dm[group, 1].wait()
        part = delta_at(group, yp, 1)
        far_d[group, 1] = copy(part, part, dev(y=ym))

    def give_over(group):
        dp[group, 1].wait()
        over[group].append(copy(delta_at(group, ym), delta_at(group, ym), twin))
        dm[group, 0].wait()
        over[group].append(copy(delta_at(group, yp), delta_at(group, yp), twin))

    def give_end(group):
        far_d[group, 0].wait()
        far_d[group, 1].wait()
        over[group].append(copy(delta_at(group, yf), delta_at(group, yf), twin))

    def given(group):
        for made in over[group]:
            made.wait()

    def delta(kind, part, q, owners=(0, 1)):
        return jnp.concatenate([DL[part, :, :, kind, q, half].reshape(256, 128) for half in owners], axis=1)

    def delta_all(kind, part, owners=(0, 1)):
        return jnp.concatenate([delta(kind, part, q, owners) for q in range(2)], axis=0)

    halves = (h, 1 - h)

    def grads_of_weights(i, part):
        for r in range(2):
            if i == 0:
                Z[0, 2 * part + r] = nn(GT[halves[r]], delta_all(0, part)).reshape(2, 256, 256)
            elif i == 1:
                block = nn(GT[halves[r]], delta_all(1, part, (cc, c))).reshape(2, 256, 256)
                ZU[0, 2 * part + r] = block[:, :, :128]
                ZU[1, 2 * part + r] = block[:, :, 128:]
            else:
                block = tn(delta_all(2, part), gathered(1, halves[r]))
                for j in range(2):
                    Z[2, 2 * part + r, j] = jnp.concatenate(
                        [block[j * 128 : j * 128 + 128, :256], block[j * 128 : j * 128 + 128, 256:]], axis=0
                    )

    zfar, znear = {}, {}

    def stream(i):
        if i in (0, 2):
            return [View(ref, i) for ref in (Z, ZS, ZF, ZN)]
        return [View(ref, i // 2) for ref in (ZU, ZSU, ZFU, ZNU)]

    def wsum_near(i):
        part, out, _, near = stream(i)
        if i == 2:
            for side, to_z in enumerate((zo, zn)):
                out[side] = part[side].astype(BF16)
                znear[2, side] = copy(out.at(side), near.at(side), dev(z=to_z))
            return
        out[0, 1] = part[0, 1].astype(BF16)
        znear[i, 0, 1] = copy(out.at(0, 1), near.at(0, 1), dev(z=zo))
        out[1, 0] = part[1, 0].astype(BF16)
        znear[i, 1, 0] = copy(out.at(1, 0), near.at(1, 0), dev(z=zn))

    def wsum_far(i):
        part, out, far, _ = stream(i)
        out[2] = part[3].astype(BF16)
        if i == 2:
            zfar[2] = copy(out.at(2), far.at(), dev(z=zf))
            return
        zfar[i, 0] = copy(out.at(2, 0), far.at(0), dev(z=zn))
        zfar[i, 1] = copy(out.at(2, 1), far.at(1), dev(z=zo))

    def wsum_middle(i):
        part, out, far, near = stream(i)
        zfar[i, 0].wait()
        out[0, 0] = (part[0, 0] + far[0].astype(F32)).astype(BF16)
        znear[i, 0, 0] = copy(out.at(0, 0), near.at(0, 0), dev(z=zo))
        zfar[i, 1].wait()
        out[1, 1] = (part[1, 1] + far[1].astype(F32)).astype(BF16)
        znear[i, 1, 1] = copy(out.at(1, 1), near.at(1, 1), dev(z=zn))

    last = []
    half_at = pl.ds(pl.multiple_of(c * 512, 512), 512)

    def wsum_end(i):
        part, _, far, near = stream(i)
        sums = []
        for half in range(2):
            for side in range(2):
                znear[(i, side) if i == 2 else (i, side, half)].wait()
            total = part[2, half] + near[0, half].astype(F32) + near[1, half].astype(F32)
            if i == 2:
                zfar[2].wait()
                total = total + far[half].astype(F32)
            sums.append(total)
        done = [total * factor for total in sums]
        if i == 0:
            for half in range(2):
                low, high = done[half][:, :128], done[half][:, 128:]
                SX[0, pl.ds(half * 256, 256), :] = jnp.where(c == 0, high, low)
                S[0, pl.ds(half * 256, 256), :] = jnp.where(c == 0, low, high)
            last.append(copy(SX.at[0], gg_ref.at[half_at, :], twin))
            gg_ref[half_at, :] = S[0]
        elif i == 1:
            for half in range(2):
                SX[1, pl.ds(half * 256, 256), :] = done[half]
            last.append(copy(SX.at[1], ug_ref.at[half_at, :], twin))
        elif i == 3:
            for half in range(2):
                ug_ref[pl.ds(pl.multiple_of(c * 512 + half * 256, 256), 256), :] = done[half]
        else:
            blocks = [jnp.concatenate([part[:128], part[128:]], axis=1) for part in done]
            SD[...] = jnp.where(c == 0, blocks[1], blocks[0])
            last.append(copy(SD, dg_ref.at[:, half_at], twin))
            dg_ref[:, half_at] = jnp.where(c == 0, blocks[0], blocks[1])

    def input_rows(q):
        left = jnp.concatenate([delta(kind, part, q) for part in range(2) for kind in range(2)], axis=1)
        for k in range(2):
            right = jnp.concatenate(
                [WG[kind, k, 2 * sides[part] + b] for part in range(2) for kind in range(2) for b in range(2)], axis=1
            )
            term = nt(left, right).reshape(4, 2, 32, 512)
            X[2 * q, :, k] = term[:, 0]
            X[2 * q + 1, :, k] = term[:, 1]

    xfar, xnear = {}, {}

    def isum_start(q):
        XB[q] = X[q, xf].astype(BF16)
        xfar[q, 0] = copy(XB.at[q, 0], XF.at[q, 0], dev(x=xp))
        xfar[q, 1] = copy(XB.at[q, 1], XF.at[q, 1], dev(x=xm))
        xnear[q, 0, 1] = copy(X.at[q, xp, 1], XN.at[q, 0, 1], dev(x=xp))
        xnear[q, 1, 0] = copy(X.at[q, xm, 0], XN.at[q, 1, 0], dev(x=xm))

    def isum_middle(q):
        xfar[q, 0].wait()
        X[q, xp, 0] += XF[q, 0].astype(F32)
        xnear[q, 0, 0] = copy(X.at[q, xp, 0], XN.at[q, 0, 0], dev(x=xp))
        xfar[q, 1].wait()
        X[q, xm, 1] += XF[q, 1].astype(F32)
        xnear[q, 1, 1] = copy(X.at[q, xm, 1], XN.at[q, 1, 1], dev(x=xm))

    def isum_end(q):
        for side in range(2):
            for half in range(2):
                xnear[q, side, half].wait()
        for k in range(2):
            IB[q, k] = (X[q, x, k] + XN[q, 0, k] + XN[q, 1, k]).astype(BF16)

    FIRST, SECOND = COPIES, COPIES + 4

    def arrives(index, ref):
        return pltpu.make_async_copy(ref, ref, recv.at[index])

    def send_back(e):
        far = turn(y - x, e)
        copy_back(IB.at[e], BB.at[far], dev(y=turn(x, -e)), far == 0, FIRST + far)

    def copy_back(src, dst, to, here, index):
        made = Copy(sems, src, dst, to, here, index)
        made.done = True
        sent.append(made.start())

    def pass_back():
        for d in range(4):
            arrives(FIRST + d, BB.at[d]).wait()
            to_x = turn(y, d)
            far = turn(to_x - x, 0)
            for other in (1, 0):
                copy_back(
                    BB.at[d, ll if other else l],
                    ig_ref.at[pl.ds(pl.multiple_of(l * 128 + x * 32, 32), 32), :],
                    dev(x=to_x, z=zo if other else z),
                    None if other else far == 0,
                    SECOND + 2 * far + other,
                )

    def back_here():
        for n in range(8):
            arrives(SECOND + n, ig_ref.at[pl.ds(0, 32), :]).wait()

    GATE_UP, HIDDEN = 0, 1
    both = (0, 2)
    gate_up = [((part, part + 1), both, both) for part in range(2)]
    down = [(both, (2, 3), (q, q + 1)) for q in range(2)]
    hidden = [((part, part + 1), (2, 3), both) for part in range(2)]
    deltas = [(both, both, (q, q + 1)) for q in range(2)]
    move(0)
    send_weights(0)
    send_weights_to(0, 0, False)
    send_weights_to(0, 0, True)
    send_weights_to(0, 1, False)
    send_weights_to(0, 1, True)
    move(1)
    send_weights(1)
    send_weights_to(1, 0, False)
    send_weights_to(1, 0, True)
    send_weights_to(1, 1, False)
    send_weights_to(1, 1, True)
    send_weights(2)
    spread(0, 0)
    spread(0, 1)
    pass_weights(0, 0)
    pass_tokens(0, 0)
    pass_tokens(0, 1)
    pass_weights(0, 1)
    spread(1, 0)
    spread(1, 1)
    weights_here(0, 0)
    pass_weights(1, 1)
    send_weights_to(2, 0, False)
    pass_weights(1, 0)
    send_weights_to(2, 0, True)
    send_weights_to(2, 1, True)
    send_weights_to(2, 1, False)
    tokens_here(0)
    weights_here(1, 0)
    multiply(gate_up[0])
    sum_start(gate_up[0])
    pass_tokens(1, 0)
    weights_here(0, 1)
    weights_here(1, 1)
    multiply(gate_up[1])
    sum_middle(gate_up[0])
    pass_weights(2, 0)
    sum_start(gate_up[1])
    pass_tokens(1, 1)
    pass_weights(2, 1)
    for k in range(2):
        GT[k] = gathered(0, k).T
    make_hidden(gate_up[0])
    give(hidden[0])
    sum_middle(gate_up[1])
    weights_here(2, 0)
    weights_here(2, 1)
    tokens_here(1)
    multiply(down[0])
    multiply(down[1])
    give_on(hidden[0])
    give_over(hidden[0])
    sum_start(down[0])
    sum_start(down[1])
    make_hidden(gate_up[1])
    give(hidden[1])
    give_end(hidden[0])
    sum_middle(down[0])
    sum_middle(down[1])
    given(hidden[0])
    grads_of_weights(2, 0)
    wsum_near(2)
    give_on(hidden[1])
    give_over(hidden[1])
    make_deltas(down[0])
    give(deltas[0])
    make_deltas(down[1])
    give(deltas[1])
    give_end(hidden[1])
    given(hidden[1])
    grads_of_weights(2, 1)
    wsum_far(2)
    give_on(deltas[0])
    give_over(deltas[0])
    give_on(deltas[1])
    give_over(deltas[1])
    give_end(deltas[0])
    give_end(deltas[1])
    given(deltas[0])
    input_rows(0)
    isum_start(0)
    isum_start(1)
    given(deltas[1])
    grads_of_weights(0, 1)
    wsum_far(0)
    grads_of_weights(0, 0)
    wsum_near(0)
    input_rows(1)
    isum_start(2)
    isum_start(3)
    grads_of_weights(1, 1)
    wsum_far(1)
    wsum_far(3)
    grads_of_weights(1, 0)
    wsum_near(1)
    wsum_near(3)
    isum_middle(0)
    isum_middle(1)
    isum_middle(2)
    isum_middle(3)
    wsum_middle(0)
    isum_end(0)
    send_back(0)
    wsum_middle(1)
    wsum_middle(3)
    isum_end(1)
    send_back(1)
    isum_end(2)
    send_back(2)
    isum_end(3)
    send_back(3)
    wsum_end(2)
    pass_back()
    wsum_end(0)
    wsum_end(1)
    wsum_end(3)
    back_here()
    for made in last:
        made.wait()
    for made in sent:
        assert made.done and sems[2][0] <= COPIES
        made.sent()


def put_out(a, b, c, d, a_out, b_out, c_out, d_out, sems):
    copies = [
        pltpu.make_async_copy(src, dst, sems.at[n])
        for n, (src, dst) in enumerate([(a, a_out), (b, b_out), (c, c_out), (d, d_out)])
    ]
    for made in copies:
        made.start()
    for made in copies:
        made.wait()


def solution(mesh):
    def shards(tokens, out_grad, gate_weight, up_weight, down_weight):
        factor = 1.0 / math.sqrt(tokens.shape[0] * mesh.shape["fsdp"])
        vmem = pl.BlockSpec(memory_space=pltpu.VMEM)
        made = pl.pallas_call(
            functools.partial(kernel, factor),
            out_shape=(
                pltpu.VMEM((256, 512), BF16),
                pltpu.VMEM((1024, 128), F32),
                pltpu.VMEM((1024, 128), F32),
                pltpu.VMEM((128, 1024), F32),
            ),
            in_specs=[pl.BlockSpec(memory_space=pl.ANY)] * 5,
            out_specs=(vmem,) * 4,
            scratch_shapes=[
                pltpu.VMEM((2, 256, 512), BF16),
                pltpu.VMEM((2, 1024, 128), BF16),
                pltpu.VMEM((128, 1024), BF16),
                pltpu.VMEM((2, 2, 2, 4, 64, 512), BF16),
                pltpu.VMEM((2, 512, 512), BF16),
                pltpu.VMEM((2, 2, 4, 512, 128), BF16),
                pltpu.VMEM((2, 4, 128, 512), BF16),
                pltpu.VMEM((2, 3, 2, 2, 4, 2, 32, 128), F32),
                pltpu.VMEM((2, 3, 2, 4, 2, 32, 128), F32),
                pltpu.VMEM((2, 3, 2, 2, 32, 128), F32),
                pltpu.VMEM((2, 3, 2, 2, 2, 32, 128), F32),
                pltpu.VMEM((2, 2, 2, 2, 32, 128), F32),
                pltpu.VMEM((2, 2, 4, 3, 2, 2, 32, 128), BF16),
                pltpu.VMEM((4, 4, 2, 32, 512), F32),
                pltpu.VMEM((4, 2, 32, 512), BF16),
                pltpu.VMEM((4, 2, 32, 512), BF16),
                pltpu.VMEM((4, 2, 2, 32, 512), F32),
                pltpu.VMEM((4, 2, 32, 512), BF16),
                pltpu.VMEM((4, 2, 32, 512), BF16),
                pltpu.VMEM((3, 4, 2, 256, 256), F32),
                pltpu.VMEM((3, 3, 2, 256, 256), BF16),
                pltpu.VMEM((3, 2, 256, 256), BF16),
                pltpu.VMEM((3, 2, 2, 256, 256), BF16),
                pltpu.VMEM((2, 4, 2, 256, 128), F32),
                pltpu.VMEM((2, 3, 2, 256, 128), BF16),
                pltpu.VMEM((2, 2, 256, 128), BF16),
                pltpu.VMEM((2, 2, 2, 256, 128), BF16),
                pltpu.VMEM((2, 512, 128), F32),
                pltpu.VMEM((2, 512, 128), F32),
                pltpu.VMEM((128, 512), F32),
                pltpu.SemaphoreType.DMA((COPIES + 12,)),
                pltpu.SemaphoreType.DMA((COPIES + 12,)),
                pltpu.SemaphoreType.DMA((3,)),
                pltpu.SemaphoreType.DMA((5,)),
            ],
            compiler_params=pltpu.CompilerParams(
                collective_id=0, has_side_effects=True, vmem_limit_bytes=60 * 1024 * 1024
            ),
        )(tokens, out_grad, gate_weight, up_weight, down_weight)
        return pl.pallas_call(
            put_out,
            out_shape=tuple(jax.ShapeDtypeStruct(part.shape, part.dtype) for part in made),
            in_specs=[vmem] * 4,
            out_specs=(pl.BlockSpec(memory_space=pl.ANY),) * 4,
            scratch_shapes=[pltpu.SemaphoreType.DMA((4,))],
        )(*(pltpu.with_memory_space_constraint(part, pltpu.VMEM) for part in made))

    return jax.shard_map(
        shards,
        mesh=mesh,
        in_specs=(P("fsdp", "tp"),) * 4 + (P("tp", "fsdp"),),
        out_specs=(P("fsdp", "tp"),) * 3 + (P("tp", "fsdp"),),
        check_vma=False,
    )
```

```python
import functools
import math

import jax
import jax.numpy as jnp
from jax import lax
from jax.experimental import pallas as pl
from jax.experimental.pallas import tpu as pltpu
from jax.sharding import PartitionSpec as P

MESH = pl.DeviceIdType.MESH
F32, BF16 = jnp.float32, jnp.bfloat16
COPIES = 200


class Copy:
    def __init__(self, sems, src, dst, to, here=None, index=None):
        if index is None:
            index = sems[2][0]
            sems[2][0] += 1
        send, recv = sems[0].at[index], sems[1].at[index]
        self.remote = pltpu.make_async_remote_copy(
            src_ref=src, dst_ref=dst, send_sem=send, recv_sem=recv, device_id=to, device_id_type=MESH
        )
        self.local = None if here is None else pltpu.make_async_copy(src, dst, recv)
        self.here = here
        self.done = False

    def start(self):
        if self.here is None:
            self.remote.start()
        else:
            pl.when(self.here)(self.local.start)
            pl.when(jnp.logical_not(self.here))(self.remote.start)
        return self

    def wait(self):
        if not self.done:
            self.remote.wait_recv()
        self.done = True

    def sent(self):
        if self.here is None:
            self.remote.wait_send()
        else:
            pl.when(jnp.logical_not(self.here))(self.remote.wait_send)


class View:
    def __init__(self, ref, *lead):
        self.ref, self.lead = ref, lead

    def place(self, key):
        return (*self.lead, *(key if isinstance(key, tuple) else (key,)))

    def __getitem__(self, key):
        return self.ref[self.place(key)]

    def __setitem__(self, key, value):
        self.ref[self.place(key)] = value

    def at(self, *key):
        return self.ref.at[self.place(key)]


def nt(a, b):
    return lax.dot_general(a, b, (((1,), (1,)), ((), ())), preferred_element_type=F32)


def tn(a, b):
    return lax.dot_general(a, b, (((0,), (0,)), ((), ())), preferred_element_type=F32)


def nn(a, b):
    return jnp.dot(a, b, preferred_element_type=F32)


def kernel(
    factor,
    tok_ref, grd_ref, gate_ref, up_ref, down_ref,
    ig_ref, gg_ref, ug_ref, dg_ref,
    TV, WV, WDV, G, GT, WG, WD, PS, DR, RF, RN, GU, DL, X, XB, XF, XN, IB, BB,
    Z, ZS, ZF, ZN, ZU, ZSU, ZFU, ZNU, S, SX, SD,
    send, recv, local_sem, load_sem,
):
    f, t = lax.axis_index("fsdp"), lax.axis_index("tp")
    h, y = lax.div(f, 4), lax.rem(f, 4)
    c = lax.rem(t, 2)
    x = lax.rem(lax.div(t, 2), 4)
    l = lax.div(t, 8)
    z = 2 * h + l
    sems = (send, recv, [0])
    sent = []

    def dev(x=x, y=y, z=z, c=c):
        return (lax.div(z, 2) * 4 + y, (lax.rem(z, 2) * 4 + x) * 2 + c)

    def copy(src, dst, to, here=None, index=None):
        made = Copy(sems, src, dst, to, here, index)
        sent.append(made)
        return made.start()

    def turn(v, k):
        return lax.rem(v + k + 4, 4)

    xp, xm, yp, ym, zp, zm = (turn(v, k) for v in (x, y, z) for k in (1, -1))
    yf, xf, zf = turn(y, 2), turn(x, 2), turn(z, 2)
    cc, ll = 1 - c, 1 - l
    zo = 2 * h + ll
    zn = turn(z, 2 * l - 1)
    diagonal = x == y
    twin = dev(c=cc)

    loads = [
        pltpu.make_async_copy(src, dst, load_sem.at[n])
        for n, (src, dst) in enumerate(
            [(tok_ref, TV.at[0]), (grd_ref, TV.at[1]), (gate_ref, WV.at[0]), (up_ref, WV.at[1]), (down_ref, WDV)]
        )
    ]
    for load in loads:
        load.start()

    barrier = pltpu.get_barrier_semaphore()
    peers = [
        twin, dev(x=xp), dev(x=xm), dev(y=yp), dev(y=ym),
        dev(z=zp), dev(z=zm), dev(z=zf), dev(z=zp, c=cc), dev(z=zm, c=cc),
    ]
    for e in range(4):
        there, back_there = dict(x=turn(y, e), y=x), dict(x=y, y=turn(x, -e))
        peers += [dev(z=zo, **there), dev(z=zo, **back_there)]
        if e > 0:
            peers += [dev(**there), dev(**back_there)]
    for peer in peers:
        pl.semaphore_signal(barrier, inc=1, device_id=peer, device_id_type=MESH)

    @pl.when(jnp.logical_not(diagonal))
    def _():
        pl.semaphore_signal(barrier, inc=2, device_id=dev(x=y, y=x), device_id_type=MESH)
        pl.semaphore_wait(barrier, len(peers) + 2)

    @pl.when(diagonal)
    def _():
        pl.semaphore_wait(barrier, len(peers))

    moved = {}

    def move(a):
        loads[a].wait()
        for other in (1, 0):
            to_l = ll if other else l
            for e in range(4):
                to_x = turn(y, e)
                moved[a, other, e] = copy(
                    TV.at[a, pl.ds(pl.multiple_of(to_l * 128 + to_x * 32, 32), 32), :],
                    G.at[a, l, e // 2, to_x, pl.ds(e % 2 * 32, 32), :],
                    dev(x=to_x, y=x, z=zo if other else z),
                    diagonal if e == 0 and not other else None,
                )

    def weight_piece(i, k):
        half = pl.multiple_of(k * 512, 512)
        if i < 2:
            return WV.at[i, pl.ds(half, 512), :]
        return WDV.at[:, pl.ds(half, 512)]

    def weight_slot(i, at_z, core):
        at_h, block = lax.div(at_z, 2), lax.rem(at_z, 2) * 2 + core
        return WG.at[i, at_h, block] if i < 2 else WD.at[at_h, block]

    own_weights, from_twin, wn, wo, far_w = {}, {}, {}, {}, {}
    cores = (c, cc)

    def send_weights(i):
        loads[2 + i].wait()
        slot = weight_slot(i, z, c)
        mine = pltpu.make_async_copy(weight_piece(i, c), slot, local_sem.at[i])
        mine.start()
        own_weights[i] = mine
        from_twin[i] = copy(weight_piece(i, cc), slot, twin)

    def send_weights_to(i, s, over_n):
        to_z, made = (zn, wn) if over_n else (zo, wo)
        made[i, s] = copy(weight_piece(i, cores[s]), weight_slot(i, z, c), dev(z=to_z, c=cores[s]))

    def pass_weights(i, s):
        over_n = s == 0 or i == 0
        arrived, at_z, to_z = (wo, zo, zn) if over_n else (wn, zn, zo)
        arrived[i, s].wait()
        slot = weight_slot(i, at_z, cores[s])
        far_w[i, s] = copy(slot, slot, dev(z=to_z))

    def weights_here(i, part):
        if part == 0:
            for s in range(2):
                wn[i, s].wait()
                wo[i, s].wait()
        else:
            own_weights[i].wait()
            from_twin[i].wait()
            far_w[i, 0].wait()
            far_w[i, 1].wait()

    gp, gm, far_g = {}, {}, {}

    def spread(a, other):
        for e in range(4):
            moved[a, other, e].wait()
        slot = G.at[a, ll if other else l, :, x]
        gp[a, other] = copy(slot, slot, dev(x=xp))
        gm[a, other] = copy(slot, slot, dev(x=xm))

    def pass_tokens(a, side):
        if side == 0:
            gp[a, 0].wait()
            slot = G.at[a, l, :, xm]
            far_g[a, 0] = copy(slot, slot, dev(x=xp))
        else:
            gm[a, 1].wait()
            slot = G.at[a, ll, :, xp]
            far_g[a, 1] = copy(slot, slot, dev(x=xm))

    def tokens_here(a):
        gp[a, 1].wait()
        gm[a, 0].wait()
        far_g[a, 0].wait()
        far_g[a, 1].wait()

    sides = (ll, l)

    def gathered(a, k):
        return G[a, k].reshape(512, 512)

    def multiply(unit):
        parts, arrays_of, chunks = unit
        to_twin[unit] = []
        for i in range(*arrays_of):
            for part in range(*parts):
                l_to = sides[part]
                a = min(i // 2, 1)
                total = None
                for k in range(2):
                    rows = gathered(a, k) if chunks == (0, 2) else G[a, k, chunks[0]].reshape(256, 512)
                    if i < 2:
                        right = jnp.concatenate([WG[i, k, 2 * l_to], WG[i, k, 2 * l_to + 1]], axis=1)
                        term = nn(rows, right)
                    else:
                        right = jnp.concatenate([WD[k, 2 * l_to], WD[k, 2 * l_to + 1]], axis=0)
                        term = nt(rows, right)
                    total = term if total is None else total + term
                for half in range(2):
                    block = total[:, half * 128 : half * 128 + 128]
                    PS[part, i, chunks[0] : chunks[1], :, :, half] = block.reshape(
                        chunks[1] - chunks[0], 2, 4, 32, 128
                    )
            one = (parts, (i, i + 1), chunks)
            to_twin[unit].append(copy(at(PS, one, cc), at(DR, one), twin))

    to_twin, yfar, ynear = {}, {}, {}

    def at(ref, unit, *more):
        return ref.at[(*(pl.ds(first, end - first) for first, end in unit), *more)]

    def over_unit(unit):
        parts, arrays_of, chunks = unit
        return [(p, i, q) for p in range(*parts) for i in range(*arrays_of) for q in range(*chunks)]

    def sum_start(unit):
        for made in to_twin[unit]:
            made.wait()
        for u in over_unit(unit):
            PS[(*u, c)] += DR[u]
        yfar[unit, 0] = copy(at(PS, unit, c, yf, 0), at(RF, unit, 0), dev(y=yp))
        yfar[unit, 1] = copy(at(PS, unit, c, yf, 1), at(RF, unit, 1), dev(y=ym))
        ynear[unit, 0, 1] = copy(at(PS, unit, c, yp, 1), at(RN, unit, 0, 1), dev(y=yp))
        ynear[unit, 1, 0] = copy(at(PS, unit, c, ym, 0), at(RN, unit, 1, 0), dev(y=ym))

    def sum_middle(unit):
        yfar[unit, 0].wait()
        for u in over_unit(unit):
            PS[(*u, c, yp, 0)] += RF[(*u, 0)]
        ynear[unit, 0, 0] = copy(at(PS, unit, c, yp, 0), at(RN, unit, 0, 0), dev(y=yp))
        yfar[unit, 1].wait()
        for u in over_unit(unit):
            PS[(*u, c, ym, 1)] += RF[(*u, 1)]
        ynear[unit, 1, 1] = copy(at(PS, unit, c, ym, 1), at(RN, unit, 1, 1), dev(y=ym))

    def sum_arrived(unit):
        for side in range(2):
            for half in range(2):
                ynear[unit, side, half].wait()

    def sum_end(part, i, q):
        return PS[part, i, q, c, y] + RN[part, i, q, 0] + RN[part, i, q, 1]

    def make_hidden(unit):
        sum_arrived(unit)
        for part in range(*unit[0]):
            for q in range(2):
                gate, up = sum_end(part, 0, q), sum_end(part, 1, q)
                GU[part, 0, q] = gate
                GU[part, 1, q] = up
                DL[part, c, y, 2, q] = (gate * jax.nn.sigmoid(gate) * up).astype(BF16)

    def make_deltas(unit):
        sum_arrived(unit)
        for part, _, q in over_unit(unit):
            gate, up, hidden_grad = GU[part, 0, q], GU[part, 1, q], sum_end(part, 2, q)
            squashed = jax.nn.sigmoid(gate)
            activated = gate * squashed
            slope = squashed * (1.0 + gate * (1.0 - squashed))
            DL[part, c, y, 0, q] = (hidden_grad * up * slope).astype(BF16)
            DL[part, c, y, 1, q] = (hidden_grad * activated).astype(BF16)

    dp, dm, far_d, over = {}, {}, {}, {}

    def delta_at(group, at_y, *half):
        parts, kinds, chunks = (pl.ds(first, end - first) for first, end in group)
        return DL.at[(parts, c, at_y, kinds, chunks, *half)]

    def give(group):
        for half in range(2):
            part = delta_at(group, y, half)
            dp[group, half] = copy(part, part, dev(y=yp))
            part = delta_at(group, y, 1 - half)
            dm[group, 1 - half] = copy(part, part, dev(y=ym))
        over[group] = [copy(delta_at(group, y), delta_at(group, y), twin)]

    def give_on(group):
        dp[group, 0].wait()
        part = delta_at(group, ym, 0)
        far_d[group, 0] = copy(part, part, dev(y=yp))
        dm[group, 1].wait()
        part = delta_at(group, yp, 1)
        far_d[group, 1] = copy(part, part, dev(y=ym))

    def give_over(group):
        dp[group, 1].wait()
        over[group].append(copy(delta_at(group, ym), delta_at(group, ym), twin))
        dm[group, 0].wait()
        over[group].append(copy(delta_at(group, yp), delta_at(group, yp), twin))

    def give_end(group):
        far_d[group, 0].wait()
        far_d[group, 1].wait()
        over[group].append(copy(delta_at(group, yf), delta_at(group, yf), twin))

    def given(group):
        for made in over[group]:
            made.wait()

    def delta(kind, part, q, owners=(0, 1)):
        return jnp.concatenate([DL[part, :, :, kind, q, half].reshape(256, 128) for half in owners], axis=1)

    def delta_all(kind, part, owners=(0, 1)):
        return jnp.concatenate([delta(kind, part, q, owners) for q in range(2)], axis=0)

    halves = (h, 1 - h)

    def grads_of_weights(i, part):
        for r in range(2):
            if i == 0:
                Z[0, 2 * part + r] = nn(GT[halves[r]], delta_all(0, part)).reshape(2, 256, 256)
            elif i == 1:
                block = nn(GT[halves[r]], delta_all(1, part, (cc, c))).reshape(2, 256, 256)
                ZU[0, 2 * part + r] = block[:, :, :128]
                ZU[1, 2 * part + r] = block[:, :, 128:]
            else:
                block = tn(delta_all(2, part), gathered(1, halves[r]))
                for j in range(2):
                    Z[2, 2 * part + r, j] = jnp.concatenate(
                        [block[j * 128 : j * 128 + 128, :256], block[j * 128 : j * 128 + 128, 256:]], axis=0
                    )

    zfar, znear = {}, {}

    def stream(i):
        if i in (0, 2):
            return [View(ref, i) for ref in (Z, ZS, ZF, ZN)]
        return [View(ref, i // 2) for ref in (ZU, ZSU, ZFU, ZNU)]

    def wsum_near(i):
        part, out, _, near = stream(i)
        if i == 2:
            for side, to_z in enumerate((zo, zn)):
                out[side] = part[side].astype(BF16)
                znear[2, side] = copy(out.at(side), near.at(side), dev(z=to_z))
            return
        out[0, 1] = part[0, 1].astype(BF16)
        znear[i, 0, 1] = copy(out.at(0, 1), near.at(0, 1), dev(z=zo))
        out[1, 0] = part[1, 0].astype(BF16)
        znear[i, 1, 0] = copy(out.at(1, 0), near.at(1, 0), dev(z=zn))

    def wsum_far(i):
        part, out, far, _ = stream(i)
        out[2] = part[3].astype(BF16)
        if i == 2:
            zfar[2] = copy(out.at(2), far.at(), dev(z=zf))
            return
        zfar[i, 0] = copy(out.at(2, 0), far.at(0), dev(z=zn))
        zfar[i, 1] = copy(out.at(2, 1), far.at(1), dev(z=zo))

    def wsum_middle(i):
        part, out, far, near = stream(i)
        zfar[i, 0].wait()
        out[0, 0] = (part[0, 0] + far[0].astype(F32)).astype(BF16)
        znear[i, 0, 0] = copy(out.at(0, 0), near.at(0, 0), dev(z=zo))
        zfar[i, 1].wait()
        out[1, 1] = (part[1, 1] + far[1].astype(F32)).astype(BF16)
        znear[i, 1, 1] = copy(out.at(1, 1), near.at(1, 1), dev(z=zn))

    last = []
    half_at = pl.ds(pl.multiple_of(c * 512, 512), 512)

    def wsum_end(i):
        part, _, far, near = stream(i)
        sums = []
        for half in range(2):
            for side in range(2):
                znear[(i, side) if i == 2 else (i, side, half)].wait()
            total = part[2, half] + near[0, half].astype(F32) + near[1, half].astype(F32)
            if i == 2:
                zfar[2].wait()
                total = total + far[half].astype(F32)
            sums.append(total)
        done = [total * factor for total in sums]
        if i == 0:
            for half in range(2):
                low, high = done[half][:, :128], done[half][:, 128:]
                SX[0, pl.ds(half * 256, 256), :] = jnp.where(c == 0, high, low)
                S[0, pl.ds(half * 256, 256), :] = jnp.where(c == 0, low, high)
            last.append(copy(SX.at[0], gg_ref.at[half_at, :], twin))
            gg_ref[half_at, :] = S[0]
        elif i == 1:
            for half in range(2):
                SX[1, pl.ds(half * 256, 256), :] = done[half]
            last.append(copy(SX.at[1], ug_ref.at[half_at, :], twin))
        elif i == 3:
            for half in range(2):
                ug_ref[pl.ds(pl.multiple_of(c * 512 + half * 256, 256), 256), :] = done[half]
        else:
            blocks = [jnp.concatenate([part[:128], part[128:]], axis=1) for part in done]
            SD[...] = jnp.where(c == 0, blocks[1], blocks[0])
            last.append(copy(SD, dg_ref.at[:, half_at], twin))
            dg_ref[:, half_at] = jnp.where(c == 0, blocks[0], blocks[1])

    def input_rows(q):
        left = jnp.concatenate([delta(kind, part, q) for part in range(2) for kind in range(2)], axis=1)
        for k in range(2):
            right = jnp.concatenate(
                [WG[kind, k, 2 * sides[part] + b] for part in range(2) for kind in range(2) for b in range(2)], axis=1
            )
            term = nt(left, right).reshape(4, 2, 32, 512)
            X[2 * q, :, k] = term[:, 0]
            X[2 * q + 1, :, k] = term[:, 1]

    xfar, xnear = {}, {}

    def isum_start(q):
        XB[q] = X[q, xf].astype(BF16)
        xfar[q, 0] = copy(XB.at[q, 0], XF.at[q, 0], dev(x=xp))
        xfar[q, 1] = copy(XB.at[q, 1], XF.at[q, 1], dev(x=xm))
        xnear[q, 0, 1] = copy(X.at[q, xp, 1], XN.at[q, 0, 1], dev(x=xp))
        xnear[q, 1, 0] = copy(X.at[q, xm, 0], XN.at[q, 1, 0], dev(x=xm))

    def isum_middle(q):
        xfar[q, 0].wait()
        X[q, xp, 0] += XF[q, 0].astype(F32)
        xnear[q, 0, 0] = copy(X.at[q, xp, 0], XN.at[q, 0, 0], dev(x=xp))
        xfar[q, 1].wait()
        X[q, xm, 1] += XF[q, 1].astype(F32)
        xnear[q, 1, 1] = copy(X.at[q, xm, 1], XN.at[q, 1, 1], dev(x=xm))

    def isum_end(q):
        for side in range(2):
            for half in range(2):
                xnear[q, side, half].wait()
        for k in range(2):
            IB[q, k] = (X[q, x, k] + XN[q, 0, k] + XN[q, 1, k]).astype(BF16)

    FIRST, SECOND = COPIES, COPIES + 4

    def arrives(index, ref):
        return pltpu.make_async_copy(ref, ref, recv.at[index])

    def send_back(e):
        far = turn(y - x, e)
        copy_back(IB.at[e], BB.at[far], dev(y=turn(x, -e)), far == 0, FIRST + far)

    def copy_back(src, dst, to, here, index):
        made = Copy(sems, src, dst, to, here, index)
        made.done = True
        sent.append(made.start())

    def pass_back():
        for d in range(4):
            arrives(FIRST + d, BB.at[d]).wait()
            to_x = turn(y, d)
            far = turn(to_x - x, 0)
            for other in (1, 0):
                copy_back(
                    BB.at[d, ll if other else l],
                    ig_ref.at[pl.ds(pl.multiple_of(l * 128 + x * 32, 32), 32), :],
                    dev(x=to_x, z=zo if other else z),
                    None if other else far == 0,
                    SECOND + 2 * far + other,
                )

    def back_here():
        for n in range(8):
            arrives(SECOND + n, ig_ref.at[pl.ds(0, 32), :]).wait()

    GATE_UP, HIDDEN = 0, 1
    both = (0, 2)
    gate_up = [((part, part + 1), both, both) for part in range(2)]
    down = [(both, (2, 3), (q, q + 1)) for q in range(2)]
    hidden = [((part, part + 1), (2, 3), both) for part in range(2)]
    deltas = [(both, both, (q, q + 1)) for q in range(2)]
    move(0)
    send_weights(0)
    send_weights_to(0, 0, False)
    send_weights_to(0, 0, True)
    send_weights_to(0, 1, False)
    send_weights_to(0, 1, True)
    move(1)
    send_weights(1)
    send_weights_to(1, 0, False)
    send_weights_to(1, 0, True)
    send_weights_to(1, 1, False)
    send_weights_to(1, 1, True)
    send_weights(2)
    spread(0, 0)
    spread(0, 1)
    pass_weights(0, 0)
    pass_tokens(0, 0)
    pass_tokens(0, 1)
    pass_weights(0, 1)
    spread(1, 0)
    spread(1, 1)
    weights_here(0, 0)
    pass_weights(1, 1)
    send_weights_to(2, 0, False)
    pass_weights(1, 0)
    send_weights_to(2, 0, True)
    send_weights_to(2, 1, True)
    send_weights_to(2, 1, False)
    tokens_here(0)
    weights_here(1, 0)
    multiply(gate_up[0])
    for k in range(2):
        GT[k] = gathered(0, k).T
    sum_start(gate_up[0])
    pass_tokens(1, 0)
    weights_here(0, 1)
    weights_here(1, 1)
    multiply(gate_up[1])
    sum_middle(gate_up[0])
    pass_weights(2, 0)
    sum_start(gate_up[1])
    pass_tokens(1, 1)
    pass_weights(2, 1)
    make_hidden(gate_up[0])
    give(hidden[0])
    sum_middle(gate_up[1])
    weights_here(2, 0)
    weights_here(2, 1)
    tokens_here(1)
    multiply(down[0])
    multiply(down[1])
    give_on(hidden[0])
    give_over(hidden[0])
    sum_start(down[0])
    sum_start(down[1])
    make_hidden(gate_up[1])
    give(hidden[1])
    give_end(hidden[0])
    sum_middle(down[0])
    sum_middle(down[1])
    given(hidden[0])
    grads_of_weights(2, 0)
    wsum_near(2)
    give_on(hidden[1])
    give_over(hidden[1])
    make_deltas(down[0])
    give(deltas[0])
    make_deltas(down[1])
    give(deltas[1])
    give_end(hidden[1])
    given(hidden[1])
    grads_of_weights(2, 1)
    wsum_far(2)
    give_on(deltas[0])
    give_over(deltas[0])
    give_on(deltas[1])
    give_over(deltas[1])
    give_end(deltas[0])
    give_end(deltas[1])
    given(deltas[0])
    input_rows(0)
    isum_start(0)
    isum_start(1)
    given(deltas[1])
    grads_of_weights(0, 1)
    wsum_far(0)
    grads_of_weights(0, 0)
    wsum_near(0)
    input_rows(1)
    isum_start(2)
    isum_start(3)
    grads_of_weights(1, 1)
    wsum_far(1)
    wsum_far(3)
    grads_of_weights(1, 0)
    wsum_near(1)
    wsum_near(3)
    isum_middle(0)
    isum_middle(1)
    isum_middle(2)
    isum_middle(3)
    wsum_middle(0)
    isum_end(0)
    send_back(0)
    wsum_middle(1)
    wsum_middle(3)
    isum_end(1)
    send_back(1)
    isum_end(2)
    send_back(2)
    isum_end(3)
    send_back(3)
    wsum_end(2)
    pass_back()
    wsum_end(0)
    wsum_end(1)
    wsum_end(3)
    back_here()
    for made in last:
        made.wait()
    for made in sent:
        assert made.done and sems[2][0] <= COPIES
        made.sent()


def put_out(a, b, c, d, a_out, b_out, c_out, d_out, sems):
    copies = [
        pltpu.make_async_copy(src, dst, sems.at[n])
        for n, (src, dst) in enumerate([(a, a_out), (b, b_out), (c, c_out), (d, d_out)])
    ]
    for made in copies:
        made.start()
    for made in copies:
        made.wait()


def solution(mesh):
    def shards(tokens, out_grad, gate_weight, up_weight, down_weight):
        factor = 1.0 / math.sqrt(tokens.shape[0] * mesh.shape["fsdp"])
        vmem = pl.BlockSpec(memory_space=pltpu.VMEM)
        made = pl.pallas_call(
            functools.partial(kernel, factor),
            out_shape=(
                pltpu.VMEM((256, 512), BF16),
                pltpu.VMEM((1024, 128), F32),
                pltpu.VMEM((1024, 128), F32),
                pltpu.VMEM((128, 1024), F32),
            ),
            in_specs=[pl.BlockSpec(memory_space=pl.ANY)] * 5,
            out_specs=(vmem,) * 4,
            scratch_shapes=[
                pltpu.VMEM((2, 256, 512), BF16),
                pltpu.VMEM((2, 1024, 128), BF16),
                pltpu.VMEM((128, 1024), BF16),
                pltpu.VMEM((2, 2, 2, 4, 64, 512), BF16),
                pltpu.VMEM((2, 512, 512), BF16),
                pltpu.VMEM((2, 2, 4, 512, 128), BF16),
                pltpu.VMEM((2, 4, 128, 512), BF16),
                pltpu.VMEM((2, 3, 2, 2, 4, 2, 32, 128), F32),
                pltpu.VMEM((2, 3, 2, 4, 2, 32, 128), F32),
                pltpu.VMEM((2, 3, 2, 2, 32, 128), F32),
                pltpu.VMEM((2, 3, 2, 2, 2, 32, 128), F32),
                pltpu.VMEM((2, 2, 2, 2, 32, 128), F32),
                pltpu.VMEM((2, 2, 4, 3, 2, 2, 32, 128), BF16),
                pltpu.VMEM((4, 4, 2, 32, 512), F32),
                pltpu.VMEM((4, 2, 32, 512), BF16),
                pltpu.VMEM((4, 2, 32, 512), BF16),
                pltpu.VMEM((4, 2, 2, 32, 512), F32),
                pltpu.VMEM((4, 2, 32, 512), BF16),
                pltpu.VMEM((4, 2, 32, 512), BF16),
                pltpu.VMEM((3, 4, 2, 256, 256), F32),
                pltpu.VMEM((3, 3, 2, 256, 256), BF16),
                pltpu.VMEM((3, 2, 256, 256), BF16),
                pltpu.VMEM((3, 2, 2, 256, 256), BF16),
                pltpu.VMEM((2, 4, 2, 256, 128), F32),
                pltpu.VMEM((2, 3, 2, 256, 128), BF16),
                pltpu.VMEM((2, 2, 256, 128), BF16),
                pltpu.VMEM((2, 2, 2, 256, 128), BF16),
                pltpu.VMEM((2, 512, 128), F32),
                pltpu.VMEM((2, 512, 128), F32),
                pltpu.VMEM((128, 512), F32),
                pltpu.SemaphoreType.DMA((COPIES + 12,)),
                pltpu.SemaphoreType.DMA((COPIES + 12,)),
                pltpu.SemaphoreType.DMA((3,)),
                pltpu.SemaphoreType.DMA((5,)),
            ],
            compiler_params=pltpu.CompilerParams(
                collective_id=0, has_side_effects=True, vmem_limit_bytes=60 * 1024 * 1024
            ),
        )(tokens, out_grad, gate_weight, up_weight, down_weight)
        return pl.pallas_call(
            put_out,
            out_shape=tuple(jax.ShapeDtypeStruct(part.shape, part.dtype) for part in made),
            in_specs=[vmem] * 4,
            out_specs=(pl.BlockSpec(memory_space=pl.ANY),) * 4,
            scratch_shapes=[pltpu.SemaphoreType.DMA((4,))],
        )(*(pltpu.with_memory_space_constraint(part, pltpu.VMEM) for part in made))

    return jax.shard_map(
        shards,
        mesh=mesh,
        in_specs=(P("fsdp", "tp"),) * 4 + (P("tp", "fsdp"),),
        out_specs=(P("fsdp", "tp"),) * 3 + (P("tp", "fsdp"),),
        check_vma=False,
    )
```
